256 devices in a mesh: pipe: 2 (over core), dp: 64 (over z, y, x_lo), tensor: 2 (over x_hi).
Axes of the slice: x: 4 (x_hi: 2, x_lo: 2; x = x_hi * 2 + x_lo), y: 4, z: 8, core: 2. Of those that a mesh axis runs over, the one named last changes fastest.
Arguments:
- hidden_in: bfloat16 [2, 128, 2, 64, 3584], P('pipe', 'dp'), may hold values from -60 to 60, as said below
- attention_probs: bfloat16 [2, 128, 2, 14, 64, 64], P('pipe', 'dp', None, 'tensor'), may hold values from 0 to 1, as said below
- norm_gain: float32 [2, 3584], P('pipe'), may hold values from 0.5 to 1.5
- value_weight: bfloat16 [2, 3584, 256], P('pipe', None, 'tensor'), may hold values from -0.09375 to 0.09375
- output_weight: bfloat16 [2, 1792, 3584], P('pipe', 'tensor'), may hold values from -0.125 to 0.125
- head_grad: bfloat16 [128, 2, 64, 3584], P('dp', 'tensor'), may hold values from -16 to 16
- policy_logprob: float32 [128, 2, 64], P('dp'), may hold values from -3 to -0.2
- reference_logprob: float32 [128, 2], P('dp'), may hold values from -96 to -12.8
- sequence_bounds: int32 [128, 3], P('dp'), may hold values from 1 to 64, as said below
Outputs:
- section_cotangent: bfloat16 [2, 128, 2, 64, 3584], P('pipe', 'dp', 'tensor')
- value_gradient: float32 [2, 3584, 256], P('pipe', 'dp', 'tensor')
- output_gradient: float32 [2, 3584, 1792], P('pipe', 'dp', 'tensor')
- gain_gradient: float32 [2, 3584], P('pipe', 'dp')
The draws below stay inside these ranges and needn't reach their ends.
Inputs may be any that keep to these rules, and one draw needn't show every extreme that they name: `sequence_bounds`: entry 0 is the prompt length, shared by the two sequences of a pair; a sequence's response is the positions from entry 0 up to its end (entry 1 for the chosen, entry 2 for the rejected sequence), and holds one position or more. `attention_probs`: each row is a causal attention distribution: zero above the diagonal, summing to one before rounding. `hidden_in`: activations of varying size from token to token.
All inputs are finite; a program needn't handle non-finite values.
Results may differ from the reference program's by a relative error of at most 0.017.
Values may be sent and summed in bfloat16 or wider, within the bound.
No kernel may reach another device: no remote copies, remote signals or barrier semaphores. Data moves between devices by JAX's collectives and lax.ppermute only.
A program may use at most 128 MiB of HBM per device.

```python
import math
import jax
import jax.numpy as jnp
from jax import lax

D = 3584
HEADS = 14
KV_HEADS = 2
HEAD_DIM = 128
SEQ = 64
PAIRS = 128
N_PIPE = 2
N_TENSOR = 2


def draw_hidden_in(key, part):
    key_main, key_scale = jax.random.split(key, 2)
    full_shape = (N_PIPE, PAIRS, 2, SEQ, D)
    row_scale = jnp.exp(jax.random.uniform(key_scale, (N_PIPE, PAIRS, 2, SEQ, 1), jnp.float32, 0.0, math.log(10.0)))
    noise = jnp.clip(jax.random.normal(key_main, full_shape, jnp.float32), -6.0, 6.0)
    return (row_scale * noise).astype(jnp.bfloat16)


def draw_attention_probs(key, part):
    key_noise, key_temper, key_slope = jax.random.split(key, 3)
    full_shape = (N_PIPE, PAIRS, 2, HEADS, SEQ, SEQ)
    head_shape = (N_PIPE, 1, 1, HEADS, 1, 1)
    temper = jnp.exp(jax.random.uniform(key_temper, head_shape, jnp.float32, math.log(0.5), math.log(3.0)))
    decay_slope = jnp.exp(jax.random.uniform(key_slope, head_shape, jnp.float32, math.log(0.5 / SEQ), 0.0))
    query_pos = jnp.arange(SEQ)[:, None]
    key_pos = jnp.arange(SEQ)[None, :]
    distance = (query_pos - key_pos).astype(jnp.float32)
    logits = jax.random.normal(key_noise, full_shape, jnp.float32) * temper - decay_slope * distance
    logits = jnp.where(key_pos <= query_pos, logits, -1000000000.0)
    return jax.nn.softmax(logits, axis=-1).astype(jnp.bfloat16)


def draw_sequence_bounds(key, part):
    key_prompt, key_extra, key_pick = jax.random.split(key, 3)
    pair_index = jnp.arange(PAIRS, dtype=jnp.int32)
    prompt = jax.random.randint(key_prompt, (PAIRS,), 1, SEQ // 4 + 1, jnp.int32)
    base_length = SEQ // 8 + SEQ // 2 * pair_index // PAIRS
    extra = jax.random.randint(key_extra, (PAIRS, 2), 0, SEQ // 8 + 1, jnp.int32)
    ends = jnp.minimum(prompt[:, None] + base_length[:, None] + extra, SEQ)
    picked = jax.random.randint(key_pick, (), 0, PAIRS, jnp.int32)
    full_end = (pair_index == picked)[:, None] & (jnp.arange(2, dtype=jnp.int32)[None, :] == 1)
    ends = jnp.where(full_end, SEQ, ends)
    return jnp.concatenate([prompt[:, None], ends], axis=1).astype(jnp.int32)


def levels(stream_key, dims, shards, smallest, largest):
    def one(position, shards_of):
        steps = jax.random.uniform(jax.random.fold_in(jax.random.fold_in(stream_key, 6), position), (shards_of,), jnp.float32, smallest / len(shards), largest / len(shards))
        return jnp.repeat(jnp.exp(steps), dims[position] // shards_of).reshape((-1,) + (1,) * (len(dims) - position - 1))

    factor_of = one(*shards[0])
    for cut in shards[1:]:
        factor_of = factor_of * one(*cut)
    return factor_of


def gaussian(stream_key, dims, deviation, most, cuts=(), held_as=jnp.bfloat16):
    factor_of = levels(stream_key, dims, cuts, -0.22, 0.18) if cuts else 1.0
    drawn = jax.random.normal(stream_key, dims, jnp.float32) * deviation * factor_of
    return jnp.minimum(jnp.maximum(drawn, -most), most).astype(held_as)


def setup_inputs(seed: int = 0) -> dict:
    key_of = jax.random.split(jax.random.key(seed), 10)
    hidden_in = draw_hidden_in(jax.random.fold_in(key_of[9], 71), 0)
    attention_probs = draw_attention_probs(jax.random.fold_in(key_of[9], 71), 0)
    norm_gain = jnp.clip(1.0 + 0.1 * jax.random.normal(key_of[2], (N_PIPE, D), jnp.float32), 0.5, 1.5)
    value_weight = gaussian(key_of[3], (N_PIPE, D, KV_HEADS * HEAD_DIM), D ** -0.5, 0.09375, ((0, 2), (2, 2)))
    output_weight = gaussian(key_of[4], (N_PIPE, HEADS * HEAD_DIM, D), (HEADS * HEAD_DIM) ** -0.5, 0.125, ((0, 2), (1, 2)))
    head_grad = gaussian(key_of[5], (PAIRS, 2, SEQ, D), 4.0, 16.0, ((0, 64), (1, 2)))
    policy_logprob = jnp.clip(-3.0 + 2.8 * jax.random.uniform(key_of[6], (PAIRS, 2, SEQ), jnp.float32) ** levels(key_of[6], (PAIRS, 2, SEQ), ((0, 64),), -0.2, 0.2), -3.0, -0.2)
    reference_logprob = jnp.clip(-96.0 + 83.2 * jax.random.uniform(key_of[7], (PAIRS, 2), jnp.float32) ** levels(key_of[7], (PAIRS, 2), ((0, 64),), -0.2, 0.2), -96.0, -12.8)
    sequence_bounds = draw_sequence_bounds(jax.random.fold_in(key_of[9], 71), 0)
    return dict(hidden_in=hidden_in, attention_probs=attention_probs, norm_gain=norm_gain, value_weight=value_weight, output_weight=output_weight, head_grad=head_grad, policy_logprob=policy_logprob, reference_logprob=reference_logprob, sequence_bounds=sequence_bounds)


EPSILON = 1e-06
DPO_BETA = 0.25
LIKELIHOOD_COEF = 0.2

def section_backward(inputs, pattern, gain_vector, value_matrix, output_matrix, upstream):
    group_size = HEADS // KV_HEADS
    input_float = inputs.astype(jnp.float32)
    inverse_rms = lax.rsqrt(lax.optimization_barrier(jnp.mean(input_float * input_float, axis=-1, keepdims=True)) + EPSILON)
    normed = (input_float * inverse_rms * gain_vector).astype(jnp.bfloat16)
    values = jnp.einsum('pcsd,dk->pcsk', normed.astype(jnp.float32), value_matrix.astype(jnp.float32)).astype(jnp.bfloat16)
    grouped = pattern.astype(jnp.float32).reshape(PAIRS, 2, KV_HEADS, group_size, SEQ, SEQ)
    values_heads = values.astype(jnp.float32).reshape(PAIRS, 2, SEQ, KV_HEADS, HEAD_DIM)
    mixed = jnp.einsum('pckgst,pctke->pcskge', grouped, values_heads).astype(jnp.bfloat16)
    mixed = mixed.reshape(PAIRS, 2, SEQ, HEADS * HEAD_DIM)
    upstream_float = upstream.astype(jnp.float32)
    mixed_grad = jnp.einsum('pcsd,hd->pcsh', upstream_float, output_matrix.astype(jnp.float32)).astype(jnp.bfloat16)
    mixed_heads = mixed_grad.astype(jnp.float32).reshape(PAIRS, 2, SEQ, KV_HEADS, group_size, HEAD_DIM)
    values_grad = jnp.einsum('pckgst,pcskge->pctke', grouped, mixed_heads).astype(jnp.bfloat16)
    values_grad = values_grad.reshape(PAIRS, 2, SEQ, KV_HEADS * HEAD_DIM)
    group_columns = KV_HEADS * HEAD_DIM // N_TENSOR
    grad_groups = values_grad.astype(jnp.float32).reshape(PAIRS, 2, SEQ, N_TENSOR, group_columns)
    weight_groups = value_matrix.astype(jnp.float32).reshape(D, N_TENSOR, group_columns)
    normed_grad = jnp.zeros((PAIRS, 2, SEQ, D), jnp.float32)
    for group_index in range(N_TENSOR):
        group_term = jnp.einsum('pcsk,dk->pcsd', grad_groups[:, :, :, group_index, :], weight_groups[:, group_index, :])
        rounded = lax.optimization_barrier(group_term.astype(jnp.bfloat16))
        normed_grad = normed_grad + rounded.astype(jnp.float32)
    gain_total = lax.optimization_barrier(jnp.sum(normed_grad * input_float * inverse_rms, axis=(0, 1, 2)))
    scaled = normed_grad * gain_vector
    cubed = inverse_rms * inverse_rms * inverse_rms
    input_grad = inverse_rms * scaled - input_float * cubed * lax.optimization_barrier(jnp.mean(input_float * scaled, axis=-1, keepdims=True))
    new_rows = (upstream_float + input_grad).astype(jnp.bfloat16)
    mixed_total = jnp.einsum('pcsd,pcsh->dh', upstream_float, mixed.astype(jnp.float32))
    value_total = jnp.einsum('pcsd,pcsk->dk', normed.astype(jnp.float32), values_grad.astype(jnp.float32))
    return (new_rows, value_total, mixed_total, gain_total)

def reference(hidden_in, attention_probs, norm_gain, value_weight, output_weight, head_grad, policy_logprob, reference_logprob, sequence_bounds):
    positions = jnp.arange(SEQ, dtype=jnp.int32)
    response_bool = (positions[None, None, :] >= sequence_bounds[:, 0:1, None]) & (positions[None, None, :] < sequence_bounds[:, 1:3, None])
    response_mask = response_bool.astype(jnp.float32)
    sequence_logprob = lax.optimization_barrier(jnp.sum(response_mask * policy_logprob, axis=-1))
    margin = DPO_BETA * (sequence_logprob[:, 0] - reference_logprob[:, 0] - (sequence_logprob[:, 1] - reference_logprob[:, 1]))
    weight_pair = jax.nn.sigmoid(-margin)
    chosen_total = jnp.sum(response_bool[:, 0, :].astype(jnp.int32))
    likelihood_scale = LIKELIHOOD_COEF * jnp.asarray(PAIRS, jnp.float32) / chosen_total.astype(jnp.float32)
    chosen_weight = -DPO_BETA * weight_pair[:, None] * response_mask[:, 0] - likelihood_scale * response_mask[:, 0]
    rejected_weight = DPO_BETA * weight_pair[:, None] * response_mask[:, 1]
    token_weight = jnp.stack([chosen_weight, rejected_weight], axis=1)
    upstream = (token_weight[..., None] * head_grad.astype(jnp.float32)).astype(jnp.bfloat16)
    cotangents = []
    value_list = []
    output_list = []
    gain_list = []
    for section_index in range(N_PIPE - 1, -1, -1):
        upstream, value_total, mixed_total, gain_total = section_backward(hidden_in[section_index], attention_probs[section_index], norm_gain[section_index], value_weight[section_index], output_weight[section_index], upstream)
        cotangents.insert(0, upstream)
        value_list.insert(0, value_total)
        output_list.insert(0, mixed_total)
        gain_list.insert(0, gain_total)
    return (jnp.stack(cotangents), jnp.stack(value_list), jnp.stack(output_list), jnp.stack(gain_list))
```

```python
import jax
import jax.numpy as jnp
from jax import lax
from jax.sharding import Mesh, PartitionSpec as P

HEAD_DIM = 128
EPSILON = 1e-06
DPO_BETA = 0.25
LIKELIHOOD_COEF = 0.2
NZ, NY, NX, NT = 8, 4, 2, 2
F32, BF16 = jnp.float32, jnp.bfloat16


def paired(block, axis, size, distance, section=None):
    if section is None:
        return lax.ppermute(block, axis, [(i, i ^ distance) for i in range(size)])
    base = section * size
    route = [(base + i, base + (i ^ distance)) for i in range(size)]
    return lax.ppermute(block, ("pipe", axis), route)


def halved(parts, axis, size, distance, bit, section):
    mine = lax.dynamic_index_in_dim(parts, bit, 0, keepdims=False)
    other = lax.dynamic_index_in_dim(parts, 1 - bit, 0, keepdims=False)
    got = paired(other, axis, size, distance, section)
    return mine.astype(F32) + got.astype(F32)


def body(
    hidden_in,
    attention_probs,
    norm_gain,
    value_weight,
    output_weight,
    head_grad,
    policy_logprob,
    reference_logprob,
    sequence_bounds,
):
    section = lax.axis_index("pipe")
    zi, yi, xi, ti = (lax.axis_index(a) for a in ("z", "y", "x", "t"))
    pairs, _, seq, width = hidden_in.shape[1:]
    heads = attention_probs.shape[3]
    tokens = pairs * 2 * seq
    gain = norm_gain[0]
    wv = value_weight[0]
    wo = output_weight[0]
    inputs = hidden_in[0]
    pattern = attention_probs[0]
    own_head = head_grad[:, 0]

    other_head = lax.ppermute(own_head, ("pipe", "t"), [(2, 3), (3, 2)])
    other_wv = lax.ppermute(wv, ("x", "t"), [(0, 3), (3, 0), (1, 2), (2, 1)])

    positions = jnp.arange(seq, dtype=jnp.int32)
    response_bool = (positions[None, None, :] >= sequence_bounds[:, 0:1, None]) & (
        positions[None, None, :] < sequence_bounds[:, 1:3, None]
    )
    count = jnp.sum(response_bool[:, 0, :].astype(jnp.int32)).reshape(1, 1)
    count = jnp.broadcast_to(count, (8, 128))
    for axis, size in (("x", NX), ("y", NY), ("z", NZ)):
        distance = 1
        while distance < size:
            count = count + paired(count, axis, size, distance)
            distance *= 2
    chosen_total = count[0, 0]
    mask = response_bool.astype(F32)
    sequence_logprob = jnp.sum(mask * policy_logprob, axis=-1)
    margin = DPO_BETA * (
        sequence_logprob[:, 0]
        - reference_logprob[:, 0]
        - (sequence_logprob[:, 1] - reference_logprob[:, 1])
    )
    weight_pair = jax.nn.sigmoid(-margin)
    pair_total = pairs * NZ * NY * NX
    scale = LIKELIHOOD_COEF * jnp.asarray(pair_total, F32) / chosen_total.astype(F32)
    chosen_weight = -DPO_BETA * weight_pair[:, None] * mask[:, 0] - scale * mask[:, 0]
    rejected_weight = DPO_BETA * weight_pair[:, None] * mask[:, 1]
    token_weight = jnp.stack([chosen_weight, rejected_weight], axis=1)

    x = inputs.astype(F32)
    inverse_rms = lax.rsqrt(jnp.mean(x * x, axis=-1, keepdims=True) + EPSILON)
    normed = (x * inverse_rms * gain).astype(BF16)
    values = jnp.dot(normed, wv, preferred_element_type=F32).astype(BF16)
    mixed = jnp.einsum("pchqk,pcke->pcqhe", pattern, values, preferred_element_type=F32)
    mixed = mixed.astype(BF16).reshape(tokens, heads * HEAD_DIM)
    normed_flat = normed.reshape(tokens, width)

    def around(block, shift):
        return lax.ppermute(block, "y", [(i, (i + shift) % NY) for i in range(NY)])

    mixed_all = [mixed] + [around(mixed, s) for s in range(1, NY)]

    def by_owner(matrix_t, shift):
        blocks = matrix_t.reshape(NZ, NY, -1, matrix_t.shape[-1])
        rows = lax.dynamic_index_in_dim(blocks, (yi + shift) % NY, 1, keepdims=False)
        return rows.reshape(-1, matrix_t.shape[-1])

    def to_owners(matrix_t, section_id):
        base = section_id * NY
        got = [by_owner(matrix_t, 0)]
        for s in range(1, NY):
            route = [(base + i, base + (i + s) % NY) for i in range(NY)]
            got.append(lax.ppermute(by_owner(matrix_t, s), ("pipe", "y"), route))
        return got

    full_wv = (
        jnp.where(ti == 0, wv, other_wv),
        jnp.where(ti == 0, other_wv, wv),
    )

    def backward(upstream, section_id):
        flat = upstream.reshape(tokens, width)
        dy_blocks = to_owners(flat.T, section_id)
        mixed_grad = lax.dot_general(
            flat, wo, (((1,), (1,)), ((), ())), preferred_element_type=F32
        ).astype(BF16)
        mixed_grad = mixed_grad.reshape(pairs, 2, seq, heads, HEAD_DIM)
        values_grad = jnp.einsum(
            "pchqk,pcqhe->pcke", pattern, mixed_grad, preferred_element_type=F32
        ).astype(BF16)
        route = [(section_id * 2, section_id * 2 + 1), (section_id * 2 + 1, section_id * 2)]
        other_values = lax.ppermute(values_grad, ("pipe", "t"), route)
        grads = (
            jnp.where(ti == 0, values_grad, other_values),
            jnp.where(ti == 0, other_values, values_grad),
        )
        normed_grad = jnp.zeros((), F32)
        for part, weight in zip(grads, full_wv):
            term = jnp.einsum("pcsk,dk->pcsd", part, weight, preferred_element_type=F32)
            normed_grad = normed_grad + term.astype(BF16).astype(F32)
        scaled = normed_grad * gain
        cubed = inverse_rms * inverse_rms * inverse_rms
        input_grad = inverse_rms * scaled - x * cubed * jnp.mean(
            x * scaled, axis=-1, keepdims=True
        )
        new_rows = (upstream.astype(F32) + input_grad).astype(BF16)

        value_part = lax.dot_general(
            normed_flat,
            values_grad.reshape(tokens, HEAD_DIM),
            (((0,), (0,)), ((), ())),
            preferred_element_type=F32,
        ).astype(BF16)
        value_blocks = to_owners(value_part, section_id)
        value_rows = sum(b.astype(F32) for b in value_blocks)
        output_rows = sum(
            jnp.dot(a, b, preferred_element_type=F32) for a, b in zip(dy_blocks, mixed_all)
        )
        return new_rows, value_rows, output_rows

    def finished(rows, section_id):
        n = rows.shape[-1]
        parts = rows.astype(BF16).reshape(NZ, NX, -1, n).transpose(1, 0, 2, 3)
        rows = halved(parts, "x", NX, 1, xi, section_id)
        for distance in (1, 2, 4):
            bit = (zi // distance) % 2
            parts = rows.astype(BF16).reshape(-1, 2, rows.shape[-2], n)
            rows = halved(parts.transpose(1, 0, 2, 3), "z", NZ, distance, bit, section_id)
        return rows.reshape(-1, n)

    cut = 384
    top = jnp.where(
        ti == 0, jnp.stack([own_head, other_head], 1), jnp.stack([other_head, own_head], 1)
    )
    upstream = (token_weight[..., None] * top.astype(F32)).astype(BF16)

    def reduced(value_rows, output_rows, section_id):
        first = finished(jnp.concatenate([value_rows, output_rows[:, :cut]], 1), section_id)
        second = finished(output_rows[:, cut:], section_id)
        return first, second

    rows_1, value_1, output_1 = backward(upstream, 1)
    incoming = lax.ppermute(rows_1, "pipe", [(1, 0)])
    rows_0, value_0, output_0 = backward(incoming, 0)
    first_1, second_1 = reduced(value_1, output_1, 1)
    first_0, second_0 = reduced(value_0, output_0, 0)

    upper = section == 1
    first = jnp.where(upper, first_1, first_0)
    second = jnp.where(upper, second_1, second_0)
    own_rows_1 = lax.dynamic_index_in_dim(rows_1, ti, 1, keepdims=True)
    own_rows_0 = lax.dynamic_index_in_dim(rows_0, ti, 1, keepdims=True)
    own_rows = jnp.where(upper, own_rows_1, own_rows_0)

    value_share = first[:, :HEAD_DIM]
    output_share = jnp.concatenate([first[:, HEAD_DIM:], second], 1)
    start = ((zi * NY + yi) * NX + xi) * value_share.shape[0]
    own_wv = lax.dynamic_slice_in_dim(wv, start, value_share.shape[0], 0).astype(F32)
    own_gain = lax.dynamic_slice_in_dim(gain, start, value_share.shape[0], 0)
    gain_part = jnp.sum(own_wv * value_share, axis=1) / own_gain
    gain_rows = gain_part + paired(gain_part, "t", NT, 1)
    return own_rows[None], value_share[None], output_share[None], gain_rows[None]


def solution(mesh):
    fine = Mesh(
        mesh.devices.reshape(2, NZ, NY, NX, NT), ("pipe", "z", "y", "x", "t")
    )
    dp = ("z", "y", "x")
    in_specs = (
        P("pipe", dp, None, None, None),
        P("pipe", dp, None, "t", None, None),
        P("pipe", None),
        P("pipe", None, "t"),
        P("pipe", "t", None),
        P(dp, "t", None, None),
        P(dp, None, None),
        P(dp, None),
        P(dp, None),
    )
    out_specs = (
        P("pipe", dp, "t", None, None),
        P("pipe", dp, "t"),
        P("pipe", dp, "t"),
        P("pipe", dp),
    )
    return jax.shard_map(body, mesh=fine, in_specs=in_specs, out_specs=out_specs, check_vma=False)
```

```python
import jax
import jax.numpy as jnp
from jax import lax
from jax.experimental import pallas as pl
from jax.experimental.pallas import tpu as pltpu
from jax.sharding import Mesh, PartitionSpec as P

HEAD_DIM = 128
EPSILON = 1e-06
DPO_BETA = 0.25
LIKELIHOOD_COEF = 0.2
NZ, NY, NX, NT = 8, 4, 2, 2
F32, BF16 = jnp.float32, jnp.bfloat16


def paired(block, axis, size, distance, section=None):
    if section is None:
        return lax.ppermute(block, axis, [(i, i ^ distance) for i in range(size)])
    base = section * size
    route = [(base + i, base + (i ^ distance)) for i in range(size)]
    return lax.ppermute(block, ("pipe", axis), route)


def four_way(parts, own, send):
    total = lax.dynamic_index_in_dim(parts, own, 0, keepdims=False).astype(F32)
    got = [
        send(lax.dynamic_index_in_dim(parts, own ^ k, 0, keepdims=False), k) for k in (1, 2, 3)
    ]
    for block in got:
        total = total + block.astype(F32)
    return total


def over_xz(block, k, section):
    base = section * NZ * NX
    route = [
        (base + z * NX + x, base + (z ^ (k >> 1)) * NX + (x ^ (k & 1)))
        for z in range(NZ)
        for x in range(NX)
    ]
    return lax.ppermute(block, ("pipe", "z", "x"), route)


VMEM = pl.BlockSpec(memory_space=pltpu.VMEM)
SMEM = pl.BlockSpec(memory_space=pltpu.SMEM)


def dot(a, b, contract):
    return lax.dot_general(a, b, (contract, ((), ())), preferred_element_type=F32)


def rms_of(x):
    return lax.rsqrt(jnp.mean(x * x, axis=-1, keepdims=True) + EPSILON)


def forward_kernel(x_ref, gain_ref, wv_ref, pattern_ref, normed_ref, mixed_ref):
    rows = 2 * pattern_ref.shape[2]
    heads, seq = pattern_ref.shape[1:3]
    for start in range(0, x_ref.shape[0], rows):
        x = x_ref[start : start + rows].astype(F32)
        normed = (x * rms_of(x) * gain_ref[...]).astype(BF16)
        normed_ref[start : start + rows] = normed
        values = dot(normed, wv_ref[...], ((1,), (0,))).astype(BF16)
        for part in range(2):
            pattern = pattern_ref[start // seq + part].reshape(heads * seq, seq)
            mixed = dot(pattern, values[part * seq : (part + 1) * seq], ((1,), (0,))).astype(BF16)
            for h in range(heads):
                mixed_ref[
                    start + part * seq : start + (part + 1) * seq, h * HEAD_DIM : (h + 1) * HEAD_DIM
                ] = mixed[h * seq : (h + 1) * seq]


def values_kernel(active_ref, dy_ref, wo_ref, pattern_ref, values_ref):
    @pl.when(active_ref[0] == 1)
    def _():
        sequences, heads, seq, _ = pattern_ref.shape
        mixed = dot(dy_ref[...], wo_ref[...], ((1,), (1,))).astype(BF16)
        for n in range(sequences):
            stacked = jnp.concatenate(
                [
                    mixed[n * seq : (n + 1) * seq, h * HEAD_DIM : (h + 1) * HEAD_DIM]
                    for h in range(heads)
                ],
                axis=0,
            )
            pattern = pattern_ref[n].reshape(heads * seq, seq)
            values_ref[n * seq : (n + 1) * seq] = dot(pattern, stacked, ((0,), (0,))).astype(BF16)


def rows_kernel(
    active_ref, own_ref, other_ref, own_wv_ref, other_wv_ref, x_ref, gain_ref, raw_ref, weight_ref,
    rows_ref, dy_ref, values_ref,
):
    @pl.when(active_ref[0] == 1)
    def _():
        rows = 64
        for start in range(0, x_ref.shape[0], rows):
            at = slice(start, start + rows)
            weight = weight_ref[at]
            own = (weight * own_ref[at].astype(F32)).astype(BF16)
            other = (weight * other_ref[at].astype(F32)).astype(BF16)
            values_ref[at] = own
            first = dot(own, own_wv_ref[...], ((1,), (1,))).astype(BF16)
            second = dot(other, other_wv_ref[...], ((1,), (1,))).astype(BF16)
            scaled = (first.astype(F32) + second.astype(F32)) * gain_ref[...]
            x = x_ref[at].astype(F32)
            inverse = rms_of(x)
            input_grad = inverse * scaled - x * (inverse * inverse * inverse) * jnp.mean(
                x * scaled, axis=-1, keepdims=True
            )
            dy = (weight * raw_ref[at].astype(F32)).astype(BF16)
            dy_ref[at] = dy
            rows_ref[at] = (dy.astype(F32) + input_grad).astype(BF16)


def owners_kernel(active_ref, y_ref, dy_ref, *refs):
    out_refs, turned_ref = refs[:-1], refs[-1]

    @pl.when(active_ref[0] == 1)
    def _():
        turned_ref[...] = dy_ref[...].T
        size = out_refs[0].shape[0] // NZ
        for s, out_ref in enumerate(out_refs):
            owner = (y_ref[0] + s) % NY
            for z in range(NZ):
                start = pl.multiple_of((z * NY + owner) * size, 16)
                out_ref[z * size : (z + 1) * size] = turned_ref[pl.ds(start, size)]


def shaped(*dims):
    return jax.ShapeDtypeStruct(dims, BF16)


def after(block, *others):
    return lax.optimization_barrier((block, *others))[0]


def body(
    hidden_in,
    attention_probs,
    norm_gain,
    value_weight,
    output_weight,
    head_grad,
    policy_logprob,
    reference_logprob,
    sequence_bounds,
):
    section = lax.axis_index("pipe")
    zi, yi, xi, ti = (lax.axis_index(a) for a in ("z", "y", "x", "t"))
    pairs, _, seq, width = hidden_in.shape[1:]
    heads = attention_probs.shape[3]
    tokens = pairs * 2 * seq
    gain = norm_gain[0]
    wv = value_weight[0]
    wo = output_weight[0]
    inputs = hidden_in[0]
    pattern = attention_probs[0]
    own_head = head_grad[:, 0]

    other_head = lax.ppermute(own_head, ("pipe", "t"), [(2, 3), (3, 2)])

    positions = jnp.arange(seq, dtype=jnp.int32)
    response_bool = (positions[None, None, :] >= sequence_bounds[:, 0:1, None]) & (
        positions[None, None, :] < sequence_bounds[:, 1:3, None]
    )
    count = jnp.sum(response_bool[:, 0, :].astype(jnp.int32)).reshape(1, 1)
    count = jnp.broadcast_to(count, (8, 128))
    for axis, size in (("x", NX), ("y", NY), ("z", NZ)):
        distance = 1
        while distance < size:
            count = count + paired(count, axis, size, distance, 0)
            distance *= 2
    chosen_total = lax.ppermute(count, "pipe", [(0, 1)])[0, 0]
    mask = response_bool.astype(F32)
    sequence_logprob = jnp.sum(mask * policy_logprob, axis=-1)
    margin = DPO_BETA * (
        sequence_logprob[:, 0]
        - reference_logprob[:, 0]
        - (sequence_logprob[:, 1] - reference_logprob[:, 1])
    )
    weight_pair = jax.nn.sigmoid(-margin)
    pair_total = pairs * NZ * NY * NX
    scale = LIKELIHOOD_COEF * jnp.asarray(pair_total, F32) / chosen_total.astype(F32)
    sequence_weight = jnp.stack(
        [-DPO_BETA * weight_pair - scale, DPO_BETA * weight_pair], axis=1
    )[:, :, None, None]

    def across(block, section_id):
        pairs_xt = ((0, 3), (3, 0), (1, 2), (2, 1))
        base = section_id * 4
        return lax.ppermute(block, ("pipe", "x", "t"), [(base + a, base + b) for a, b in pairs_xt])

    other_wv_1 = across(after(wv, other_head), 1)

    x = inputs.reshape(tokens, width)
    patterns = pattern.reshape(pairs * 2, heads, seq, seq)
    normed, mixed = pl.pallas_call(
        forward_kernel,
        out_shape=(shaped(tokens, width), shaped(tokens, heads * HEAD_DIM)),
        in_specs=[VMEM] * 4,
        out_specs=(VMEM, VMEM),
    )(x, norm_gain, wv, patterns)

    def around(block, shift):
        return lax.ppermute(block, "y", [(i, (i + shift) % NY) for i in range(NY)])

    mixed_all = [mixed] + [around(mixed, s) for s in range(1, NY)]

    def by_owner(matrix_t, shift):
        blocks = matrix_t.reshape(NZ, NY, -1, matrix_t.shape[-1])
        rows = lax.dynamic_index_in_dim(blocks, (yi + shift) % NY, 1, keepdims=False)
        return rows.reshape(-1, matrix_t.shape[-1])

    def values_of(active, dy):
        return pl.pallas_call(
            values_kernel,
            out_shape=shaped(tokens, HEAD_DIM),
            in_specs=[SMEM] + [VMEM] * 3,
            out_specs=VMEM,
        )(active, dy, wo, patterns)

    def rows_of(active, own, other, other_wv, raw, weight):
        return pl.pallas_call(
            rows_kernel,
            out_shape=(shaped(tokens, width), shaped(tokens, width), shaped(tokens, HEAD_DIM)),
            in_specs=[SMEM] + [VMEM] * 8,
            out_specs=(VMEM, VMEM, VMEM),
        )(active, own, other, wv, other_wv, x, norm_gain, raw, weight)

    def owners_of(active, dy):
        return pl.pallas_call(
            owners_kernel,
            out_shape=(shaped(width // NY, tokens),) * NY,
            in_specs=[SMEM, SMEM, VMEM],
            out_specs=(VMEM,) * NY,
            scratch_shapes=[pltpu.VMEM((width, tokens), BF16)],
        )(active, yi.astype(jnp.int32).reshape(1), dy)

    def swapped(values, section_id):
        route = [(section_id * 2, section_id * 2 + 1), (section_id * 2 + 1, section_id * 2)]
        return lax.ppermute(values, ("pipe", "t"), route)

    def sent(blocks, section_id):
        base = section_id * NY
        got = [blocks[0]]
        for s in range(1, NY):
            route = [(base + i, base + (i + s) % NY) for i in range(NY)]
            got.append(lax.ppermute(blocks[s], ("pipe", "y"), route))
        return got

    def value_blocks(values, section_id):
        part = dot(normed, values, ((0,), (0,))).astype(BF16)
        return sent([by_owner(part, s) for s in range(NY)], section_id)

    def products(dy_blocks, value_parts):
        value_rows = sum(b.astype(F32) for b in value_parts)
        output_rows = sum(dot(a, b, ((1,), (0,))) for a, b in zip(dy_blocks, mixed_all))
        return value_rows, output_rows

    def finished(value_rows, output_rows, section_id):
        rows = jnp.concatenate([value_rows, output_rows], 1).astype(BF16)
        n = rows.shape[-1]
        parts = rows.reshape(4, 2, NX, -1, n).transpose(1, 2, 0, 3, 4).reshape(4, 4, -1, n)
        own = (zi % 2) * NX + xi
        rows = four_way(parts, own, lambda block, k: over_xz(block, k, section_id))
        parts = rows.astype(BF16)
        return four_way(parts, zi // 2, lambda block, k: over_xz(block, k << 2, section_id))

    upper = section == 1
    is_upper = upper.astype(jnp.int32).reshape(1)
    is_lower = 1 - is_upper
    other_wv_0 = across(after(wv, count, mixed), 0)

    top = jnp.where(
        ti == 0, jnp.stack([own_head, other_head], 1), jnp.stack([other_head, own_head], 1)
    )
    raw = jnp.where(response_bool[..., None], top, jnp.zeros((), BF16)).reshape(tokens, width)
    raw = after(raw, mixed)

    own_1 = values_of(is_upper, raw)
    other_1 = swapped(own_1, 1)
    weight = jnp.broadcast_to(sequence_weight, (pairs, 2, seq, 1)).reshape(tokens, 1)
    rows_1, dy_1, values_1 = rows_of(is_upper, own_1, other_1, other_wv_1, raw, weight)
    incoming = lax.ppermute(rows_1, "pipe", [(1, 0)])
    dy_blocks_1 = sent(owners_of(is_upper, dy_1), 1)
    value_parts_1 = value_blocks(values_1, 1)

    blocks_0 = owners_of(is_lower, incoming)
    dy_blocks_0 = sent(blocks_0, 0)
    own_0 = values_of(is_lower, after(incoming, *blocks_0))
    other_0 = swapped(own_0, 0)
    value_parts_0 = value_blocks(own_0, 0)
    rows_0, _, _ = rows_of(
        is_lower, own_0, other_0, other_wv_0, incoming, jnp.ones((tokens, 1), F32)
    )
    share_1 = finished(*products(dy_blocks_1, value_parts_1), 1)
    share_0 = finished(*products(dy_blocks_0, value_parts_0), 0)

    share = jnp.where(upper, share_1, share_0)
    own_rows = jnp.where(
        upper,
        *(
            lax.dynamic_index_in_dim(r.reshape(pairs, 2, seq, width), ti, 1, keepdims=True)
            for r in (rows_1, rows_0)
        ),
    )

    value_share = share[:, :HEAD_DIM]
    output_share = share[:, HEAD_DIM:]
    start = ((zi * NY + yi) * NX + xi) * value_share.shape[0]
    own_wv = lax.dynamic_slice_in_dim(wv, start, value_share.shape[0], 0).astype(F32)
    own_gain = lax.dynamic_slice_in_dim(gain, start, value_share.shape[0], 0)
    gain_part = jnp.sum(own_wv * value_share, axis=1) / own_gain
    gain_rows = gain_part + paired(gain_part, "t", NT, 1)
    return own_rows[None], value_share[None], output_share[None], gain_rows[None]


def solution(mesh):
    fine = Mesh(
        mesh.devices.reshape(2, NZ, NY, NX, NT), ("pipe", "z", "y", "x", "t")
    )
    dp = ("z", "y", "x")
    in_specs = (
        P("pipe", dp, None, None, None),
        P("pipe", dp, None, "t", None, None),
        P("pipe", None),
        P("pipe", None, "t"),
        P("pipe", "t", None),
        P(dp, "t", None, None),
        P(dp, None, None),
        P(dp, None),
        P(dp, None),
    )
    out_specs = (
        P("pipe", dp, "t", None, None),
        P("pipe", dp, "t"),
        P("pipe", dp, "t"),
        P("pipe", dp),
    )
    return jax.shard_map(body, mesh=fine, in_specs=in_specs, out_specs=out_specs, check_vma=False)
```

```python
import jax
import jax.numpy as jnp
from jax import lax
from jax.experimental import pallas as pl
from jax.experimental.pallas import tpu as pltpu
from jax.sharding import Mesh, PartitionSpec as P


HEAD_DIM = 128
EPSILON = 1e-06
DPO_BETA = 0.25
LIKELIHOOD_COEF = 0.2
NZ, NY, NX, NT = 8, 4, 2, 2
F32, BF16 = jnp.float32, jnp.bfloat16


def paired(block, axis, size, distance, section=None):
    if section is None:
        return lax.ppermute(block, axis, [(i, i ^ distance) for i in range(size)])
    base = section * size
    route = [(base + i, base + (i ^ distance)) for i in range(size)]
    return lax.ppermute(block, ("pipe", axis), route)


def over_xz(block, k):
    route = [
        (z * NX + x, (z ^ (k >> 1)) * NX + (x ^ (k & 1))) for z in range(NZ) for x in range(NX)
    ]
    return lax.ppermute(block, ("z", "x"), route)


VMEM = pl.BlockSpec(memory_space=pltpu.VMEM)
SMEM = pl.BlockSpec(memory_space=pltpu.SMEM)


def dot(a, b, contract):
    return lax.dot_general(a, b, (contract, ((), ())), preferred_element_type=F32)


def rms_of(x):
    return lax.rsqrt(jnp.mean(x * x, axis=-1, keepdims=True) + EPSILON)


def forward_kernel(x_ref, gain_ref, wv_ref, pattern_ref, normed_ref, mixed_ref):
    rows = 2 * pattern_ref.shape[2]
    heads, seq = pattern_ref.shape[1:3]
    for start in range(0, x_ref.shape[0], rows):
        x = x_ref[start : start + rows].astype(F32)
        normed = (x * rms_of(x) * gain_ref[...]).astype(BF16)
        normed_ref[start : start + rows] = normed
        values = dot(normed, wv_ref[...], ((1,), (0,))).astype(BF16)
        for part in range(2):
            pattern = pattern_ref[start // seq + part].reshape(heads * seq, seq)
            mixed = dot(pattern, values[part * seq : (part + 1) * seq], ((1,), (0,))).astype(BF16)
            for h in range(heads):
                mixed_ref[
                    start + part * seq : start + (part + 1) * seq, h * HEAD_DIM : (h + 1) * HEAD_DIM
                ] = mixed[h * seq : (h + 1) * seq]


def values_kernel(active_ref, dy_ref, wo_ref, pattern_ref, values_ref, mixed_ref):
    step = pl.program_id(0)

    @pl.when(active_ref[0] == 1)
    def _():
        part = dot(dy_ref[...], wo_ref[...], ((1,), (1,)))

        @pl.when(step == 0)
        def _():
            mixed_ref[...] = part

        @pl.when(step > 0)
        def _():
            mixed_ref[...] += part

        @pl.when(step == pl.num_programs(0) - 1)
        def _():
            sequences, heads, seq, _ = pattern_ref.shape
            for n in range(sequences):
                stacked = jnp.concatenate(
                    [
                        mixed_ref[
                            n * seq : (n + 1) * seq, h * HEAD_DIM : (h + 1) * HEAD_DIM
                        ].astype(BF16)
                        for h in range(heads)
                    ],
                    axis=0,
                )
                pattern = pattern_ref[n].reshape(heads * seq, seq)
                values = dot(pattern, stacked, ((0,), (0,))).astype(BF16)
                values_ref[n * seq : (n + 1) * seq] = values


def rows_kernel(
    active_ref, tensor_ref, own_ref, other_ref, own_wv_ref, other_wv_ref, x_ref, gain_ref, dy_ref,
    rows_ref,
):
    @pl.when(active_ref[0] == 1)
    def _():
        first = dot(own_ref[...], own_wv_ref[...], ((1,), (1,))).astype(BF16)
        second = dot(other_ref[...], other_wv_ref[...], ((1,), (1,))).astype(BF16)
        scaled = (first.astype(F32) + second.astype(F32)) * gain_ref[...]
        x = x_ref[...].astype(F32)
        inverse = rms_of(x)
        pull = (inverse * inverse * inverse) * jnp.mean(x * scaled, axis=-1, keepdims=True)
        rows_ref[...] = (dy_ref[...].astype(F32) + (inverse * scaled - x * pull)).astype(BF16)


def owners_kernel(active_ref, y_ref, dy_ref, weight_ref, values_ref, normed_ref, *refs):
    out_refs, turned_ref = refs[:-1], refs[-1]

    @pl.when(active_ref[0] == 1)
    def _():
        tokens, width = dy_ref.shape
        weight = weight_ref[...]
        values = (weight * values_ref[...].astype(F32)).astype(BF16)
        for start in range(0, width, 512):
            at = slice(start, start + 512)
            dy = (weight * dy_ref[:, at].astype(F32)).astype(BF16)
            turned_ref[at, :tokens] = dy.T
            turned_ref[at, tokens:] = dot(normed_ref[:, at], values, ((0,), (0,))).astype(BF16)
        size = out_refs[0].shape[0] // NZ
        for s, out_ref in enumerate(out_refs):
            owner = (y_ref[0] + s) % NY
            for z in range(NZ):
                start = pl.multiple_of((z * NY + owner) * size, 16)
                out_ref[z * size : (z + 1) * size] = turned_ref[pl.ds(start, size)]


def products_kernel(upper_ref, own_ref, *refs):
    upper_blocks, lower_blocks, mixed_refs = refs[:NY], refs[NY : 2 * NY], refs[2 * NY : 3 * NY]
    out_refs, total_ref = refs[3 * NY : -1], refs[-1]
    tokens = mixed_refs[0].shape[0]

    def add_up(blocks):
        total_ref[:, :HEAD_DIM] = sum(b[:, tokens:].astype(F32) for b in blocks)
        total_ref[:, HEAD_DIM:] = sum(
            dot(b[:, :tokens], m[...], ((1,), (0,))) for b, m in zip(blocks, mixed_refs)
        )

    @pl.when(upper_ref[0] == 1)
    def _():
        add_up(upper_blocks)

    @pl.when(upper_ref[0] == 0)
    def _():
        add_up(lower_blocks)

    size = out_refs[0].shape[1]
    for k, out_ref in enumerate(out_refs):
        start = pl.multiple_of((own_ref[0] ^ k) * size, 8)
        out_ref[0] = total_ref[pl.ds(start, size)].astype(BF16)


def stage_kernel(own_ref, a_ref, b_ref, c_ref, d_ref, *out_refs):
    for k, out_ref in enumerate(out_refs):
        j = own_ref[0] ^ k
        total = sum(r[j].astype(F32) for r in (a_ref, b_ref, c_ref, d_ref))
        out_ref[...] = total.astype(out_ref.dtype)


def last_kernel(a_ref, b_ref, c_ref, d_ref, wv_ref, gain_ref, value_ref, output_ref, part_ref):
    total = a_ref[...] + sum(r[...].astype(F32) for r in (b_ref, c_ref, d_ref))
    value = total[:, :HEAD_DIM]
    value_ref[0] = value
    output_ref[0] = total[:, HEAD_DIM:]
    part_ref[...] = jnp.sum(wv_ref[...] * value, axis=1, keepdims=True) / gain_ref[...]


def shaped(*dims):
    return jax.ShapeDtypeStruct(dims, BF16)


def after(block, *others):
    return lax.optimization_barrier((block, *others))[0]


def section_step(
    hidden_in,
    attention_probs,
    norm_gain,
    value_weight,
    output_weight,
    head_grad,
    policy_logprob,
    reference_logprob,
    sequence_bounds,
):
    section = lax.axis_index("pipe")
    zi, yi, xi, ti = (lax.axis_index(a) for a in ("z", "y", "x", "t"))
    pairs, _, seq, width = hidden_in.shape[1:]
    heads = attention_probs.shape[3]
    tokens = pairs * 2 * seq
    gain = norm_gain[0]
    wv = value_weight[0]
    wo = output_weight[0]
    inputs = hidden_in[0]
    pattern = attention_probs[0]
    own_head = head_grad[:, 0]

    other_head = lax.ppermute(own_head, ("pipe", "t"), [(2, 3), (3, 2)])

    positions = jnp.arange(seq, dtype=jnp.int32)
    response_bool = (positions[None, None, :] >= sequence_bounds[:, 0:1, None]) & (
        positions[None, None, :] < sequence_bounds[:, 1:3, None]
    )
    ends = jnp.clip(sequence_bounds[:, :2], 0, seq)
    count = jnp.sum(jnp.maximum(ends[:, 1] - ends[:, 0], 0)).reshape(1, 1)
    count = lax.optimization_barrier(jnp.broadcast_to(count, (8, 128)))
    steps = (("y", NY, 1), ("y", NY, 2), ("x", NX, 1), ("z", NZ, 1), ("z", NZ, 2), ("z", NZ, 4))
    for axis, size, distance in steps:
        got = paired(count, axis, size, distance, 0)
        count = count + got
    mask = response_bool.astype(F32)
    sequence_logprob = jnp.sum(mask * policy_logprob, axis=-1)
    margin = DPO_BETA * (
        sequence_logprob[:, 0]
        - reference_logprob[:, 0]
        - (sequence_logprob[:, 1] - reference_logprob[:, 1])
    )
    weight_pair = jax.nn.sigmoid(-margin)

    def across(block, section_id):
        pairs_xt = ((0, 3), (3, 0), (1, 2), (2, 1))
        base = section_id * 4
        route = [(base + a, base + b) for a, b in pairs_xt]
        return lax.ppermute(block, ("pipe", "x", "t"), route)

    other_wv_1 = across(after(wv, other_head), 1)

    x = inputs.reshape(tokens, width)
    patterns = pattern.reshape(pairs * 2, heads, seq, seq)
    normed, mixed = pl.pallas_call(
        forward_kernel,
        out_shape=(shaped(tokens, width), shaped(tokens, heads * HEAD_DIM)),
        in_specs=[VMEM] * 4,
        out_specs=(VMEM, VMEM),
    )(x, norm_gain, wv, patterns)

    def around(block, shift):
        return lax.ppermute(block, "y", [(i, (i + shift) % NY) for i in range(NY)])

    mixed_all = [mixed] + [around(mixed, s) for s in range(1, NY)]

    def values_of(active, dy):
        block = 512
        return pl.pallas_call(
            values_kernel,
            out_shape=shaped(tokens, HEAD_DIM),
            grid_spec=pltpu.PrefetchScalarGridSpec(
                num_scalar_prefetch=1,
                grid=(width // block,),
                in_specs=[
                    pl.BlockSpec((tokens, block), lambda i, on: (0, i * on[0])),
                    pl.BlockSpec((heads * HEAD_DIM, block), lambda i, on: (0, i * on[0])),
                    pl.BlockSpec((pairs * 2, heads, seq, seq), lambda i, on: (0, 0, 0, 0)),
                ],
                out_specs=pl.BlockSpec((tokens, HEAD_DIM), lambda i, on: (0, 0)),
                scratch_shapes=[pltpu.VMEM((tokens, heads * HEAD_DIM), F32)],
            ),
        )(active, dy, wo, patterns)

    def rows_of(active, own, other, other_wv, dy, own_only):
        count = pairs if own_only else pairs * 2

        def pick(n, on, t):
            return ((n * 2 + t[0] if own_only else n) * on[0], 0)

        def whole(n, on, t):
            return (0, 0)

        return pl.pallas_call(
            rows_kernel,
            out_shape=shaped(count * seq, width),
            grid_spec=pltpu.PrefetchScalarGridSpec(
                num_scalar_prefetch=2,
                grid=(count,),
                in_specs=[
                    pl.BlockSpec((seq, HEAD_DIM), pick),
                    pl.BlockSpec((seq, HEAD_DIM), pick),
                    pl.BlockSpec((width, HEAD_DIM), whole),
                    pl.BlockSpec((width, HEAD_DIM), whole),
                    pl.BlockSpec((seq, width), pick),
                    pl.BlockSpec((1, width), whole),
                    pl.BlockSpec((seq, width), pick),
                ],
                out_specs=pl.BlockSpec((seq, width), lambda n, on, t: (n, 0)),
            ),
        )(active, ti.astype(jnp.int32).reshape(1), own, other, wv, other_wv, x, norm_gain, dy)

    def owners_of(active, dy, weight, values):
        return pl.pallas_call(
            owners_kernel,
            out_shape=(shaped(width // NY, tokens + HEAD_DIM),) * NY,
            in_specs=[SMEM, SMEM] + [VMEM] * 4,
            out_specs=(VMEM,) * NY,
            scratch_shapes=[pltpu.VMEM((width, tokens + HEAD_DIM), BF16)],
        )(active, yi.astype(jnp.int32).reshape(1), dy, weight, values, normed)

    def swapped(values, section_id):
        route = [(section_id * 2, section_id * 2 + 1), (section_id * 2 + 1, section_id * 2)]
        return lax.ppermute(values, ("pipe", "t"), route)

    def sent(blocks, section_id):
        base = section_id * NY
        got = [blocks[0]]
        for s in range(1, NY):
            route = [(base + i, base + (i + s) % NY) for i in range(NY)]
            got.append(lax.ppermute(blocks[s], ("pipe", "y"), route))
        return got

    upper = section == 1
    is_upper = upper.astype(jnp.int32).reshape(1)
    is_lower = 1 - is_upper
    columns = HEAD_DIM * (heads + 1)
    share_rows = width // (NZ * NY * NX)

    top = jnp.where(
        ti == 0, jnp.stack([own_head, other_head], 1), jnp.stack([other_head, own_head], 1)
    )
    raw = jnp.where(response_bool[..., None], top, jnp.zeros((), BF16)).reshape(tokens, width)
    raw = after(raw, mixed)
    own_1 = values_of(is_upper, raw)
    other_1 = swapped(own_1, 1)
    rows_1 = rows_of(is_upper, own_1, other_1, other_wv_1, raw, False)
    incoming = lax.ppermute(rows_1, "pipe", [(1, 0)])

    count = after(count, rows_1)
    count_up = lax.ppermute(count, "pipe", [(0, 1)])
    chosen_total = jnp.where(upper, count_up, count)[0, 0]
    pair_total = pairs * NZ * NY * NX
    scale = LIKELIHOOD_COEF * jnp.asarray(pair_total, F32) / chosen_total.astype(F32)
    weights = jnp.stack([-DPO_BETA * weight_pair - scale, DPO_BETA * weight_pair], axis=1)
    weight = jnp.broadcast_to(weights[:, :, None], (pairs, 2, seq)).reshape(tokens, 1)

    turned_1 = owners_of(is_upper, raw, weight, own_1)
    blocks_1 = sent(turned_1, 1)

    other_wv_0 = across(after(wv, count, mixed), 0)
    own_0 = values_of(is_lower, incoming)
    other_0 = swapped(own_0, 0)
    turned_0 = owners_of(is_lower, incoming, weight, own_0)
    blocks_0 = sent(turned_0, 0)

    first_own = ((zi % 2) * NX + xi).astype(jnp.int32).reshape(1)
    group = width // NY // 4

    def rows_if(wanted):
        return pl.BlockSpec(
            (group, tokens + HEAD_DIM),
            lambda i, on, own: ((i * on[0] if wanted else i * (1 - on[0])), 0),
        )

    parts = pl.pallas_call(
        products_kernel,
        out_shape=(shaped(4, share_rows, columns),) * 4,
        grid_spec=pltpu.PrefetchScalarGridSpec(
            num_scalar_prefetch=2,
            grid=(4,),
            in_specs=[rows_if(True)] * NY
            + [rows_if(False)] * NY
            + [pl.BlockSpec((tokens, heads * HEAD_DIM), lambda i, on, own: (0, 0))] * NY,
            out_specs=(pl.BlockSpec((1, share_rows, columns), lambda i, on, own: (i, 0, 0)),) * 4,
            scratch_shapes=[pltpu.VMEM((group, columns), F32)],
        ),
    )(is_upper, first_own, *blocks_1, *after(tuple(blocks_0), other_0), *mixed_all)
    got = [parts[0]] + [over_xz(parts[k], k) for k in (1, 2, 3)]
    parts = pl.pallas_call(
        stage_kernel,
        out_shape=(jax.ShapeDtypeStruct((share_rows, columns), F32),)
        + (shaped(share_rows, columns),) * 3,
        in_specs=[SMEM] + [VMEM] * 4,
        out_specs=(VMEM,) * 4,
    )((zi // 2).astype(jnp.int32).reshape(1), *got)
    got = [parts[0]] + [over_xz(parts[k], k << 2) for k in (1, 2, 3)]

    rows_0 = rows_of(is_lower, own_0, other_0, other_wv_0, incoming, True)
    own_1_rows = lax.dynamic_index_in_dim(rows_1.reshape(pairs, 2, seq, width), ti, 1, False)
    own_rows = jnp.where(upper, own_1_rows, rows_0.reshape(pairs, seq, width)).astype(F32)
    own_weight = lax.dynamic_index_in_dim(weights, ti, 1, False)[:, None, None]
    own_rows = (own_weight * own_rows).astype(BF16)[:, None]

    start = ((zi * NY + yi) * NX + xi) * share_rows
    own_wv = lax.dynamic_slice_in_dim(wv, start, share_rows, 0).astype(F32)
    own_gain = lax.dynamic_slice_in_dim(gain, start, share_rows, 0).reshape(share_rows, 1)
    value_share, output_share, gain_part = pl.pallas_call(
        last_kernel,
        out_shape=(
            jax.ShapeDtypeStruct((1, share_rows, HEAD_DIM), F32),
            jax.ShapeDtypeStruct((1, share_rows, columns - HEAD_DIM), F32),
            jax.ShapeDtypeStruct((share_rows, 1), F32),
        ),
        in_specs=[VMEM] * 6,
        out_specs=(VMEM,) * 3,
    )(*got, own_wv, own_gain)
    gain_part = gain_part.reshape(1, share_rows)
    gain_rows = gain_part + paired(gain_part, "t", NT, 1)
    return own_rows[None], value_share, output_share, gain_rows


def solution(mesh):
    fine = Mesh(
        mesh.devices.reshape(2, NZ, NY, NX, NT), ("pipe", "z", "y", "x", "t")
    )
    dp = ("z", "y", "x")
    in_specs = (
        P("pipe", dp, None, None, None),
        P("pipe", dp, None, "t", None, None),
        P("pipe", None),
        P("pipe", None, "t"),
        P("pipe", "t", None),
        P(dp, "t", None, None),
        P(dp, None, None),
        P(dp, None),
        P(dp, None),
    )
    out_specs = (
        P("pipe", dp, "t", None, None),
        P("pipe", dp, "t"),
        P("pipe", dp, "t"),
        P("pipe", dp),
    )
    return jax.shard_map(section_step, mesh=fine, in_specs=in_specs, out_specs=out_specs, check_vma=False)
```

```python
import jax
import jax.numpy as jnp
from jax import lax
from jax.experimental import pallas as pl
from jax.experimental.pallas import tpu as pltpu
from jax.sharding import Mesh, PartitionSpec as P


HEAD_DIM = 128
EPSILON = 1e-06
DPO_BETA = 0.25
LIKELIHOOD_COEF = 0.2
NZ, NY, NX, NT = 8, 4, 2, 2
F32, BF16 = jnp.float32, jnp.bfloat16


def paired(block, axis, size, distance, section=None):
    if section is None:
        return lax.ppermute(block, axis, [(i, i ^ distance) for i in range(size)])
    base = section * size
    route = [(base + i, base + (i ^ distance)) for i in range(size)]
    return lax.ppermute(block, ("pipe", axis), route)


def over_xz(block, k):
    route = [
        (z * NX + x, (z ^ (k >> 1)) * NX + (x ^ (k & 1))) for z in range(NZ) for x in range(NX)
    ]
    return lax.ppermute(block, ("z", "x"), route)


VMEM = pl.BlockSpec(memory_space=pltpu.VMEM)
SMEM = pl.BlockSpec(memory_space=pltpu.SMEM)
ANY = pl.BlockSpec(memory_space=pl.ANY)


def dot(a, b, contract):
    return lax.dot_general(a, b, (contract, ((), ())), preferred_element_type=F32)


def rms_of(x):
    return lax.rsqrt(jnp.mean(x * x, axis=-1, keepdims=True) + EPSILON)


def forward_kernel(x_ref, gain_ref, wv_ref, pattern_ref, *refs):
    mixed_ref, turned_ref, normed_t_ref = refs[-3:]
    heads, seq = pattern_ref.shape[1:3]
    x = x_ref[...].astype(F32)
    normed = (x * rms_of(x) * gain_ref[...]).astype(BF16)
    normed_t_ref[...] = normed.T
    values = dot(normed, wv_ref[...], ((1,), (0,))).astype(BF16)
    for part in range(2):
        at = slice(part * seq, (part + 1) * seq)
        pattern = pattern_ref[part].reshape(heads * seq, seq)
        turned_ref[part] = pattern.T
        mixed = dot(pattern, values[at], ((1,), (0,))).astype(BF16)
        for h in range(heads):
            mixed_ref[at, h * HEAD_DIM : (h + 1) * HEAD_DIM] = mixed[h * seq : (h + 1) * seq]


def add_values(step, dy, wo_ref, turned_refs, values_ref, mixed_ref):
    part = dot(dy, wo_ref[...], ((1,), (1,)))

    @pl.when(step == 0)
    def _():
        mixed_ref[...] = part

    @pl.when(step > 0)
    def _():
        mixed_ref[...] += part

    @pl.when(step == pl.num_programs(0) - 1)
    def _():
        per_pair, seq, depth = turned_refs[0].shape
        for n in range(per_pair * len(turned_refs)):
            at = slice(n * seq, (n + 1) * seq)
            mixed = mixed_ref[at].astype(BF16)
            stacked = jnp.concatenate(
                [mixed[:, h * HEAD_DIM : (h + 1) * HEAD_DIM] for h in range(depth // seq)], axis=0
            )
            turned = turned_refs[n // per_pair][n % per_pair]
            values_ref[at] = dot(turned, stacked, ((1,), (0,))).astype(BF16)


def upper_values_kernel(
    active_ref, tensor_ref, own_ref, other_ref, mask_ref, wo_ref, a_ref, b_ref,
    values_ref, raw_ref, mixed_ref,
):
    @pl.when(active_ref[0] == 1)
    def _():
        first = tensor_ref[0] == 0
        seq = own_ref.shape[1]
        for p in range(own_ref.shape[0]):
            own, other = own_ref[p].astype(F32), other_ref[p].astype(F32)
            for c, head in enumerate((jnp.where(first, own, other), jnp.where(first, other, own))):
                at = slice((2 * p + c) * seq, (2 * p + c + 1) * seq)
                raw_ref[at] = (mask_ref[at] * head).astype(BF16)
        step = pl.program_id(0)
        add_values(step, raw_ref[...], wo_ref, (a_ref, b_ref), values_ref, mixed_ref)


def lower_values_kernel(active_ref, dy_ref, wo_ref, a_ref, b_ref, values_ref, mixed_ref):
    @pl.when(active_ref[0] == 1)
    def _():
        step = pl.program_id(0)
        add_values(step, dy_ref[...], wo_ref, (a_ref, b_ref), values_ref, mixed_ref)


def rows_of_sequence(own_ref, other_ref, own_wv_ref, other_wv_ref, x_ref, gain_ref, dy_ref):
    first = dot(own_ref[...], own_wv_ref[...], ((1,), (1,))).astype(BF16)
    second = dot(other_ref[...], other_wv_ref[...], ((1,), (1,))).astype(BF16)
    scaled = (first.astype(F32) + second.astype(F32)) * gain_ref[...]
    x = x_ref[...].astype(F32)
    inverse = rms_of(x)
    pull = (inverse * inverse * inverse) * jnp.mean(x * scaled, axis=-1, keepdims=True)
    return dy_ref[...].astype(F32) + (inverse * scaled - x * pull)


def rows_kernel(active_ref, *refs):
    @pl.when(active_ref[0] == 1)
    def _():
        refs[-1][...] = rows_of_sequence(*refs[:-1]).astype(BF16)


def own_rows_kernel(active_ref, tensor_ref, weight_ref, done_ref, *refs):
    @pl.when(active_ref[0] == 1)
    def _():
        refs[-1][0] = (weight_ref[...] * rows_of_sequence(*refs[:-1])).astype(BF16)

    @pl.when(active_ref[0] == 0)
    def _():
        refs[-1][0] = (weight_ref[...] * done_ref[...].astype(F32)).astype(BF16)


def owners_kernel(upper_ref, y_ref, *refs):
    (upper_dy, upper_values, lower_dy, lower_values, weight_ref, a_ref, b_ref), refs = (
        refs[:7],
        refs[7:],
    )
    out_refs, turned_ref, dy_buffer, sems = refs[:NY], refs[NY], refs[NY + 1], refs[NY + 2]
    block = 896

    def turn(dy_hbm, values_ref):
        tokens, width = dy_hbm.shape
        copies = [
            pltpu.make_async_copy(
                dy_hbm.at[:, start : start + block], dy_buffer.at[n], sems.at[n]
            )
            for n, start in enumerate(range(0, width, block))
        ]
        for copy in copies:
            copy.start()
        weight = weight_ref[...]
        values = (weight * values_ref[...].astype(F32)).astype(BF16)
        half = tokens // 2
        turned_ref[:, tokens:] = (
            dot(a_ref[...], values[:half], ((1,), (0,)))
            + dot(b_ref[...], values[half:], ((1,), (0,)))
        ).astype(BF16)
        for n, copy in enumerate(copies):
            copy.wait()
            dy = (weight * dy_buffer[n].astype(F32)).astype(BF16)
            turned_ref[n * block : (n + 1) * block, :tokens] = dy.T

    @pl.when(upper_ref[0] == 1)
    def _():
        turn(upper_dy, upper_values)

    @pl.when(upper_ref[0] == 0)
    def _():
        turn(lower_dy, lower_values)

    size = out_refs[0].shape[0] // NZ
    for s, out_ref in enumerate(out_refs):
        owner = (y_ref[0] + s) % NY
        for z in range(NZ):
            start = pl.multiple_of((z * NY + owner) * size, 16)
            out_ref[z * size : (z + 1) * size] = turned_ref[pl.ds(start, size)]


def products_kernel(own_ref, *refs):
    blocks, mixed_refs, out_refs, total_ref = refs[:NY], refs[NY : 2 * NY], refs[2 * NY : -1], refs[-1]
    tokens = mixed_refs[0].shape[0]
    total_ref[:, :HEAD_DIM] = sum(b[:, tokens:].astype(F32) for b in blocks)
    total_ref[:, HEAD_DIM:] = sum(
        dot(b[:, :tokens], m[...], ((1,), (0,))) for b, m in zip(blocks, mixed_refs)
    )
    count, size = out_refs[0].shape[:2]
    for k, out_ref in enumerate(out_refs):
        for n in range(count):
            start = pl.multiple_of((n * 4 + (own_ref[0] ^ k)) * size, 8)
            out_ref[n] = total_ref[pl.ds(start, size)].astype(BF16)


def stage_kernel(own_ref, a_ref, b_ref, c_ref, d_ref, *out_refs):
    for k, out_ref in enumerate(out_refs):
        j = own_ref[0] ^ k
        total = sum(r[j].astype(F32) for r in (a_ref, b_ref, c_ref, d_ref))
        out_ref[...] = total.astype(out_ref.dtype)


def last_kernel(a_ref, b_ref, c_ref, d_ref, wv_ref, gain_ref, value_ref, output_ref, part_ref):
    total = a_ref[...] + sum(r[...].astype(F32) for r in (b_ref, c_ref, d_ref))
    value = total[:, :HEAD_DIM]
    value_ref[0] = value
    output_ref[0] = total[:, HEAD_DIM:]
    row = lax.dot_general(
        jnp.ones((8, HEAD_DIM), F32),
        wv_ref[...] * value,
        (((1,), (1,)), ((), ())),
        precision=lax.Precision.HIGHEST,
        preferred_element_type=F32,
    )
    part_ref[...] = row[:1] / gain_ref[...]


def shaped(*dims):
    return jax.ShapeDtypeStruct(dims, BF16)


def after(block, *others):
    return lax.optimization_barrier((block, *others))[0]


def section_step(
    hidden_in,
    attention_probs,
    norm_gain,
    value_weight,
    output_weight,
    head_grad,
    policy_logprob,
    reference_logprob,
    sequence_bounds,
):
    section = lax.axis_index("pipe")
    zi, yi, xi, ti = (lax.axis_index(a) for a in ("z", "y", "x", "t"))
    pairs, _, seq, width = hidden_in.shape[1:]
    heads = attention_probs.shape[3]
    tokens = pairs * 2 * seq
    gain = norm_gain[0]
    wv = value_weight[0]
    wo = output_weight[0]
    inputs = hidden_in[0]
    pattern = attention_probs[0]
    own_head = head_grad[:, 0]

    other_head = lax.ppermute(own_head, ("pipe", "t"), [(2, 3), (3, 2)])

    positions = jnp.arange(seq, dtype=jnp.int32)
    response_bool = (positions[None, None, :] >= sequence_bounds[:, 0:1, None]) & (
        positions[None, None, :] < sequence_bounds[:, 1:3, None]
    )
    ends = jnp.clip(sequence_bounds[:, :2], 0, seq)
    count = jnp.sum(jnp.maximum(ends[:, 1] - ends[:, 0], 0)).reshape(1, 1)
    count = lax.optimization_barrier(jnp.broadcast_to(count, (8, 128)))

    def exchanged(block, z, y, x):
        base = NZ * NY * NX
        route = []
        for device in range(base):
            zz, yy, xx = device // (NY * NX), device // NX % NY, device % NX
            route.append((device, ((zz ^ z) * NY + (yy ^ y)) * NX + (xx ^ x)))
        return lax.ppermute(block, ("pipe", "z", "y", "x"), route)

    for steps in (
        ((0, 0, 1), (0, 1, 0), (0, 1, 1)),
        ((1, 0, 0), (0, 2, 0), (1, 2, 0)),
        ((2, 0, 0),),
        ((4, 0, 0),),
    ):
        got = [exchanged(count, *at) for at in steps]
        count = count + sum(got)
    mask = response_bool.astype(F32)
    sequence_logprob = jnp.sum(mask * policy_logprob, axis=-1)
    margin = DPO_BETA * (
        sequence_logprob[:, 0]
        - reference_logprob[:, 0]
        - (sequence_logprob[:, 1] - reference_logprob[:, 1])
    )
    weight_pair = jax.nn.sigmoid(-margin)

    def across(block, section_id):
        pairs_xt = ((0, 3), (3, 0), (1, 2), (2, 1))
        base = section_id * 4
        route = [(base + a, base + b) for a, b in pairs_xt]
        return lax.ppermute(block, ("pipe", "x", "t"), route)

    other_wv_1 = across(wv, 1)

    x = inputs.reshape(tokens, width)
    patterns = pattern.reshape(pairs * 2, heads, seq, seq)
    half = tokens // pairs

    def forward(p, *earlier):
        return pl.pallas_call(
            forward_kernel,
            out_shape=(
                shaped(tokens, heads * HEAD_DIM),
                shaped(2, seq, heads * seq),
                shaped(width, half),
            ),
            grid=(1,),
            in_specs=[
                pl.BlockSpec((half, width), lambda i: (p, 0)),
                pl.BlockSpec((1, width), lambda i: (0, 0)),
                pl.BlockSpec((width, HEAD_DIM), lambda i: (0, 0)),
                pl.BlockSpec((2, heads, seq, seq), lambda i: (p, 0, 0, 0)),
            ]
            + [ANY] * len(earlier),
            out_specs=(
                pl.BlockSpec((half, heads * HEAD_DIM), lambda i: (p, 0)),
                pl.BlockSpec((2, seq, heads * seq), lambda i: (0, 0, 0)),
                pl.BlockSpec((width, half), lambda i: (0, 0)),
            ),
            input_output_aliases={4: 0} if earlier else {},
        )(x, norm_gain, wv, patterns, *earlier)

    mixed, turned_0, normed_0 = forward(0)
    mixed, turned_1, normed_1 = forward(1, mixed)

    def around(shift):
        return lax.ppermute(mixed, "y", [(i, (i + shift) % NY) for i in range(NY)])

    mixed_all = [mixed] + [around(s) for s in range(1, NY)]

    upper = section == 1
    is_upper = upper.astype(jnp.int32).reshape(1)
    is_lower = 1 - is_upper
    tensor = ti.astype(jnp.int32).reshape(1)
    block = width // 2

    def values_of(kernel, scalars, blocks, more):
        def along(*shape):
            rank = len(shape)
            return pl.BlockSpec(shape, lambda i, on, *_: (0,) * (rank - 1) + (i * on[0],))

        def whole(*shape):
            return pl.BlockSpec(shape, lambda i, *_: (0,) * len(shape))

        out_shape = [shaped(tokens, HEAD_DIM)] + [shaped(tokens, width)] * more
        out_specs = [whole(tokens, HEAD_DIM)] + [along(tokens, block)] * more
        in_specs = [
            along(*b.shape[:-1], block) if b.shape[-1] == width else whole(*b.shape)
            for b in blocks
        ]
        return pl.pallas_call(
            kernel,
            out_shape=out_shape,
            grid_spec=pltpu.PrefetchScalarGridSpec(
                num_scalar_prefetch=len(scalars),
                grid=(width // block,),
                in_specs=in_specs,
                out_specs=out_specs,
                scratch_shapes=[pltpu.VMEM((tokens, heads * HEAD_DIM), F32)],
            ),
        )(*scalars, *blocks)

    def whole_of(*shape):
        return pl.BlockSpec(shape, lambda n, *_: (0,) * len(shape))

    def rows_of(active, own, other, other_wv, dy):
        def pick(n, on):
            return (n * on[0], 0)

        return pl.pallas_call(
            rows_kernel,
            out_shape=shaped(tokens, width),
            grid_spec=pltpu.PrefetchScalarGridSpec(
                num_scalar_prefetch=1,
                grid=(pairs * 2,),
                in_specs=[
                    pl.BlockSpec((seq, HEAD_DIM), pick),
                    pl.BlockSpec((seq, HEAD_DIM), pick),
                    whole_of(width, HEAD_DIM),
                    whole_of(width, HEAD_DIM),
                    pl.BlockSpec((seq, width), pick),
                    whole_of(1, width),
                    pl.BlockSpec((seq, width), pick),
                ],
                out_specs=pl.BlockSpec((seq, width), pick),
            ),
        )(active, own, other, wv, other_wv, x, norm_gain, dy)

    def own_rows_of(active, weight, done, own, other, other_wv, dy):
        def pick(n, on, t):
            return ((n * 2 + t[0]) * on[0], 0)

        def mine(n, on, t):
            return (n * 2 + t[0], 0)

        return pl.pallas_call(
            own_rows_kernel,
            out_shape=shaped(1, pairs * seq, width),
            grid_spec=pltpu.PrefetchScalarGridSpec(
                num_scalar_prefetch=2,
                grid=(pairs,),
                in_specs=[
                    pl.BlockSpec((seq, 1), mine),
                    pl.BlockSpec((seq, width), lambda n, on, t: ((n * 2 + t[0]) * (1 - on[0]), 0)),
                    pl.BlockSpec((seq, HEAD_DIM), pick),
                    pl.BlockSpec((seq, HEAD_DIM), pick),
                    whole_of(width, HEAD_DIM),
                    whole_of(width, HEAD_DIM),
                    pl.BlockSpec((seq, width), pick),
                    whole_of(1, width),
                    pl.BlockSpec((seq, width), pick),
                ],
                out_specs=pl.BlockSpec((1, seq, width), lambda n, on, t: (0, n, 0)),
            ),
        )(active, tensor, weight, done, own, other, wv, other_wv, x, norm_gain, dy)

    def swapped(values, section_id):
        route = [(section_id * 2, section_id * 2 + 1), (section_id * 2 + 1, section_id * 2)]
        return lax.ppermute(values, ("pipe", "t"), route)

    columns = HEAD_DIM * (heads + 1)
    share_rows = width // (NZ * NY * NX)

    mask_column = mask.reshape(tokens, 1)
    own_1, raw = values_of(
        upper_values_kernel,
        (is_upper, tensor),
        (own_head, other_head, mask_column, wo, turned_0, turned_1),
        1,
    )
    other_1 = swapped(own_1, 1)
    rows_1 = rows_of(is_upper, own_1, other_1, other_wv_1, raw)
    incoming = lax.ppermute(rows_1, "pipe", [(1, 0)])

    count = after(count, rows_1)
    count_up = lax.ppermute(count, "pipe", [(0, 1)])
    chosen_total = jnp.where(upper, count_up, count)[0, 0]
    pair_total = pairs * NZ * NY * NX
    scale = LIKELIHOOD_COEF * jnp.asarray(pair_total, F32) / chosen_total.astype(F32)
    weights = jnp.stack([-DPO_BETA * weight_pair - scale, DPO_BETA * weight_pair], axis=1)
    weight = jnp.broadcast_to(weights[:, :, None], (pairs, 2, seq)).reshape(tokens, 1)

    (own_0,) = values_of(lower_values_kernel, (is_lower,), (incoming, wo, turned_0, turned_1), 0)
    other_0 = swapped(own_0, 0)
    other_wv_0 = across(after(wv, count), 0)

    turned = pl.pallas_call(
        owners_kernel,
        out_shape=(shaped(width // NY, tokens + HEAD_DIM),) * NY,
        in_specs=[SMEM, SMEM, ANY, VMEM, ANY, VMEM, VMEM, VMEM, VMEM],
        out_specs=(VMEM,) * NY,
        scratch_shapes=[
            pltpu.VMEM((width, tokens + HEAD_DIM), BF16),
            pltpu.VMEM((4, tokens, 896), BF16),
            pltpu.SemaphoreType.DMA((4,)),
        ],
    )(
        is_upper, yi.astype(jnp.int32).reshape(1), raw, own_1, incoming, own_0, weight,
        normed_0, normed_1,
    )
    blocks = [turned[0]]
    for s in range(1, NY):
        route = [(i, (i + s) % NY) for i in range(NY)]
        blocks.append(lax.ppermute(turned[s], "y", route))

    first_own = ((zi % 2) * NX + xi).astype(jnp.int32).reshape(1)
    group = width // NY // 2

    parts = pl.pallas_call(
        products_kernel,
        out_shape=(shaped(4, share_rows, columns),) * 4,
        grid_spec=pltpu.PrefetchScalarGridSpec(
            num_scalar_prefetch=1,
            grid=(2,),
            in_specs=[pl.BlockSpec((group, tokens + HEAD_DIM), lambda i, own: (i, 0))] * NY
            + [whole_of(tokens, heads * HEAD_DIM)] * NY,
            out_specs=(pl.BlockSpec((2, share_rows, columns), lambda i, own: (i, 0, 0)),) * 4,
            scratch_shapes=[pltpu.VMEM((group, columns), F32)],
        ),
    )(first_own, *after(tuple(blocks), other_0), *mixed_all)
    got = [parts[0]] + [over_xz(parts[k], k) for k in (1, 2, 3)]
    parts = pl.pallas_call(
        stage_kernel,
        out_shape=(jax.ShapeDtypeStruct((share_rows, columns), F32),)
        + (shaped(share_rows, columns),) * 3,
        in_specs=[SMEM] + [VMEM] * 4,
        out_specs=(VMEM,) * 4,
    )((zi // 2).astype(jnp.int32).reshape(1), *got)
    got = [parts[0]] + [over_xz(parts[k], k << 2) for k in (1, 2, 3)]

    own_rows = own_rows_of(is_lower, weight, rows_1, own_0, other_0, other_wv_0, incoming)
    start = ((zi * NY + yi) * NX + xi) * share_rows
    own_wv = lax.dynamic_slice_in_dim(wv, start, share_rows, 0).astype(F32)
    own_gain = lax.dynamic_slice_in_dim(gain, start, share_rows, 0).reshape(1, share_rows)
    value_share, output_share, gain_part = pl.pallas_call(
        last_kernel,
        out_shape=(
            jax.ShapeDtypeStruct((1, share_rows, HEAD_DIM), F32),
            jax.ShapeDtypeStruct((1, share_rows, columns - HEAD_DIM), F32),
            jax.ShapeDtypeStruct((1, share_rows), F32),
        ),
        in_specs=[VMEM] * 6,
        out_specs=(VMEM,) * 3,
    )(*got, own_wv, own_gain)
    gain_rows = gain_part + paired(gain_part, "t", NT, 1)
    return own_rows.reshape(1, pairs, 1, seq, width), value_share, output_share, gain_rows


def solution(mesh):
    fine = Mesh(
        mesh.devices.reshape(2, NZ, NY, NX, NT), ("pipe", "z", "y", "x", "t")
    )
    dp = ("z", "y", "x")
    in_specs = (
        P("pipe", dp, None, None, None),
        P("pipe", dp, None, "t", None, None),
        P("pipe", None),
        P("pipe", None, "t"),
        P("pipe", "t", None),
        P(dp, "t", None, None),
        P(dp, None, None),
        P(dp, None),
        P(dp, None),
    )
    out_specs = (
        P("pipe", dp, "t", None, None),
        P("pipe", dp, "t"),
        P("pipe", dp, "t"),
        P("pipe", dp),
    )
    return jax.shard_map(section_step, mesh=fine, in_specs=in_specs, out_specs=out_specs, check_vma=False)
```

```python
import jax
import jax.numpy as jnp
from jax import lax
from jax.experimental import pallas as pl
from jax.experimental.pallas import tpu as pltpu
from jax.sharding import Mesh, PartitionSpec as P


HEAD_DIM = 128
EPSILON = 1e-06
DPO_BETA = 0.25
LIKELIHOOD_COEF = 0.2
NZ, NY, NX, NT = 8, 4, 2, 2
F32, BF16 = jnp.float32, jnp.bfloat16


def paired(block, axis, size, distance, section=None):
    if section is None:
        return lax.ppermute(block, axis, [(i, i ^ distance) for i in range(size)])
    base = section * size
    route = [(base + i, base + (i ^ distance)) for i in range(size)]
    return lax.ppermute(block, ("pipe", axis), route)


def over_xz(block, k):
    route = [
        (z * NX + x, (z ^ (k >> 1)) * NX + (x ^ (k & 1))) for z in range(NZ) for x in range(NX)
    ]
    return lax.ppermute(block, ("z", "x"), route)


VMEM = pl.BlockSpec(memory_space=pltpu.VMEM)
SMEM = pl.BlockSpec(memory_space=pltpu.SMEM)
ANY = pl.BlockSpec(memory_space=pl.ANY)


def dot(a, b, contract):
    return lax.dot_general(a, b, (contract, ((), ())), preferred_element_type=F32)


def rms_of(x):
    return lax.rsqrt(jnp.mean(x * x, axis=-1, keepdims=True) + EPSILON)


def deal(out_refs, source_ref, first_owner):
    size = source_ref.shape[0] // (NZ * NY)
    for s, out_ref in enumerate(out_refs):
        owner = (first_owner + s) % NY
        for z in range(NZ):
            start = pl.multiple_of((z * NY + owner) * size, 16)
            out_ref[z * size : (z + 1) * size] = source_ref[pl.ds(start, size)]


def forward_kernel(y_ref, x_ref, gain_ref, wv_ref, pattern_ref, *refs):
    mixed_ref, turned_ref, normed_refs, normed_t_ref = refs[-7], refs[-6], refs[-5:-1], refs[-1]
    heads, seq = pattern_ref.shape[1:3]
    x = x_ref[...].astype(F32)
    normed = (x * rms_of(x) * gain_ref[...]).astype(BF16)
    normed_t_ref[...] = normed.T
    deal(normed_refs, normed_t_ref, y_ref[0])
    values = dot(normed, wv_ref[...], ((1,), (0,))).astype(BF16)
    for part in range(2):
        at = slice(part * seq, (part + 1) * seq)
        pattern = pattern_ref[part].reshape(heads * seq, seq)
        turned_ref[part] = pattern.T
        mixed = dot(pattern, values[at], ((1,), (0,))).astype(BF16)
        for h in range(heads):
            mixed_ref[at, h * HEAD_DIM : (h + 1) * HEAD_DIM] = mixed[h * seq : (h + 1) * seq]


def add_values(step, dy, wo_ref, turned_refs, values_ref, mixed_ref):
    part = dot(dy, wo_ref[...], ((1,), (1,)))

    @pl.when(step == 0)
    def _():
        mixed_ref[...] = part

    @pl.when(step > 0)
    def _():
        mixed_ref[...] += part

    @pl.when(step == pl.num_programs(0) - 1)
    def _():
        per_pair, seq, depth = turned_refs[0].shape
        for n in range(per_pair * len(turned_refs)):
            at = slice(n * seq, (n + 1) * seq)
            mixed = mixed_ref[at].astype(BF16)
            stacked = jnp.concatenate(
                [mixed[:, h * HEAD_DIM : (h + 1) * HEAD_DIM] for h in range(depth // seq)], axis=0
            )
            turned = turned_refs[n // per_pair][n % per_pair]
            values_ref[at] = dot(turned, stacked, ((1,), (0,))).astype(BF16)


def upper_values_kernel(
    active_ref, tensor_ref, own_ref, other_ref, mask_ref, wo_ref, a_ref, b_ref,
    values_ref, raw_ref, mixed_ref,
):
    @pl.when(active_ref[0] == 1)
    def _():
        first = tensor_ref[0] == 0
        seq = own_ref.shape[1]
        for p in range(own_ref.shape[0]):
            own, other = own_ref[p].astype(F32), other_ref[p].astype(F32)
            for c, head in enumerate((jnp.where(first, own, other), jnp.where(first, other, own))):
                at = slice((2 * p + c) * seq, (2 * p + c + 1) * seq)
                raw_ref[at] = (mask_ref[at] * head).astype(BF16)
        step = pl.program_id(0)
        add_values(step, raw_ref[...], wo_ref, (a_ref, b_ref), values_ref, mixed_ref)


def lower_values_kernel(active_ref, dy_ref, wo_ref, a_ref, b_ref, values_ref, mixed_ref):
    @pl.when(active_ref[0] == 1)
    def _():
        step = pl.program_id(0)
        add_values(step, dy_ref[...], wo_ref, (a_ref, b_ref), values_ref, mixed_ref)


def rows_of_sequence(own_ref, other_ref, own_wv_ref, other_wv_ref, x_ref, gain_ref, dy_ref):
    first = dot(own_ref[...], own_wv_ref[...], ((1,), (1,))).astype(BF16)
    second = dot(other_ref[...], other_wv_ref[...], ((1,), (1,))).astype(BF16)
    scaled = (first.astype(F32) + second.astype(F32)) * gain_ref[...]
    x = x_ref[...].astype(F32)
    inverse = rms_of(x)
    pull = (inverse * inverse * inverse) * jnp.mean(x * scaled, axis=-1, keepdims=True)
    return dy_ref[...].astype(F32) + (inverse * scaled - x * pull)


def rows_kernel(active_ref, *refs):
    @pl.when(active_ref[0] == 1)
    def _():
        refs[-1][...] = rows_of_sequence(*refs[:-1]).astype(BF16)


def own_rows_kernel(active_ref, tensor_ref, weight_ref, done_ref, *refs):
    @pl.when(active_ref[0] == 1)
    def _():
        refs[-1][0] = (weight_ref[...] * rows_of_sequence(*refs[:-1])).astype(BF16)

    @pl.when(active_ref[0] == 0)
    def _():
        refs[-1][0] = (weight_ref[...] * done_ref[...].astype(F32)).astype(BF16)


EXTRA = 16


def owners_kernel(upper_ref, y_ref, *refs):
    (upper_dy, upper_values, lower_dy, lower_values, weight_ref), refs = refs[:5], refs[5:]
    out_refs, turned_ref, dy_buffer, sems = refs[:NY], refs[NY], refs[NY + 1], refs[NY + 2]
    block = dy_buffer.shape[2]

    def turn(dy_hbm, values_ref):
        tokens, width = dy_hbm.shape
        copies = [
            pltpu.make_async_copy(
                dy_hbm.at[:, start : start + block], dy_buffer.at[n], sems.at[n]
            )
            for n, start in enumerate(range(0, width, block))
        ]
        for copy in copies:
            copy.start()
        weight = weight_ref[...]
        high = weight.astype(BF16).astype(F32)
        rest = jnp.zeros((EXTRA - 2, tokens), F32)
        below = jnp.concatenate([high, weight - high, rest], axis=0).astype(BF16)
        values_t = values_ref[...].T
        for out_ref in out_refs:
            rows = out_ref.shape[0]
            out_ref[rows - EXTRA - HEAD_DIM : rows - EXTRA] = values_t
            out_ref[rows - EXTRA :] = below
        for n, copy in enumerate(copies):
            copy.wait()
            turned_ref[n * block : (n + 1) * block] = dy_buffer[n].T

    @pl.when(upper_ref[0] == 1)
    def _():
        turn(upper_dy, upper_values)

    @pl.when(upper_ref[0] == 0)
    def _():
        turn(lower_dy, lower_values)

    deal(out_refs, turned_ref, y_ref[0])


def products_kernel(own_ref, scale_ref, *refs):
    groups, refs = [refs[n * NY : (n + 1) * NY] for n in range(5)], refs[5 * NY :]
    out_refs, total_ref = refs[:-1], refs[-1]
    tokens = groups[0][0].shape[1]
    lane = lax.broadcasted_iota(jnp.int32, (1, tokens), 1)
    chosen = jnp.where(lane // 64 % 2 == 0, scale_ref[0], 0.0)
    value, output = 0.0, 0.0
    for dy_ref, values_ref, weight_ref, normed_ref, mixed_ref in zip(*groups):
        rows = weight_ref[...].astype(F32)
        weight = rows[0:1] + rows[1:2] - chosen
        dy = (weight * dy_ref[...].astype(F32)).astype(BF16)
        values_t = (weight * values_ref[...].astype(F32)).astype(BF16)
        output = output + dot(dy, mixed_ref[...], ((1,), (0,)))
        value = value + dot(normed_ref[...], values_t, ((1,), (1,)))
    total_ref[:, :HEAD_DIM] = value
    total_ref[:, HEAD_DIM:] = output
    count, size = out_refs[0].shape[:2]
    for k, out_ref in enumerate(out_refs):
        for n in range(count):
            start = pl.multiple_of((n * 4 + (own_ref[0] ^ k)) * size, 8)
            out_ref[n] = total_ref[pl.ds(start, size)].astype(BF16)


def stage_kernel(own_ref, a_ref, b_ref, c_ref, d_ref, *out_refs):
    for k, out_ref in enumerate(out_refs):
        j = own_ref[0] ^ k
        total = sum(r[j].astype(F32) for r in (a_ref, b_ref, c_ref, d_ref))
        out_ref[...] = total.astype(out_ref.dtype)


def last_kernel(a_ref, b_ref, c_ref, d_ref, wv_ref, gain_ref, value_ref, output_ref, part_ref):
    total = a_ref[...] + sum(r[...].astype(F32) for r in (b_ref, c_ref, d_ref))
    value = total[:, :HEAD_DIM]
    value_ref[0] = value
    output_ref[0] = total[:, HEAD_DIM:]
    row = lax.dot_general(
        jnp.ones((8, HEAD_DIM), F32),
        wv_ref[...] * value,
        (((1,), (1,)), ((), ())),
        precision=lax.Precision.HIGHEST,
        preferred_element_type=F32,
    )
    part_ref[...] = row[:1] / gain_ref[...]


def shaped(*dims):
    return jax.ShapeDtypeStruct(dims, BF16)


def after(block, *others):
    return lax.optimization_barrier((block, *others))[0]


def section_step(
    hidden_in,
    attention_probs,
    norm_gain,
    value_weight,
    output_weight,
    head_grad,
    policy_logprob,
    reference_logprob,
    sequence_bounds,
):
    section = lax.axis_index("pipe")
    zi, yi, xi, ti = (lax.axis_index(a) for a in ("z", "y", "x", "t"))
    pairs, _, seq, width = hidden_in.shape[1:]
    heads = attention_probs.shape[3]
    tokens = pairs * 2 * seq
    gain = norm_gain[0]
    wv = value_weight[0]
    wo = output_weight[0]
    inputs = hidden_in[0]
    pattern = attention_probs[0]
    own_head = head_grad[:, 0]

    other_head = lax.ppermute(own_head, ("pipe", "t"), [(2, 3), (3, 2)])

    positions = jnp.arange(seq, dtype=jnp.int32)
    response_bool = (positions[None, None, :] >= sequence_bounds[:, 0:1, None]) & (
        positions[None, None, :] < sequence_bounds[:, 1:3, None]
    )
    ends = jnp.clip(sequence_bounds[:, :2], 0, seq)
    count = jnp.sum(jnp.maximum(ends[:, 1] - ends[:, 0], 0)).reshape(1, 1)
    count = lax.optimization_barrier(jnp.broadcast_to(count, (8, 128)))

    def exchanged(block, z, y, x, section_id):
        base = NZ * NY * NX
        route = []
        for device in range(base):
            zz, yy, xx = device // (NY * NX), device // NX % NY, device % NX
            other = ((zz ^ z) * NY + (yy ^ y)) * NX + (xx ^ x)
            route.append((section_id * base + device, section_id * base + other))
        return lax.ppermute(block, ("pipe", "z", "y", "x"), route)

    for steps in (((0, 0, 1), (0, 1, 0), (0, 1, 1)), ((1, 0, 0), (0, 2, 0), (1, 2, 0))):
        got = [exchanged(count, *at, 0) for at in steps]
        count = count + sum(got)
    mask = response_bool.astype(F32)
    sequence_logprob = jnp.sum(mask * policy_logprob, axis=-1)
    margin = DPO_BETA * (
        sequence_logprob[:, 0]
        - reference_logprob[:, 0]
        - (sequence_logprob[:, 1] - reference_logprob[:, 1])
    )
    weight_pair = jax.nn.sigmoid(-margin)

    def across(block, section_id):
        pairs_xt = ((0, 3), (3, 0), (1, 2), (2, 1))
        base = section_id * 4
        route = [(base + a, base + b) for a, b in pairs_xt]
        return lax.ppermute(block, ("pipe", "x", "t"), route)

    other_wv_1 = across(wv, 1)

    x = inputs.reshape(tokens, width)
    patterns = pattern.reshape(pairs * 2, heads, seq, seq)
    half = tokens // pairs

    y_index = yi.astype(jnp.int32).reshape(1)

    def forward(p, *earlier):
        return pl.pallas_call(
            forward_kernel,
            out_shape=(shaped(tokens, heads * HEAD_DIM), shaped(2, seq, heads * seq))
            + (shaped(width // NY, tokens),) * NY,
            grid_spec=pltpu.PrefetchScalarGridSpec(
                num_scalar_prefetch=1,
                grid=(1,),
                in_specs=[
                    pl.BlockSpec((half, width), lambda i, y: (p, 0)),
                    pl.BlockSpec((1, width), lambda i, y: (0, 0)),
                    pl.BlockSpec((width, HEAD_DIM), lambda i, y: (0, 0)),
                    pl.BlockSpec((2, heads, seq, seq), lambda i, y: (p, 0, 0, 0)),
                ]
                + [ANY] * len(earlier),
                out_specs=(
                    pl.BlockSpec((half, heads * HEAD_DIM), lambda i, y: (p, 0)),
                    pl.BlockSpec((2, seq, heads * seq), lambda i, y: (0, 0, 0)),
                )
                + (pl.BlockSpec((width // NY, half), lambda i, y: (0, p)),) * NY,
                scratch_shapes=[pltpu.VMEM((width, half), BF16)],
            ),
            input_output_aliases={5: 0, 6: 2, 7: 3, 8: 4, 9: 5} if earlier else {},
        )(y_index, x, norm_gain, wv, patterns, *earlier)

    mixed, turned_0, *normed = forward(0)
    mixed, turned_1, *normed = forward(1, mixed, *normed)

    def around(block, shift):
        return lax.ppermute(block, "y", [(i, (i + shift) % NY) for i in range(NY)])

    mixed_all = [mixed] + [around(mixed, s) for s in range(1, NY)]
    normed_all = [normed[0]] + [around(normed[s], s) for s in range(1, NY)]

    upper = section == 1
    is_upper = upper.astype(jnp.int32).reshape(1)
    is_lower = 1 - is_upper
    tensor = ti.astype(jnp.int32).reshape(1)
    block = width // 2

    def values_of(kernel, scalars, blocks, more):
        def along(*shape):
            rank = len(shape)
            return pl.BlockSpec(shape, lambda i, on, *_: (0,) * (rank - 1) + (i * on[0],))

        def whole(*shape):
            return pl.BlockSpec(shape, lambda i, *_: (0,) * len(shape))

        out_shape = [shaped(tokens, HEAD_DIM)] + [shaped(tokens, width)] * more
        out_specs = [whole(tokens, HEAD_DIM)] + [along(tokens, block)] * more
        in_specs = [
            along(*b.shape[:-1], block) if b.shape[-1] == width else whole(*b.shape)
            for b in blocks
        ]
        return pl.pallas_call(
            kernel,
            out_shape=out_shape,
            grid_spec=pltpu.PrefetchScalarGridSpec(
                num_scalar_prefetch=len(scalars),
                grid=(width // block,),
                in_specs=in_specs,
                out_specs=out_specs,
                scratch_shapes=[pltpu.VMEM((tokens, heads * HEAD_DIM), F32)],
            ),
        )(*scalars, *blocks)

    def whole_of(*shape):
        return pl.BlockSpec(shape, lambda n, *_: (0,) * len(shape))

    def rows_of(active, own, other, other_wv, dy):
        def pick(n, on):
            return (n * on[0], 0)

        return pl.pallas_call(
            rows_kernel,
            out_shape=shaped(tokens, width),
            grid_spec=pltpu.PrefetchScalarGridSpec(
                num_scalar_prefetch=1,
                grid=(pairs * 2,),
                in_specs=[
                    pl.BlockSpec((seq, HEAD_DIM), pick),
                    pl.BlockSpec((seq, HEAD_DIM), pick),
                    whole_of(width, HEAD_DIM),
                    whole_of(width, HEAD_DIM),
                    pl.BlockSpec((seq, width), pick),
                    whole_of(1, width),
                    pl.BlockSpec((seq, width), pick),
                ],
                out_specs=pl.BlockSpec((seq, width), pick),
            ),
        )(active, own, other, wv, other_wv, x, norm_gain, dy)

    def own_rows_of(active, weight, done, own, other, other_wv, dy):
        def pick(n, on, t):
            return ((n * 2 + t[0]) * on[0], 0)

        def mine(n, on, t):
            return (n * 2 + t[0], 0)

        return pl.pallas_call(
            own_rows_kernel,
            out_shape=shaped(1, pairs * seq, width),
            grid_spec=pltpu.PrefetchScalarGridSpec(
                num_scalar_prefetch=2,
                grid=(pairs,),
                in_specs=[
                    pl.BlockSpec((seq, 1), mine),
                    pl.BlockSpec((seq, width), lambda n, on, t: ((n * 2 + t[0]) * (1 - on[0]), 0)),
                    pl.BlockSpec((seq, HEAD_DIM), pick),
                    pl.BlockSpec((seq, HEAD_DIM), pick),
                    whole_of(width, HEAD_DIM),
                    whole_of(width, HEAD_DIM),
                    pl.BlockSpec((seq, width), pick),
                    whole_of(1, width),
                    pl.BlockSpec((seq, width), pick),
                ],
                out_specs=pl.BlockSpec((1, seq, width), lambda n, on, t: (0, n, 0)),
            ),
        )(active, tensor, weight, done, own, other, wv, other_wv, x, norm_gain, dy)

    def swapped(values, section_id):
        route = [(section_id * 2, section_id * 2 + 1), (section_id * 2 + 1, section_id * 2)]
        return lax.ppermute(values, ("pipe", "t"), route)

    columns = HEAD_DIM * (heads + 1)
    share_rows = width // (NZ * NY * NX)

    mask_column = mask.reshape(tokens, 1)
    own_1, raw = values_of(
        upper_values_kernel,
        (is_upper, tensor),
        (own_head, other_head, mask_column, wo, turned_0, turned_1),
        1,
    )
    other_1 = swapped(own_1, 1)
    rows_1 = rows_of(is_upper, own_1, other_1, other_wv_1, raw)
    incoming = lax.ppermute(rows_1, "pipe", [(1, 0)])

    partial_count = lax.ppermute(count, "pipe", [(0, 1)])
    full_count = partial_count + exchanged(partial_count, 2, 0, 0, 1)
    full_count = full_count + exchanged(full_count, 4, 0, 0, 1)
    count_down = lax.ppermute(full_count, "pipe", [(1, 0)])
    chosen_total = jnp.where(upper, full_count, count_down)[0, 0]
    pair_total = pairs * NZ * NY * NX
    scale = LIKELIHOOD_COEF * jnp.asarray(pair_total, F32) / chosen_total.astype(F32)
    bare = jnp.stack([-DPO_BETA * weight_pair, DPO_BETA * weight_pair], axis=1)
    bare_row = jnp.broadcast_to(bare[:, :, None], (pairs, 2, seq)).reshape(1, tokens)
    bare_row = lax.optimization_barrier(bare_row)
    lane = lax.broadcasted_iota(jnp.int32, (1, tokens), 1)
    weight = bare_row - jnp.where(lane // seq % 2 == 0, scale, 0.0)
    weight = weight.reshape(tokens, 1)

    (own_0,) = values_of(lower_values_kernel, (is_lower,), (incoming, wo, turned_0, turned_1), 0)
    other_0 = swapped(own_0, 0)
    other_wv_0 = across(wv, 0)

    below = HEAD_DIM + EXTRA
    turned = pl.pallas_call(
        owners_kernel,
        out_shape=(shaped(width // NY + below, tokens),) * NY,
        in_specs=[SMEM, SMEM, ANY, VMEM, ANY, VMEM, VMEM],
        out_specs=(VMEM,) * NY,
        scratch_shapes=[
            pltpu.VMEM((width, tokens), BF16),
            pltpu.VMEM((4, tokens, 896), BF16),
            pltpu.SemaphoreType.DMA((4,)),
        ],
    )(is_upper, y_index, raw, own_1, incoming, own_0, bare_row)
    blocks = [turned[0]] + [around(turned[s], s) for s in range(1, NY)]

    first_own = ((zi % 2) * NX + xi).astype(jnp.int32).reshape(1)
    group = width // NY // 2

    parts = pl.pallas_call(
        products_kernel,
        out_shape=(shaped(4, share_rows, columns),) * 4,
        grid_spec=pltpu.PrefetchScalarGridSpec(
            num_scalar_prefetch=1,
            grid=(2,),
            in_specs=[SMEM]
            + [pl.BlockSpec((group, tokens), lambda i, own: (i, 0))] * NY
            + [pl.BlockSpec((HEAD_DIM, tokens), lambda i, own: (2 * group // HEAD_DIM, 0))] * NY
            + [pl.BlockSpec((EXTRA, tokens), lambda i, own: ((2 * group + HEAD_DIM) // EXTRA, 0))]
            * NY
            + [pl.BlockSpec((group, tokens), lambda i, own: (i, 0))] * NY
            + [whole_of(tokens, heads * HEAD_DIM)] * NY,
            out_specs=(pl.BlockSpec((2, share_rows, columns), lambda i, own: (i, 0, 0)),) * 4,
            scratch_shapes=[pltpu.VMEM((group, columns), F32)],
        ),
    )(
        first_own, scale.reshape(1), *after(tuple(blocks), other_0), *blocks, *blocks,
        *normed_all, *mixed_all,
    )
    got = [parts[0]] + [over_xz(parts[k], k) for k in (1, 2, 3)]
    parts = pl.pallas_call(
        stage_kernel,
        out_shape=(jax.ShapeDtypeStruct((share_rows, columns), F32),)
        + (shaped(share_rows, columns),) * 3,
        in_specs=[SMEM] + [VMEM] * 4,
        out_specs=(VMEM,) * 4,
    )((zi // 2).astype(jnp.int32).reshape(1), *got)
    got = [parts[0]] + [over_xz(parts[k], k << 2) for k in (1, 2, 3)]

    own_rows = own_rows_of(is_lower, weight, rows_1, own_0, other_0, other_wv_0, incoming)
    start = ((zi * NY + yi) * NX + xi) * share_rows
    own_wv = lax.dynamic_slice_in_dim(wv, start, share_rows, 0).astype(F32)
    own_gain = lax.dynamic_slice_in_dim(gain, start, share_rows, 0).reshape(1, share_rows)
    value_share, output_share, gain_part = pl.pallas_call(
        last_kernel,
        out_shape=(
            jax.ShapeDtypeStruct((1, share_rows, HEAD_DIM), F32),
            jax.ShapeDtypeStruct((1, share_rows, columns - HEAD_DIM), F32),
            jax.ShapeDtypeStruct((1, share_rows), F32),
        ),
        in_specs=[VMEM] * 6,
        out_specs=(VMEM,) * 3,
    )(*got, own_wv, own_gain)
    gain_rows = gain_part + paired(gain_part, "t", NT, 1)
    return own_rows.reshape(1, pairs, 1, seq, width), value_share, output_share, gain_rows


def solution(mesh):
    fine = Mesh(
        mesh.devices.reshape(2, NZ, NY, NX, NT), ("pipe", "z", "y", "x", "t")
    )
    dp = ("z", "y", "x")
    in_specs = (
        P("pipe", dp, None, None, None),
        P("pipe", dp, None, "t", None, None),
        P("pipe", None),
        P("pipe", None, "t"),
        P("pipe", "t", None),
        P(dp, "t", None, None),
        P(dp, None, None),
        P(dp, None),
        P(dp, None),
    )
    out_specs = (
        P("pipe", dp, "t", None, None),
        P("pipe", dp, "t"),
        P("pipe", dp, "t"),
        P("pipe", dp),
    )
    return jax.shard_map(section_step, mesh=fine, in_specs=in_specs, out_specs=out_specs, check_vma=False)
```

```python
import jax
import jax.numpy as jnp
from jax import lax
from jax.experimental import pallas as pl
from jax.experimental.pallas import tpu as pltpu
from jax.sharding import Mesh, PartitionSpec as P


HEAD_DIM = 128
EPSILON = 1e-06
DPO_BETA = 0.25
LIKELIHOOD_COEF = 0.2
NZ, NY, NX, NT = 8, 4, 2, 2
F32, BF16 = jnp.float32, jnp.bfloat16


def paired(block, axis, size, distance, section=None):
    if section is None:
        return lax.ppermute(block, axis, [(i, i ^ distance) for i in range(size)])
    base = section * size
    route = [(base + i, base + (i ^ distance)) for i in range(size)]
    return lax.ppermute(block, ("pipe", axis), route)


def over_xz(block, k):
    route = [
        (z * NX + x, (z ^ (k >> 1)) * NX + (x ^ (k & 1))) for z in range(NZ) for x in range(NX)
    ]
    return lax.ppermute(block, ("z", "x"), route)


VMEM = pl.BlockSpec(memory_space=pltpu.VMEM)
SMEM = pl.BlockSpec(memory_space=pltpu.SMEM)
ANY = pl.BlockSpec(memory_space=pl.ANY)


def dot(a, b, contract):
    return lax.dot_general(a, b, (contract, ((), ())), preferred_element_type=F32)


def rms_of(x):
    return lax.rsqrt(jnp.mean(x * x, axis=-1, keepdims=True) + EPSILON)


def deal(out_refs, source_ref, first_owner):
    size = source_ref.shape[0] // (NZ * NY)
    for s, out_ref in enumerate(out_refs):
        owner = (first_owner + s) % NY
        for z in range(NZ):
            start = pl.multiple_of((z * NY + owner) * size, 16)
            out_ref[z * size : (z + 1) * size] = source_ref[pl.ds(start, size)]


def forward_kernel(y_ref, x_ref, gain_ref, wv_ref, pattern_ref, *refs):
    mixed_ref, turned_ref, normed_refs, normed_t_ref = refs[-7], refs[-6], refs[-5:-1], refs[-1]
    heads, seq = pattern_ref.shape[1:3]
    x = x_ref[...].astype(F32)
    normed = (x * rms_of(x) * gain_ref[...]).astype(BF16)
    normed_t_ref[...] = normed.T
    deal(normed_refs, normed_t_ref, y_ref[0])
    values = dot(normed, wv_ref[...], ((1,), (0,))).astype(BF16)
    for part in range(2):
        at = slice(part * seq, (part + 1) * seq)
        pattern = pattern_ref[part].reshape(heads * seq, seq)
        turned_ref[part] = pattern.T
        mixed = dot(pattern, values[at], ((1,), (0,))).astype(BF16)
        for h in range(heads):
            mixed_ref[at, h * HEAD_DIM : (h + 1) * HEAD_DIM] = mixed[h * seq : (h + 1) * seq]


def add_values(step, dy, wo_ref, turned_refs, values_ref, mixed_ref):
    part = dot(dy, wo_ref[...], ((1,), (1,)))

    @pl.when(step == 0)
    def _():
        mixed_ref[...] = part

    @pl.when(step > 0)
    def _():
        mixed_ref[...] += part

    @pl.when(step == pl.num_programs(0) - 1)
    def _():
        per_pair, seq, depth = turned_refs[0].shape
        for n in range(per_pair * len(turned_refs)):
            at = slice(n * seq, (n + 1) * seq)
            mixed = mixed_ref[at].astype(BF16)
            stacked = jnp.concatenate(
                [mixed[:, h * HEAD_DIM : (h + 1) * HEAD_DIM] for h in range(depth // seq)], axis=0
            )
            turned = turned_refs[n // per_pair][n % per_pair]
            values_ref[at] = dot(turned, stacked, ((1,), (0,))).astype(BF16)


def upper_values_kernel(
    active_ref, tensor_ref, own_ref, other_ref, mask_ref, wo_ref, a_ref, b_ref,
    values_ref, raw_ref, mixed_ref,
):
    @pl.when(active_ref[0] == 1)
    def _():
        first = tensor_ref[0] == 0
        seq = own_ref.shape[1]
        for p in range(own_ref.shape[0]):
            own, other = own_ref[p].astype(F32), other_ref[p].astype(F32)
            for c, head in enumerate((jnp.where(first, own, other), jnp.where(first, other, own))):
                at = slice((2 * p + c) * seq, (2 * p + c + 1) * seq)
                raw_ref[at] = (mask_ref[at] * head).astype(BF16)
        step = pl.program_id(0)
        add_values(step, raw_ref[...], wo_ref, (a_ref, b_ref), values_ref, mixed_ref)


def lower_values_kernel(active_ref, dy_ref, wo_ref, a_ref, b_ref, values_ref, mixed_ref):
    @pl.when(active_ref[0] == 1)
    def _():
        step = pl.program_id(0)
        add_values(step, dy_ref[...], wo_ref, (a_ref, b_ref), values_ref, mixed_ref)


def rows_of_sequence(own_ref, other_ref, own_wv_ref, other_wv_ref, x_ref, gain_ref, dy_ref):
    first = dot(own_ref[...], own_wv_ref[...], ((1,), (1,))).astype(BF16)
    second = dot(other_ref[...], other_wv_ref[...], ((1,), (1,))).astype(BF16)
    scaled = (first.astype(F32) + second.astype(F32)) * gain_ref[...]
    x = x_ref[...].astype(F32)
    inverse = rms_of(x)
    pull = (inverse * inverse * inverse) * jnp.mean(x * scaled, axis=-1, keepdims=True)
    return dy_ref[...].astype(F32) + (inverse * scaled - x * pull)


def rows_kernel(active_ref, *refs):
    @pl.when(active_ref[0] == 1)
    def _():
        refs[-1][...] = rows_of_sequence(*refs[:-1]).astype(BF16)


def own_rows_kernel(active_ref, tensor_ref, weight_ref, done_ref, *refs):
    @pl.when(active_ref[0] == 1)
    def _():
        refs[-1][0] = (weight_ref[...] * rows_of_sequence(*refs[:-1])).astype(BF16)

    @pl.when(active_ref[0] == 0)
    def _():
        refs[-1][0] = (weight_ref[...] * done_ref[...].astype(F32)).astype(BF16)


EXTRA = 16


def owners_kernel(upper_ref, y_ref, *refs):
    (upper_dy, upper_values, lower_dy, lower_values, weight_ref), refs = refs[:5], refs[5:]
    out_refs, turned_ref, dy_buffer, sems = refs[:NY], refs[NY], refs[NY + 1], refs[NY + 2]
    block = dy_buffer.shape[2]

    def turn(dy_hbm, values_ref):
        tokens, width = dy_hbm.shape
        copies = [
            pltpu.make_async_copy(
                dy_hbm.at[:, start : start + block], dy_buffer.at[n], sems.at[n]
            )
            for n, start in enumerate(range(0, width, block))
        ]
        for copy in copies:
            copy.start()
        weight = weight_ref[...]
        high = weight.astype(BF16).astype(F32)
        rest = jnp.zeros((EXTRA - 2, tokens), F32)
        below = jnp.concatenate([high, weight - high, rest], axis=0).astype(BF16)
        values_t = values_ref[...].T
        for out_ref in out_refs:
            rows = out_ref.shape[0]
            out_ref[rows - EXTRA - HEAD_DIM : rows - EXTRA] = values_t
            out_ref[rows - EXTRA :] = below
        for n, copy in enumerate(copies):
            copy.wait()
            turned_ref[n * block : (n + 1) * block] = dy_buffer[n].T

    @pl.when(upper_ref[0] == 1)
    def _():
        turn(upper_dy, upper_values)

    @pl.when(upper_ref[0] == 0)
    def _():
        turn(lower_dy, lower_values)

    deal(out_refs, turned_ref, y_ref[0])


def products_kernel(own_ref, scale_ref, *refs):
    groups, refs = [refs[n * NY : (n + 1) * NY] for n in range(5)], refs[5 * NY :]
    out_refs, total_ref = refs[:-1], refs[-1]
    tokens = groups[0][0].shape[1]
    lane = lax.broadcasted_iota(jnp.int32, (1, tokens), 1)
    chosen = jnp.where(lane // 64 % 2 == 0, scale_ref[0], 0.0)
    value, output = 0.0, 0.0
    for dy_ref, values_ref, weight_ref, normed_ref, mixed_ref in zip(*groups):
        rows = weight_ref[...].astype(F32)
        weight = rows[0:1] + rows[1:2] - chosen
        dy = (weight * dy_ref[...].astype(F32)).astype(BF16)
        values_t = (weight * values_ref[...].astype(F32)).astype(BF16)
        output = output + dot(dy, mixed_ref[...], ((1,), (0,)))
        value = value + dot(normed_ref[...], values_t, ((1,), (1,)))
    total_ref[:, :HEAD_DIM] = value
    total_ref[:, HEAD_DIM:] = output
    count, size = out_refs[0].shape[:2]
    for k, out_ref in enumerate(out_refs):
        for n in range(count):
            start = pl.multiple_of((n * 4 + (own_ref[0] ^ k)) * size, 8)
            out_ref[n] = total_ref[pl.ds(start, size)].astype(BF16)


def stage_kernel(own_ref, a_ref, b_ref, c_ref, d_ref, *out_refs):
    for k, out_ref in enumerate(out_refs):
        j = own_ref[0] ^ k
        total = sum(r[j].astype(F32) for r in (a_ref, b_ref, c_ref, d_ref))
        out_ref[...] = total.astype(out_ref.dtype)


def gain_kernel(a_ref, b_ref, c_ref, d_ref, wv_ref, gain_ref, value_ref, part_ref):
    value = a_ref[...] + sum(r[...].astype(F32) for r in (b_ref, c_ref, d_ref))
    value_ref[0] = value
    row = lax.dot_general(
        jnp.ones((8, HEAD_DIM), F32),
        wv_ref[...] * value,
        (((1,), (1,)), ((), ())),
        precision=lax.Precision.HIGHEST,
        preferred_element_type=F32,
    )
    part_ref[...] = row[:1] / gain_ref[...]


def last_kernel(a_ref, b_ref, c_ref, d_ref, output_ref):
    total = a_ref[:, HEAD_DIM:]
    output_ref[0] = total + sum(r[:, HEAD_DIM:].astype(F32) for r in (b_ref, c_ref, d_ref))


def shaped(*dims):
    return jax.ShapeDtypeStruct(dims, BF16)


def after(block, *others):
    return lax.optimization_barrier((block, *others))[0]


def section_step(
    hidden_in,
    attention_probs,
    norm_gain,
    value_weight,
    output_weight,
    head_grad,
    policy_logprob,
    reference_logprob,
    sequence_bounds,
):
    section = lax.axis_index("pipe")
    zi, yi, xi, ti = (lax.axis_index(a) for a in ("z", "y", "x", "t"))
    pairs, _, seq, width = hidden_in.shape[1:]
    heads = attention_probs.shape[3]
    tokens = pairs * 2 * seq
    gain = norm_gain[0]
    wv = value_weight[0]
    wo = output_weight[0]
    inputs = hidden_in[0]
    pattern = attention_probs[0]
    own_head = head_grad[:, 0]

    other_head = lax.ppermute(own_head, ("pipe", "t"), [(2, 3), (3, 2)])

    positions = jnp.arange(seq, dtype=jnp.int32)
    response_bool = (positions[None, None, :] >= sequence_bounds[:, 0:1, None]) & (
        positions[None, None, :] < sequence_bounds[:, 1:3, None]
    )
    ends = jnp.clip(sequence_bounds[:, :2], 0, seq)
    count = jnp.sum(jnp.maximum(ends[:, 1] - ends[:, 0], 0)).reshape(1, 1)
    count = lax.optimization_barrier(jnp.broadcast_to(count, (8, 128)))

    def exchanged(block, z, y, x, section_id):
        base = NZ * NY * NX
        route = []
        for device in range(base):
            zz, yy, xx = device // (NY * NX), device // NX % NY, device % NX
            other = ((zz ^ z) * NY + (yy ^ y)) * NX + (xx ^ x)
            route.append((section_id * base + device, section_id * base + other))
        return lax.ppermute(block, ("pipe", "z", "y", "x"), route)

    for steps in (((0, 0, 1), (0, 1, 0), (0, 1, 1)), ((1, 0, 0), (0, 2, 0), (1, 2, 0))):
        got = [exchanged(count, *at, 0) for at in steps]
        count = count + sum(got)
    mask = response_bool.astype(F32)
    sequence_logprob = jnp.sum(mask * policy_logprob, axis=-1)
    margin = DPO_BETA * (
        sequence_logprob[:, 0]
        - reference_logprob[:, 0]
        - (sequence_logprob[:, 1] - reference_logprob[:, 1])
    )
    weight_pair = jax.nn.sigmoid(-margin)

    def across(block, section_id):
        pairs_xt = ((0, 3), (3, 0), (1, 2), (2, 1))
        base = section_id * 4
        route = [(base + a, base + b) for a, b in pairs_xt]
        return lax.ppermute(block, ("pipe", "x", "t"), route)

    other_wv_1 = across(wv, 1)

    x = inputs.reshape(tokens, width)
    patterns = pattern.reshape(pairs * 2, heads, seq, seq)
    half = tokens // pairs

    y_index = yi.astype(jnp.int32).reshape(1)

    def forward(p, *earlier):
        return pl.pallas_call(
            forward_kernel,
            out_shape=(shaped(tokens, heads * HEAD_DIM), shaped(2, seq, heads * seq))
            + (shaped(width // NY, tokens),) * NY,
            grid_spec=pltpu.PrefetchScalarGridSpec(
                num_scalar_prefetch=1,
                grid=(1,),
                in_specs=[
                    pl.BlockSpec((half, width), lambda i, y: (p, 0)),
                    pl.BlockSpec((1, width), lambda i, y: (0, 0)),
                    pl.BlockSpec((width, HEAD_DIM), lambda i, y: (0, 0)),
                    pl.BlockSpec((2, heads, seq, seq), lambda i, y: (p, 0, 0, 0)),
                ]
                + [ANY] * len(earlier),
                out_specs=(
                    pl.BlockSpec((half, heads * HEAD_DIM), lambda i, y: (p, 0)),
                    pl.BlockSpec((2, seq, heads * seq), lambda i, y: (0, 0, 0)),
                )
                + (pl.BlockSpec((width // NY, half), lambda i, y: (0, p)),) * NY,
                scratch_shapes=[pltpu.VMEM((width, half), BF16)],
            ),
            input_output_aliases={5: 0, 6: 2, 7: 3, 8: 4, 9: 5} if earlier else {},
        )(y_index, x, norm_gain, wv, patterns, *earlier)

    mixed, turned_0, *normed = forward(0)
    mixed, turned_1, *normed = forward(1, mixed, *normed)

    def around(block, shift):
        return lax.ppermute(block, "y", [(i, (i + shift) % NY) for i in range(NY)])

    mixed_all = [mixed] + [around(mixed, s) for s in range(1, NY)]
    normed_all = [normed[0]] + [around(normed[s], s) for s in range(1, NY)]

    upper = section == 1
    is_upper = upper.astype(jnp.int32).reshape(1)
    is_lower = 1 - is_upper
    tensor = ti.astype(jnp.int32).reshape(1)
    block = width // 4

    def values_of(kernel, scalars, blocks, more):
        def along(*shape):
            rank = len(shape)
            return pl.BlockSpec(shape, lambda i, on, *_: (0,) * (rank - 1) + (i * on[0],))

        def whole(*shape):
            return pl.BlockSpec(shape, lambda i, *_: (0,) * len(shape))

        out_shape = [shaped(tokens, HEAD_DIM)] + [shaped(tokens, width)] * more
        out_specs = [whole(tokens, HEAD_DIM)] + [along(tokens, block)] * more
        in_specs = [
            along(*b.shape[:-1], block) if b.shape[-1] == width else whole(*b.shape)
            for b in blocks
        ]
        return pl.pallas_call(
            kernel,
            out_shape=out_shape,
            grid_spec=pltpu.PrefetchScalarGridSpec(
                num_scalar_prefetch=len(scalars),
                grid=(width // block,),
                in_specs=in_specs,
                out_specs=out_specs,
                scratch_shapes=[pltpu.VMEM((tokens, heads * HEAD_DIM), F32)],
            ),
        )(*scalars, *blocks)

    def whole_of(*shape):
        return pl.BlockSpec(shape, lambda n, *_: (0,) * len(shape))

    def rows_of(active, own, other, other_wv, dy):
        def pick(n, on):
            return (n * on[0], 0)

        return pl.pallas_call(
            rows_kernel,
            out_shape=shaped(tokens, width),
            grid_spec=pltpu.PrefetchScalarGridSpec(
                num_scalar_prefetch=1,
                grid=(pairs * 2,),
                in_specs=[
                    pl.BlockSpec((seq, HEAD_DIM), pick),
                    pl.BlockSpec((seq, HEAD_DIM), pick),
                    whole_of(width, HEAD_DIM),
                    whole_of(width, HEAD_DIM),
                    pl.BlockSpec((seq, width), pick),
                    whole_of(1, width),
                    pl.BlockSpec((seq, width), pick),
                ],
                out_specs=pl.BlockSpec((seq, width), pick),
            ),
        )(active, own, other, wv, other_wv, x, norm_gain, dy)

    def own_rows_of(active, weight, done, own, other, other_wv, dy):
        def pick(n, on, t):
            return ((n * 2 + t[0]) * on[0], 0)

        def mine(n, on, t):
            return (n * 2 + t[0], 0)

        return pl.pallas_call(
            own_rows_kernel,
            out_shape=shaped(1, pairs * seq, width),
            grid_spec=pltpu.PrefetchScalarGridSpec(
                num_scalar_prefetch=2,
                grid=(pairs,),
                in_specs=[
                    pl.BlockSpec((seq, 1), mine),
                    pl.BlockSpec((seq, width), lambda n, on, t: ((n * 2 + t[0]) * (1 - on[0]), 0)),
                    pl.BlockSpec((seq, HEAD_DIM), pick),
                    pl.BlockSpec((seq, HEAD_DIM), pick),
                    whole_of(width, HEAD_DIM),
                    whole_of(width, HEAD_DIM),
                    pl.BlockSpec((seq, width), pick),
                    whole_of(1, width),
                    pl.BlockSpec((seq, width), pick),
                ],
                out_specs=pl.BlockSpec((1, seq, width), lambda n, on, t: (0, n, 0)),
            ),
        )(active, tensor, weight, done, own, other, wv, other_wv, x, norm_gain, dy)

    def swapped(values, section_id):
        route = [(section_id * 2, section_id * 2 + 1), (section_id * 2 + 1, section_id * 2)]
        return lax.ppermute(values, ("pipe", "t"), route)

    columns = HEAD_DIM * (heads + 1)
    share_rows = width // (NZ * NY * NX)

    mask_column = mask.reshape(tokens, 1)
    own_1, raw = values_of(
        upper_values_kernel,
        (is_upper, tensor),
        (own_head, other_head, mask_column, wo, turned_0, turned_1),
        1,
    )
    other_1 = swapped(own_1, 1)
    rows_1 = rows_of(is_upper, own_1, other_1, other_wv_1, raw)
    incoming = lax.ppermute(rows_1, "pipe", [(1, 0)])

    partial_count = lax.ppermute(count, "pipe", [(0, 1)])
    full_count = partial_count + exchanged(partial_count, 2, 0, 0, 1)
    full_count = full_count + exchanged(full_count, 4, 0, 0, 1)
    count_down = lax.ppermute(full_count, "pipe", [(1, 0)])
    chosen_total = jnp.where(upper, full_count, count_down)[0, 0]
    pair_total = pairs * NZ * NY * NX
    scale = LIKELIHOOD_COEF * jnp.asarray(pair_total, F32) / chosen_total.astype(F32)
    bare = jnp.stack([-DPO_BETA * weight_pair, DPO_BETA * weight_pair], axis=1)
    bare_row = jnp.broadcast_to(bare[:, :, None], (pairs, 2, seq)).reshape(1, tokens)
    bare_row = lax.optimization_barrier(bare_row)
    lane = lax.broadcasted_iota(jnp.int32, (1, tokens), 1)
    weight = bare_row - jnp.where(lane // seq % 2 == 0, scale, 0.0)
    weight = weight.reshape(tokens, 1)

    (own_0,) = values_of(lower_values_kernel, (is_lower,), (incoming, wo, turned_0, turned_1), 0)
    other_0 = swapped(own_0, 0)
    other_wv_0 = across(wv, 0)

    below = HEAD_DIM + EXTRA
    turned = pl.pallas_call(
        owners_kernel,
        out_shape=(shaped(width // NY + below, tokens),) * NY,
        in_specs=[SMEM, SMEM, ANY, VMEM, ANY, VMEM, VMEM],
        out_specs=(VMEM,) * NY,
        scratch_shapes=[
            pltpu.VMEM((width, tokens), BF16),
            pltpu.VMEM((4, tokens, 896), BF16),
            pltpu.SemaphoreType.DMA((4,)),
        ],
    )(is_upper, y_index, raw, own_1, incoming, own_0, bare_row)
    blocks = [turned[0]] + [around(turned[s], s) for s in range(1, NY)]

    first_own = ((zi % 2) * NX + xi).astype(jnp.int32).reshape(1)
    group = width // NY // 2

    parts = pl.pallas_call(
        products_kernel,
        out_shape=(shaped(4, share_rows, columns),) * 4,
        grid_spec=pltpu.PrefetchScalarGridSpec(
            num_scalar_prefetch=1,
            grid=(2,),
            in_specs=[SMEM]
            + [pl.BlockSpec((group, tokens), lambda i, own: (i, 0))] * NY
            + [pl.BlockSpec((HEAD_DIM, tokens), lambda i, own: (2 * group // HEAD_DIM, 0))] * NY
            + [pl.BlockSpec((EXTRA, tokens), lambda i, own: ((2 * group + HEAD_DIM) // EXTRA, 0))]
            * NY
            + [pl.BlockSpec((group, tokens), lambda i, own: (i, 0))] * NY
            + [whole_of(tokens, heads * HEAD_DIM)] * NY,
            out_specs=(pl.BlockSpec((2, share_rows, columns), lambda i, own: (i, 0, 0)),) * 4,
            scratch_shapes=[pltpu.VMEM((group, columns), F32)],
        ),
    )(
        first_own, scale.reshape(1), *after(tuple(blocks), other_0), *blocks, *blocks,
        *normed_all, *mixed_all,
    )
    got = [parts[0]] + [over_xz(parts[k], k) for k in (1, 2, 3)]
    parts = pl.pallas_call(
        stage_kernel,
        out_shape=(jax.ShapeDtypeStruct((share_rows, columns), F32),)
        + (shaped(share_rows, columns),) * 3,
        in_specs=[SMEM] + [VMEM] * 4,
        out_specs=(VMEM,) * 4,
    )((zi // 2).astype(jnp.int32).reshape(1), *got)
    got = [parts[0]] + [over_xz(parts[k], k << 2) for k in (1, 2, 3)]

    own_rows = own_rows_of(is_lower, weight, rows_1, own_0, other_0, other_wv_0, incoming)
    start = ((zi * NY + yi) * NX + xi) * share_rows
    own_wv = lax.dynamic_slice_in_dim(wv, start, share_rows, 0).astype(F32)
    own_gain = lax.dynamic_slice_in_dim(gain, start, share_rows, 0).reshape(1, share_rows)
    first_columns = [pl.BlockSpec((share_rows, HEAD_DIM), lambda i: (0, 0))] * 5
    value_share, gain_part = pl.pallas_call(
        gain_kernel,
        out_shape=(
            jax.ShapeDtypeStruct((1, share_rows, HEAD_DIM), F32),
            jax.ShapeDtypeStruct((1, share_rows), F32),
        ),
        grid=(1,),
        in_specs=first_columns + [pl.BlockSpec((1, share_rows), lambda i: (0, 0))],
        out_specs=(
            pl.BlockSpec((1, share_rows, HEAD_DIM), lambda i: (0, 0, 0)),
            pl.BlockSpec((1, share_rows), lambda i: (0, 0)),
        ),
    )(*got, own_wv, own_gain)
    other_part = paired(gain_part, "t", NT, 1)
    output_share = pl.pallas_call(
        last_kernel,
        out_shape=jax.ShapeDtypeStruct((1, share_rows, columns - HEAD_DIM), F32),
        in_specs=[VMEM] * 4,
        out_specs=VMEM,
    )(*got)
    gain_rows = gain_part + other_part
    return own_rows.reshape(1, pairs, 1, seq, width), value_share, output_share, gain_rows


def solution(mesh):
    fine = Mesh(
        mesh.devices.reshape(2, NZ, NY, NX, NT), ("pipe", "z", "y", "x", "t")
    )
    dp = ("z", "y", "x")
    in_specs = (
        P("pipe", dp, None, None, None),
        P("pipe", dp, None, "t", None, None),
        P("pipe", None),
        P("pipe", None, "t"),
        P("pipe", "t", None),
        P(dp, "t", None, None),
        P(dp, None, None),
        P(dp, None),
        P(dp, None),
    )
    out_specs = (
        P("pipe", dp, "t", None, None),
        P("pipe", dp, "t"),
        P("pipe", dp, "t"),
        P("pipe", dp),
    )
    return jax.shard_map(section_step, mesh=fine, in_specs=in_specs, out_specs=out_specs, check_vma=False)
```

```python
import jax
import jax.numpy as jnp
from jax import lax
from jax.experimental import pallas as pl
from jax.experimental.pallas import tpu as pltpu
from jax.sharding import Mesh, PartitionSpec as P


HEAD_DIM = 128
EPSILON = 1e-06
DPO_BETA = 0.25
LIKELIHOOD_COEF = 0.2
NZ, NY, NX, NT = 8, 4, 2, 2
F32, BF16 = jnp.float32, jnp.bfloat16


def paired(block, axis, size, distance, section=None):
    if section is None:
        return lax.ppermute(block, axis, [(i, i ^ distance) for i in range(size)])
    base = section * size
    route = [(base + i, base + (i ^ distance)) for i in range(size)]
    return lax.ppermute(block, ("pipe", axis), route)


def over_xz(block, k):
    route = [
        (z * NX + x, (z ^ (k >> 1)) * NX + (x ^ (k & 1))) for z in range(NZ) for x in range(NX)
    ]
    return lax.ppermute(block, ("z", "x"), route)


VMEM = pl.BlockSpec(memory_space=pltpu.VMEM)
SMEM = pl.BlockSpec(memory_space=pltpu.SMEM)
ANY = pl.BlockSpec(memory_space=pl.ANY)


def dot(a, b, contract):
    return lax.dot_general(a, b, (contract, ((), ())), preferred_element_type=F32)


def rms_of(x):
    return lax.rsqrt(jnp.mean(x * x, axis=-1, keepdims=True) + EPSILON)


def deal(out_refs, source_ref, first_owner):
    size = source_ref.shape[0] // (NZ * NY)
    for s, out_ref in enumerate(out_refs):
        owner = (first_owner + s) % NY
        for z in range(NZ):
            start = pl.multiple_of((z * NY + owner) * size, 16)
            out_ref[z * size : (z + 1) * size] = source_ref[pl.ds(start, size)]


def forward_kernel(y_ref, x_ref, gain_ref, wv_ref, pattern_ref, *refs):
    mixed_ref, turned_ref, normed_refs, normed_t_ref = refs[-7], refs[-6], refs[-5:-1], refs[-1]
    heads, seq = pattern_ref.shape[1:3]
    x = x_ref[...].astype(F32)
    normed = (x * rms_of(x) * gain_ref[...]).astype(BF16)
    normed_t_ref[...] = normed.T
    deal(normed_refs, normed_t_ref, y_ref[0])
    values = dot(normed, wv_ref[...], ((1,), (0,))).astype(BF16)
    for part in range(2):
        at = slice(part * seq, (part + 1) * seq)
        pattern = pattern_ref[part].reshape(heads * seq, seq)
        turned_ref[part] = pattern.T
        mixed = dot(pattern, values[at], ((1,), (0,))).astype(BF16)
        for h in range(heads):
            mixed_ref[at, h * HEAD_DIM : (h + 1) * HEAD_DIM] = mixed[h * seq : (h + 1) * seq]


def add_values(step, dy, wo_ref, turned_refs, values_ref, mixed_ref):
    part = dot(dy, wo_ref[...], ((1,), (1,)))

    @pl.when(step == 0)
    def _():
        mixed_ref[...] = part

    @pl.when(step > 0)
    def _():
        mixed_ref[...] += part

    @pl.when(step == pl.num_programs(0) - 1)
    def _():
        per_pair, seq, depth = turned_refs[0].shape
        for n in range(per_pair * len(turned_refs)):
            at = slice(n * seq, (n + 1) * seq)
            mixed = mixed_ref[at].astype(BF16)
            stacked = jnp.concatenate(
                [mixed[:, h * HEAD_DIM : (h + 1) * HEAD_DIM] for h in range(depth // seq)], axis=0
            )
            turned = turned_refs[n // per_pair][n % per_pair]
            values_ref[at] = dot(turned, stacked, ((1,), (0,))).astype(BF16)


def upper_values_kernel(
    active_ref, tensor_ref, own_ref, other_ref, mask_ref, wo_ref, a_ref, b_ref,
    values_ref, raw_ref, mixed_ref,
):
    @pl.when(active_ref[0] == 1)
    def _():
        first = tensor_ref[0] == 0
        seq = own_ref.shape[1]
        for p in range(own_ref.shape[0]):
            own, other = own_ref[p].astype(F32), other_ref[p].astype(F32)
            for c, head in enumerate((jnp.where(first, own, other), jnp.where(first, other, own))):
                at = slice((2 * p + c) * seq, (2 * p + c + 1) * seq)
                raw_ref[at] = (mask_ref[at] * head).astype(BF16)
        step = pl.program_id(0)
        add_values(step, raw_ref[...], wo_ref, (a_ref, b_ref), values_ref, mixed_ref)


def lower_values_kernel(active_ref, dy_ref, wo_ref, a_ref, b_ref, values_ref, mixed_ref):
    @pl.when(active_ref[0] == 1)
    def _():
        step = pl.program_id(0)
        add_values(step, dy_ref[...], wo_ref, (a_ref, b_ref), values_ref, mixed_ref)


def rows_of_sequence(own_ref, other_ref, own_wv_ref, other_wv_ref, x_ref, gain_ref, dy_ref):
    first = dot(own_ref[...], own_wv_ref[...], ((1,), (1,))).astype(BF16)
    second = dot(other_ref[...], other_wv_ref[...], ((1,), (1,))).astype(BF16)
    scaled = (first.astype(F32) + second.astype(F32)) * gain_ref[...]
    x = x_ref[...].astype(F32)
    inverse = rms_of(x)
    pull = (inverse * inverse * inverse) * jnp.mean(x * scaled, axis=-1, keepdims=True)
    return dy_ref[...].astype(F32) + (inverse * scaled - x * pull)


def rows_kernel(active_ref, *refs):
    @pl.when(active_ref[0] == 1)
    def _():
        refs[-1][...] = rows_of_sequence(*refs[:-1]).astype(BF16)


def own_rows_kernel(active_ref, tensor_ref, weight_ref, done_ref, *refs):
    @pl.when(active_ref[0] == 1)
    def _():
        refs[-1][0] = (weight_ref[...] * rows_of_sequence(*refs[:-1])).astype(BF16)

    @pl.when(active_ref[0] == 0)
    def _():
        refs[-1][0] = (weight_ref[...] * done_ref[...].astype(F32)).astype(BF16)


EXTRA = 16


def owners_kernel(active_ref, y_ref, dy_hbm, values_ref, weight_ref, *refs):
    out_refs, turned_ref, dy_buffer, sems = refs[:NY], refs[NY], refs[NY + 1], refs[NY + 2]
    block = dy_buffer.shape[2]

    @pl.when(active_ref[0] == 1)
    def _():
        tokens, width = dy_hbm.shape
        copies = [
            pltpu.make_async_copy(
                dy_hbm.at[:, start : start + block], dy_buffer.at[n], sems.at[n]
            )
            for n, start in enumerate(range(0, width, block))
        ]
        for copy in copies:
            copy.start()
        weight = weight_ref[...]
        high = weight.astype(BF16).astype(F32)
        rest = jnp.zeros((EXTRA - 2, tokens), F32)
        below = jnp.concatenate([high, weight - high, rest], axis=0).astype(BF16)
        values_t = values_ref[...].T
        for out_ref in out_refs:
            rows = out_ref.shape[0]
            out_ref[rows - EXTRA - HEAD_DIM : rows - EXTRA] = values_t
            out_ref[rows - EXTRA :] = below
        for n, copy in enumerate(copies):
            copy.wait()
            turned_ref[n * block : (n + 1) * block] = dy_buffer[n].T
        deal(out_refs, turned_ref, y_ref[0])


def products_kernel(own_ref, upper_ref, scale_ref, *refs):
    groups, refs = [refs[n * NY : (n + 1) * NY] for n in range(8)], refs[8 * NY :]
    out_refs, total_ref = refs[:-1], refs[-1]
    tokens = groups[0][0].shape[1]
    lane = lax.broadcasted_iota(jnp.int32, (1, tokens), 1)
    chosen = jnp.where(lane // 64 % 2 == 0, scale_ref[0], 0.0)

    def add_up(messages):
        value, output = 0.0, 0.0
        for dy_ref, values_ref, weight_ref, normed_ref, mixed_ref in zip(*messages, *groups[6:]):
            rows = weight_ref[...].astype(F32)
            weight = rows[0:1] + rows[1:2] - chosen
            dy = (weight * dy_ref[...].astype(F32)).astype(BF16)
            values_t = (weight * values_ref[...].astype(F32)).astype(BF16)
            output = output + dot(dy, mixed_ref[...], ((1,), (0,)))
            value = value + dot(normed_ref[...], values_t, ((1,), (1,)))
        total_ref[:, :HEAD_DIM] = value
        total_ref[:, HEAD_DIM:] = output

    @pl.when(upper_ref[0] == 1)
    def _():
        add_up(groups[:3])

    @pl.when(upper_ref[0] == 0)
    def _():
        add_up(groups[3:6])

    count, size = out_refs[0].shape[:2]
    for k, out_ref in enumerate(out_refs):
        for n in range(count):
            start = pl.multiple_of((n * 4 + (own_ref[0] ^ k)) * size, 8)
            out_ref[n] = total_ref[pl.ds(start, size)].astype(BF16)


def stage_kernel(own_ref, a_ref, b_ref, c_ref, d_ref, *out_refs):
    for k, out_ref in enumerate(out_refs):
        j = own_ref[0] ^ k
        total = sum(r[j].astype(F32) for r in (a_ref, b_ref, c_ref, d_ref))
        out_ref[...] = total.astype(out_ref.dtype)


def gain_kernel(a_ref, b_ref, c_ref, d_ref, wv_ref, gain_ref, value_ref, part_ref):
    value = a_ref[...] + sum(r[...].astype(F32) for r in (b_ref, c_ref, d_ref))
    value_ref[0] = value
    row = lax.dot_general(
        jnp.ones((8, HEAD_DIM), F32),
        wv_ref[...] * value,
        (((1,), (1,)), ((), ())),
        precision=lax.Precision.HIGHEST,
        preferred_element_type=F32,
    )
    part_ref[...] = row[:1] / gain_ref[...]


def last_kernel(a_ref, b_ref, c_ref, d_ref, output_ref):
    total = a_ref[:, HEAD_DIM:]
    output_ref[0] = total + sum(r[:, HEAD_DIM:].astype(F32) for r in (b_ref, c_ref, d_ref))


def shaped(*dims):
    return jax.ShapeDtypeStruct(dims, BF16)


def after(block, *others):
    return lax.optimization_barrier((block, *others))[0]


def section_step(
    hidden_in,
    attention_probs,
    norm_gain,
    value_weight,
    output_weight,
    head_grad,
    policy_logprob,
    reference_logprob,
    sequence_bounds,
):
    section = lax.axis_index("pipe")
    zi, yi, xi, ti = (lax.axis_index(a) for a in ("z", "y", "x", "t"))
    pairs, _, seq, width = hidden_in.shape[1:]
    heads = attention_probs.shape[3]
    tokens = pairs * 2 * seq
    gain = norm_gain[0]
    wv = value_weight[0]
    wo = output_weight[0]
    inputs = hidden_in[0]
    pattern = attention_probs[0]
    own_head = head_grad[:, 0]

    other_head = lax.ppermute(own_head, ("pipe", "t"), [(2, 3), (3, 2)])

    positions = jnp.arange(seq, dtype=jnp.int32)
    response_bool = (positions[None, None, :] >= sequence_bounds[:, 0:1, None]) & (
        positions[None, None, :] < sequence_bounds[:, 1:3, None]
    )
    ends = jnp.clip(sequence_bounds[:, :2], 0, seq)
    count = jnp.sum(jnp.maximum(ends[:, 1] - ends[:, 0], 0)).reshape(1, 1)
    count = lax.optimization_barrier(jnp.broadcast_to(count, (8, 128)))

    def exchanged(block, z, y, x, section_id):
        base = NZ * NY * NX
        route = []
        for device in range(base):
            zz, yy, xx = device // (NY * NX), device // NX % NY, device % NX
            other = ((zz ^ z) * NY + (yy ^ y)) * NX + (xx ^ x)
            route.append((section_id * base + device, section_id * base + other))
        return lax.ppermute(block, ("pipe", "z", "y", "x"), route)

    for steps in (((0, 0, 1), (0, 1, 0), (0, 1, 1)), ((1, 0, 0), (0, 2, 0), (1, 2, 0))):
        got = [exchanged(count, *at, 0) for at in steps]
        count = count + sum(got)
    mask = response_bool.astype(F32)
    sequence_logprob = jnp.sum(mask * policy_logprob, axis=-1)
    margin = DPO_BETA * (
        sequence_logprob[:, 0]
        - reference_logprob[:, 0]
        - (sequence_logprob[:, 1] - reference_logprob[:, 1])
    )
    weight_pair = jax.nn.sigmoid(-margin)

    def across(block, section_id):
        pairs_xt = ((0, 3), (3, 0), (1, 2), (2, 1))
        base = section_id * 4
        route = [(base + a, base + b) for a, b in pairs_xt]
        return lax.ppermute(block, ("pipe", "x", "t"), route)

    other_wv_1 = across(wv, 1)

    x = inputs.reshape(tokens, width)
    patterns = pattern.reshape(pairs * 2, heads, seq, seq)
    half = tokens // pairs

    y_index = yi.astype(jnp.int32).reshape(1)

    def forward(p, *earlier):
        return pl.pallas_call(
            forward_kernel,
            out_shape=(shaped(tokens, heads * HEAD_DIM), shaped(2, seq, heads * seq))
            + (shaped(width // NY, tokens),) * NY,
            grid_spec=pltpu.PrefetchScalarGridSpec(
                num_scalar_prefetch=1,
                grid=(1,),
                in_specs=[
                    pl.BlockSpec((half, width), lambda i, y: (p, 0)),
                    pl.BlockSpec((1, width), lambda i, y: (0, 0)),
                    pl.BlockSpec((width, HEAD_DIM), lambda i, y: (0, 0)),
                    pl.BlockSpec((2, heads, seq, seq), lambda i, y: (p, 0, 0, 0)),
                ]
                + [ANY] * len(earlier),
                out_specs=(
                    pl.BlockSpec((half, heads * HEAD_DIM), lambda i, y: (p, 0)),
                    pl.BlockSpec((2, seq, heads * seq), lambda i, y: (0, 0, 0)),
                )
                + (pl.BlockSpec((width // NY, half), lambda i, y: (0, p)),) * NY,
                scratch_shapes=[pltpu.VMEM((width, half), BF16)],
            ),
            input_output_aliases={5: 0, 6: 2, 7: 3, 8: 4, 9: 5} if earlier else {},
        )(y_index, x, norm_gain, wv, patterns, *earlier)

    mixed, turned_0, *normed = forward(0)
    mixed, turned_1, *normed = forward(1, mixed, *normed)

    def around(block, shift, sections=(0, 1)):
        route = [(n * NY + i, n * NY + (i + shift) % NY) for n in sections for i in range(NY)]
        return lax.ppermute(block, ("pipe", "y"), route)

    mixed_all = [mixed] + [around(mixed, s) for s in range(1, NY)]
    normed_all = [normed[0]] + [around(normed[s], s) for s in range(1, NY)]

    upper = section == 1
    is_upper = upper.astype(jnp.int32).reshape(1)
    is_lower = 1 - is_upper
    tensor = ti.astype(jnp.int32).reshape(1)
    block = width // 2

    def values_of(kernel, scalars, blocks, more):
        def along(*shape):
            rank = len(shape)
            return pl.BlockSpec(shape, lambda i, on, *_: (0,) * (rank - 1) + (i * on[0],))

        def whole(*shape):
            return pl.BlockSpec(shape, lambda i, *_: (0,) * len(shape))

        out_shape = [shaped(tokens, HEAD_DIM)] + [shaped(tokens, width)] * more
        out_specs = [whole(tokens, HEAD_DIM)] + [along(tokens, block)] * more
        in_specs = [
            along(*b.shape[:-1], block) if b.shape[-1] == width else whole(*b.shape)
            for b in blocks
        ]
        return pl.pallas_call(
            kernel,
            out_shape=out_shape,
            grid_spec=pltpu.PrefetchScalarGridSpec(
                num_scalar_prefetch=len(scalars),
                grid=(width // block,),
                in_specs=in_specs,
                out_specs=out_specs,
                scratch_shapes=[pltpu.VMEM((tokens, heads * HEAD_DIM), F32)],
            ),
        )(*scalars, *blocks)

    def whole_of(*shape):
        return pl.BlockSpec(shape, lambda n, *_: (0,) * len(shape))

    def rows_of(active, own, other, other_wv, dy):
        def pick(n, on):
            return (n * on[0], 0)

        return pl.pallas_call(
            rows_kernel,
            out_shape=shaped(tokens, width),
            grid_spec=pltpu.PrefetchScalarGridSpec(
                num_scalar_prefetch=1,
                grid=(pairs * 2,),
                in_specs=[
                    pl.BlockSpec((seq, HEAD_DIM), pick),
                    pl.BlockSpec((seq, HEAD_DIM), pick),
                    whole_of(width, HEAD_DIM),
                    whole_of(width, HEAD_DIM),
                    pl.BlockSpec((seq, width), pick),
                    whole_of(1, width),
                    pl.BlockSpec((seq, width), pick),
                ],
                out_specs=pl.BlockSpec((seq, width), pick),
            ),
        )(active, own, other, wv, other_wv, x, norm_gain, dy)

    def own_rows_of(active, weight, done, own, other, other_wv, dy):
        def pick(n, on, t):
            return ((n * 2 + t[0]) * on[0], 0)

        def mine(n, on, t):
            return (n * 2 + t[0], 0)

        return pl.pallas_call(
            own_rows_kernel,
            out_shape=shaped(1, pairs * seq, width),
            grid_spec=pltpu.PrefetchScalarGridSpec(
                num_scalar_prefetch=2,
                grid=(pairs,),
                in_specs=[
                    pl.BlockSpec((seq, 1), mine),
                    pl.BlockSpec((seq, width), lambda n, on, t: ((n * 2 + t[0]) * (1 - on[0]), 0)),
                    pl.BlockSpec((seq, HEAD_DIM), pick),
                    pl.BlockSpec((seq, HEAD_DIM), pick),
                    whole_of(width, HEAD_DIM),
                    whole_of(width, HEAD_DIM),
                    pl.BlockSpec((seq, width), pick),
                    whole_of(1, width),
                    pl.BlockSpec((seq, width), pick),
                ],
                out_specs=pl.BlockSpec((1, seq, width), lambda n, on, t: (0, n, 0)),
            ),
        )(active, tensor, weight, done, own, other, wv, other_wv, x, norm_gain, dy)

    def swapped(values, section_id):
        route = [(section_id * 2, section_id * 2 + 1), (section_id * 2 + 1, section_id * 2)]
        return lax.ppermute(values, ("pipe", "t"), route)

    columns = HEAD_DIM * (heads + 1)
    share_rows = width // (NZ * NY * NX)

    mask_column = mask.reshape(tokens, 1)
    own_1, raw = values_of(
        upper_values_kernel,
        (is_upper, tensor),
        (own_head, other_head, mask_column, wo, turned_0, turned_1),
        1,
    )
    other_1 = swapped(own_1, 1)
    rows_1 = rows_of(is_upper, own_1, other_1, other_wv_1, raw)
    incoming = lax.ppermute(rows_1, "pipe", [(1, 0)])

    below = HEAD_DIM + EXTRA
    bare = jnp.stack([-DPO_BETA * weight_pair, DPO_BETA * weight_pair], axis=1)
    bare_row = jnp.broadcast_to(bare[:, :, None], (pairs, 2, seq)).reshape(1, tokens)
    bare_row = lax.optimization_barrier(bare_row)

    def sent(active, dy, values, section_id):
        turned = pl.pallas_call(
            owners_kernel,
            out_shape=(shaped(width // NY + below, tokens),) * NY,
            in_specs=[SMEM, SMEM, ANY, VMEM, VMEM],
            out_specs=(VMEM,) * NY,
            scratch_shapes=[
                pltpu.VMEM((width, tokens), BF16),
                pltpu.VMEM((4, tokens, 896), BF16),
                pltpu.SemaphoreType.DMA((4,)),
            ],
        )(active, y_index, dy, values, bare_row)
        return [turned[0]] + [around(turned[s], s, (section_id,)) for s in range(1, NY)]

    blocks_1 = sent(is_upper, raw, own_1, 1)

    partial_count = lax.ppermute(count, "pipe", [(0, 1)])
    full_count = partial_count + exchanged(partial_count, 2, 0, 0, 1)
    full_count = full_count + exchanged(full_count, 4, 0, 0, 1)
    count_down = lax.ppermute(full_count, "pipe", [(1, 0)])
    chosen_total = jnp.where(upper, full_count, count_down)[0, 0]
    pair_total = pairs * NZ * NY * NX
    scale = LIKELIHOOD_COEF * jnp.asarray(pair_total, F32) / chosen_total.astype(F32)
    lane = lax.broadcasted_iota(jnp.int32, (1, tokens), 1)
    weight = bare_row - jnp.where(lane // seq % 2 == 0, scale, 0.0)
    weight = weight.reshape(tokens, 1)

    (own_0,) = values_of(lower_values_kernel, (is_lower,), (incoming, wo, turned_0, turned_1), 0)
    other_0 = swapped(own_0, 0)
    other_wv_0 = across(wv, 0)

    blocks_0 = sent(is_lower, incoming, own_0, 0)

    first_own = ((zi % 2) * NX + xi).astype(jnp.int32).reshape(1)
    group = width // NY // 2

    def message_specs(wanted):
        def step(i, on):
            return i * on[0] if wanted else i * (1 - on[0])

        at = 2 * group
        return (
            [pl.BlockSpec((group, tokens), lambda i, own, on: (step(i, on), 0))] * NY
            + [pl.BlockSpec((HEAD_DIM, tokens), lambda i, own, on: (at // HEAD_DIM, 0))] * NY
            + [pl.BlockSpec((EXTRA, tokens), lambda i, own, on: ((at + HEAD_DIM) // EXTRA, 0))] * NY
        )

    parts = pl.pallas_call(
        products_kernel,
        out_shape=(shaped(4, share_rows, columns),) * 4,
        grid_spec=pltpu.PrefetchScalarGridSpec(
            num_scalar_prefetch=2,
            grid=(2,),
            in_specs=[SMEM]
            + message_specs(True)
            + message_specs(False)
            + [pl.BlockSpec((group, tokens), lambda i, own, on: (i, 0))] * NY
            + [whole_of(tokens, heads * HEAD_DIM)] * NY,
            out_specs=(pl.BlockSpec((2, share_rows, columns), lambda i, own, on: (i, 0, 0)),)
            * 4,
            scratch_shapes=[pltpu.VMEM((group, columns), F32)],
        ),
    )(
        first_own, is_upper, scale.reshape(1), *blocks_1, *blocks_1, *blocks_1,
        *after(tuple(blocks_0), other_0), *blocks_0, *blocks_0, *normed_all, *mixed_all,
    )
    got = [parts[0]] + [over_xz(parts[k], k) for k in (1, 2, 3)]
    parts = pl.pallas_call(
        stage_kernel,
        out_shape=(jax.ShapeDtypeStruct((share_rows, columns), F32),)
        + (shaped(share_rows, columns),) * 3,
        in_specs=[SMEM] + [VMEM] * 4,
        out_specs=(VMEM,) * 4,
    )((zi // 2).astype(jnp.int32).reshape(1), *got)
    got = [parts[0]] + [over_xz(parts[k], k << 2) for k in (1, 2, 3)]

    own_rows = own_rows_of(is_lower, weight, rows_1, own_0, other_0, other_wv_0, incoming)
    start = ((zi * NY + yi) * NX + xi) * share_rows
    own_wv = lax.dynamic_slice_in_dim(wv, start, share_rows, 0).astype(F32)
    own_gain = lax.dynamic_slice_in_dim(gain, start, share_rows, 0).reshape(1, share_rows)
    first_columns = [pl.BlockSpec((share_rows, HEAD_DIM), lambda i: (0, 0))] * 5
    value_share, gain_part = pl.pallas_call(
        gain_kernel,
        out_shape=(
            jax.ShapeDtypeStruct((1, share_rows, HEAD_DIM), F32),
            jax.ShapeDtypeStruct((1, share_rows), F32),
        ),
        grid=(1,),
        in_specs=first_columns + [pl.BlockSpec((1, share_rows), lambda i: (0, 0))],
        out_specs=(
            pl.BlockSpec((1, share_rows, HEAD_DIM), lambda i: (0, 0, 0)),
            pl.BlockSpec((1, share_rows), lambda i: (0, 0)),
        ),
    )(*got, own_wv, own_gain)
    other_part = paired(gain_part, "t", NT, 1)
    output_share = pl.pallas_call(
        last_kernel,
        out_shape=jax.ShapeDtypeStruct((1, share_rows, columns - HEAD_DIM), F32),
        in_specs=[VMEM] * 4,
        out_specs=VMEM,
    )(*got)
    gain_rows = gain_part + other_part
    return own_rows.reshape(1, pairs, 1, seq, width), value_share, output_share, gain_rows


def solution(mesh):
    fine = Mesh(
        mesh.devices.reshape(2, NZ, NY, NX, NT), ("pipe", "z", "y", "x", "t")
    )
    dp = ("z", "y", "x")
    in_specs = (
        P("pipe", dp, None, None, None),
        P("pipe", dp, None, "t", None, None),
        P("pipe", None),
        P("pipe", None, "t"),
        P("pipe", "t", None),
        P(dp, "t", None, None),
        P(dp, None, None),
        P(dp, None),
        P(dp, None),
    )
    out_specs = (
        P("pipe", dp, "t", None, None),
        P("pipe", dp, "t"),
        P("pipe", dp, "t"),
        P("pipe", dp),
    )
    return jax.shard_map(section_step, mesh=fine, in_specs=in_specs, out_specs=out_specs, check_vma=False)
```

```python
import jax
import jax.numpy as jnp
from jax import lax
from jax.experimental import pallas as pl
from jax.experimental.pallas import tpu as pltpu
from jax.sharding import Mesh, PartitionSpec as P


HEAD_DIM = 128
EPSILON = 1e-06
DPO_BETA = 0.25
LIKELIHOOD_COEF = 0.2
NZ, NY, NX, NT = 8, 4, 2, 2
F32, BF16 = jnp.float32, jnp.bfloat16


def paired(block, axis, size, distance, section=None):
    if section is None:
        return lax.ppermute(block, axis, [(i, i ^ distance) for i in range(size)])
    base = section * size
    route = [(base + i, base + (i ^ distance)) for i in range(size)]
    return lax.ppermute(block, ("pipe", axis), route)


def over_xz(block, k):
    route = [
        (z * NX + x, (z ^ (k >> 1)) * NX + (x ^ (k & 1))) for z in range(NZ) for x in range(NX)
    ]
    return lax.ppermute(block, ("z", "x"), route)


VMEM = pl.BlockSpec(memory_space=pltpu.VMEM)
SMEM = pl.BlockSpec(memory_space=pltpu.SMEM)
ANY = pl.BlockSpec(memory_space=pl.ANY)


def dot(a, b, contract):
    return lax.dot_general(a, b, (contract, ((), ())), preferred_element_type=F32)


def rms_of(x):
    return lax.rsqrt(jnp.mean(x * x, axis=-1, keepdims=True) + EPSILON)


def deal(out_refs, source_ref, first_owner):
    size = source_ref.shape[0] // (NZ * NY)
    for s, out_ref in enumerate(out_refs):
        owner = (first_owner + s) % NY
        for z in range(NZ):
            start = pl.multiple_of((z * NY + owner) * size, 16)
            out_ref[z * size : (z + 1) * size] = source_ref[pl.ds(start, size)]


def forward_kernel(y_ref, x_ref, gain_ref, wv_ref, pattern_ref, *refs):
    turned_ref, operand_refs, normed_t_ref, mixed_ref = refs[-7], refs[-6:-2], refs[-2], refs[-1]
    heads, seq = pattern_ref.shape[1:3]
    x = x_ref[...].astype(F32)
    normed = (x * rms_of(x) * gain_ref[...]).astype(BF16)
    normed_t_ref[...] = normed.T
    values = dot(normed, wv_ref[...], ((1,), (0,))).astype(BF16)
    for part in range(2):
        at = slice(part * seq, (part + 1) * seq)
        pattern = pattern_ref[part].reshape(heads * seq, seq)
        turned_ref[part] = pattern.T
        mixed = dot(pattern, values[at], ((1,), (0,))).astype(BF16)
        for h in range(heads):
            mixed_ref[at, h * HEAD_DIM : (h + 1) * HEAD_DIM] = mixed[h * seq : (h + 1) * seq]
    mixed_t = mixed_ref[...].T
    above = mixed_t.shape[0]
    for operand_ref in operand_refs:
        operand_ref[:above] = mixed_t
    deal([r.at[above:] for r in operand_refs], normed_t_ref, y_ref[0])


def add_values(step, dy, wo_ref, turned_refs, values_ref, mixed_ref):
    part = dot(dy, wo_ref[...], ((1,), (1,)))

    @pl.when(step == 0)
    def _():
        mixed_ref[...] = part

    @pl.when(step > 0)
    def _():
        mixed_ref[...] += part

    @pl.when(step == pl.num_programs(0) - 1)
    def _():
        per_pair, seq, depth = turned_refs[0].shape
        for n in range(per_pair * len(turned_refs)):
            at = slice(n * seq, (n + 1) * seq)
            mixed = mixed_ref[at].astype(BF16)
            stacked = jnp.concatenate(
                [mixed[:, h * HEAD_DIM : (h + 1) * HEAD_DIM] for h in range(depth // seq)], axis=0
            )
            turned = turned_refs[n // per_pair][n % per_pair]
            values_ref[at] = dot(turned, stacked, ((1,), (0,))).astype(BF16)


def upper_values_kernel(
    active_ref, tensor_ref, own_ref, other_ref, mask_ref, wo_ref, a_ref, b_ref,
    values_ref, raw_ref, mixed_ref,
):
    @pl.when(active_ref[0] == 1)
    def _():
        first = tensor_ref[0] == 0
        seq = own_ref.shape[1]
        for p in range(own_ref.shape[0]):
            own, other = own_ref[p].astype(F32), other_ref[p].astype(F32)
            for c, head in enumerate((jnp.where(first, own, other), jnp.where(first, other, own))):
                at = slice((2 * p + c) * seq, (2 * p + c + 1) * seq)
                raw_ref[at] = (mask_ref[at] * head).astype(BF16)
        step = pl.program_id(0)
        add_values(step, raw_ref[...], wo_ref, (a_ref, b_ref), values_ref, mixed_ref)


def lower_values_kernel(active_ref, dy_ref, wo_ref, a_ref, b_ref, values_ref, mixed_ref):
    @pl.when(active_ref[0] == 1)
    def _():
        step = pl.program_id(0)
        add_values(step, dy_ref[...], wo_ref, (a_ref, b_ref), values_ref, mixed_ref)


def rows_of_sequence(own_ref, other_ref, own_wv_ref, other_wv_ref, x_ref, gain_ref, dy_ref):
    first = dot(own_ref[...], own_wv_ref[...], ((1,), (1,))).astype(BF16)
    second = dot(other_ref[...], other_wv_ref[...], ((1,), (1,))).astype(BF16)
    scaled = (first.astype(F32) + second.astype(F32)) * gain_ref[...]
    x = x_ref[...].astype(F32)
    inverse = rms_of(x)
    pull = (inverse * inverse * inverse) * jnp.mean(x * scaled, axis=-1, keepdims=True)
    return dy_ref[...].astype(F32) + (inverse * scaled - x * pull)


def rows_kernel(active_ref, *refs):
    @pl.when(active_ref[0] == 1)
    def _():
        refs[-1][...] = rows_of_sequence(*refs[:-1]).astype(BF16)


def own_rows_kernel(active_ref, tensor_ref, weight_ref, done_ref, *refs):
    @pl.when(active_ref[0] == 1)
    def _():
        refs[-1][0] = (weight_ref[...] * rows_of_sequence(*refs[:-1])).astype(BF16)

    @pl.when(active_ref[0] == 0)
    def _():
        refs[-1][0] = (weight_ref[...] * done_ref[...].astype(F32)).astype(BF16)


EXTRA = 16


def owners_kernel(upper_ref, y_ref, *refs):
    (upper_dy, upper_values, lower_dy, lower_values, weight_ref), refs = refs[:5], refs[5:]
    out_refs, turned_ref, dy_buffer, sems = refs[:NY], refs[NY], refs[NY + 1], refs[NY + 2]
    block = dy_buffer.shape[2]

    def turn(dy_hbm, values_ref):
        tokens, width = dy_hbm.shape
        copies = [
            pltpu.make_async_copy(
                dy_hbm.at[:, start : start + block], dy_buffer.at[n], sems.at[n]
            )
            for n, start in enumerate(range(0, width, block))
        ]
        for copy in copies:
            copy.start()
        weight = weight_ref[...]
        high = weight.astype(BF16).astype(F32)
        rest = jnp.zeros((EXTRA - 2, tokens), F32)
        below = jnp.concatenate([high, weight - high, rest], axis=0).astype(BF16)
        values_t = values_ref[...].T
        for out_ref in out_refs:
            rows = out_ref.shape[0]
            out_ref[rows - EXTRA - HEAD_DIM : rows - EXTRA] = values_t
            out_ref[rows - EXTRA :] = below
        for n, copy in enumerate(copies):
            copy.wait()
            turned_ref[n * block : (n + 1) * block] = dy_buffer[n].T

    @pl.when(upper_ref[0] == 1)
    def _():
        turn(upper_dy, upper_values)

    @pl.when(upper_ref[0] == 0)
    def _():
        turn(lower_dy, lower_values)

    deal(out_refs, turned_ref, y_ref[0])


def products_kernel(own_ref, scale_ref, *refs):
    groups, refs = [refs[n * NY : (n + 1) * NY] for n in range(5)], refs[5 * NY :]
    out_refs, total_ref = refs[:-1], refs[-1]
    tokens = groups[0][0].shape[1]
    lane = lax.broadcasted_iota(jnp.int32, (1, tokens), 1)
    chosen = jnp.where(lane // 64 % 2 == 0, scale_ref[0], 0.0)
    value, output = 0.0, 0.0
    for dy_ref, values_ref, weight_ref, normed_ref, mixed_ref in zip(*groups):
        rows = weight_ref[...].astype(F32)
        weight = rows[0:1] + rows[1:2] - chosen
        dy = (weight * dy_ref[...].astype(F32)).astype(BF16)
        values_t = (weight * values_ref[...].astype(F32)).astype(BF16)
        output = output + dot(dy, mixed_ref[...], ((1,), (1,)))
        value = value + dot(normed_ref[...], values_t, ((1,), (1,)))
    total_ref[:, :HEAD_DIM] = value
    total_ref[:, HEAD_DIM:] = output
    count, size = out_refs[0].shape[:2]
    for k, out_ref in enumerate(out_refs):
        for n in range(count):
            start = pl.multiple_of((n * 4 + (own_ref[0] ^ k)) * size, 8)
            out_ref[n] = total_ref[pl.ds(start, size)].astype(BF16)


def stage_kernel(own_ref, a_ref, b_ref, c_ref, d_ref, *out_refs):
    for k, out_ref in enumerate(out_refs):
        j = own_ref[0] ^ k
        total = sum(r[j].astype(F32) for r in (a_ref, b_ref, c_ref, d_ref))
        out_ref[...] = total.astype(out_ref.dtype)


def gain_kernel(a_ref, b_ref, c_ref, d_ref, wv_ref, gain_ref, value_ref, part_ref):
    value = a_ref[...] + sum(r[...].astype(F32) for r in (b_ref, c_ref, d_ref))
    value_ref[0] = value
    row = lax.dot_general(
        jnp.ones((8, HEAD_DIM), F32),
        wv_ref[...] * value,
        (((1,), (1,)), ((), ())),
        precision=lax.Precision.HIGHEST,
        preferred_element_type=F32,
    )
    part_ref[...] = row[:1] / gain_ref[...]


def last_kernel(a_ref, b_ref, c_ref, d_ref, output_ref):
    total = a_ref[:, HEAD_DIM:]
    output_ref[0] = total + sum(r[:, HEAD_DIM:].astype(F32) for r in (b_ref, c_ref, d_ref))


def shaped(*dims):
    return jax.ShapeDtypeStruct(dims, BF16)


def after(block, *others):
    return lax.optimization_barrier((block, *others))[0]


def section_step(
    hidden_in,
    attention_probs,
    norm_gain,
    value_weight,
    output_weight,
    head_grad,
    policy_logprob,
    reference_logprob,
    sequence_bounds,
):
    section = lax.axis_index("pipe")
    zi, yi, xi, ti = (lax.axis_index(a) for a in ("z", "y", "x", "t"))
    pairs, _, seq, width = hidden_in.shape[1:]
    heads = attention_probs.shape[3]
    tokens = pairs * 2 * seq
    gain = norm_gain[0]
    wv = value_weight[0]
    wo = output_weight[0]
    inputs = hidden_in[0]
    pattern = attention_probs[0]
    own_head = head_grad[:, 0]

    other_head = lax.ppermute(own_head, ("pipe", "t"), [(2, 3), (3, 2)])

    positions = jnp.arange(seq, dtype=jnp.int32)
    response_bool = (positions[None, None, :] >= sequence_bounds[:, 0:1, None]) & (
        positions[None, None, :] < sequence_bounds[:, 1:3, None]
    )
    ends = jnp.clip(sequence_bounds[:, :2], 0, seq)
    count = jnp.sum(jnp.maximum(ends[:, 1] - ends[:, 0], 0)).reshape(1, 1)
    count = lax.optimization_barrier(jnp.broadcast_to(count, (8, 128)))

    def exchanged(block, z, y, x, section_id):
        base = NZ * NY * NX
        route = []
        for device in range(base):
            zz, yy, xx = device // (NY * NX), device // NX % NY, device % NX
            other = ((zz ^ z) * NY + (yy ^ y)) * NX + (xx ^ x)
            route.append((section_id * base + device, section_id * base + other))
        return lax.ppermute(block, ("pipe", "z", "y", "x"), route)

    for steps in (((0, 0, 1), (0, 1, 0), (0, 1, 1)), ((1, 0, 0), (0, 2, 0), (1, 2, 0))):
        got = [exchanged(count, *at, 0) for at in steps]
        count = count + sum(got)
    mask = response_bool.astype(F32)
    sequence_logprob = jnp.sum(mask * policy_logprob, axis=-1)
    margin = DPO_BETA * (
        sequence_logprob[:, 0]
        - reference_logprob[:, 0]
        - (sequence_logprob[:, 1] - reference_logprob[:, 1])
    )
    weight_pair = jax.nn.sigmoid(-margin)

    def across(block, section_id):
        pairs_xt = ((0, 3), (3, 0), (1, 2), (2, 1))
        base = section_id * 4
        route = [(base + a, base + b) for a, b in pairs_xt]
        return lax.ppermute(block, ("pipe", "x", "t"), route)

    other_wv_1 = across(wv, 1)

    x = inputs.reshape(tokens, width)
    patterns = pattern.reshape(pairs * 2, heads, seq, seq)
    half = tokens // pairs

    y_index = yi.astype(jnp.int32).reshape(1)

    above = heads * HEAD_DIM

    def forward(p, *earlier):
        return pl.pallas_call(
            forward_kernel,
            out_shape=(shaped(2, seq, heads * seq),)
            + (shaped(above + width // NY, tokens),) * NY,
            grid_spec=pltpu.PrefetchScalarGridSpec(
                num_scalar_prefetch=1,
                grid=(1,),
                in_specs=[
                    pl.BlockSpec((half, width), lambda i, y: (p, 0)),
                    pl.BlockSpec((1, width), lambda i, y: (0, 0)),
                    pl.BlockSpec((width, HEAD_DIM), lambda i, y: (0, 0)),
                    pl.BlockSpec((2, heads, seq, seq), lambda i, y: (p, 0, 0, 0)),
                ]
                + [ANY] * len(earlier),
                out_specs=(pl.BlockSpec((2, seq, heads * seq), lambda i, y: (0, 0, 0)),)
                + (pl.BlockSpec((above + width // NY, half), lambda i, y: (0, p)),) * NY,
                scratch_shapes=[pltpu.VMEM((width, half), BF16), pltpu.VMEM((half, above), BF16)],
            ),
            input_output_aliases={5 + n: 1 + n for n in range(len(earlier))},
        )(y_index, x, norm_gain, wv, patterns, *earlier)

    turned_0, *operands = forward(0)
    turned_1, *operands = forward(1, *operands)

    def around(block, shift):
        return lax.ppermute(block, "y", [(i, (i + shift) % NY) for i in range(NY)])

    operands = [operands[0]] + [around(operands[s], s) for s in range(1, NY)]

    upper = section == 1
    is_upper = upper.astype(jnp.int32).reshape(1)
    is_lower = 1 - is_upper
    tensor = ti.astype(jnp.int32).reshape(1)
    block = width // 2

    def values_of(kernel, scalars, blocks, more):
        def along(*shape):
            rank = len(shape)
            return pl.BlockSpec(shape, lambda i, on, *_: (0,) * (rank - 1) + (i * on[0],))

        def whole(*shape):
            return pl.BlockSpec(shape, lambda i, *_: (0,) * len(shape))

        out_shape = [shaped(tokens, HEAD_DIM)] + [shaped(tokens, width)] * more
        out_specs = [whole(tokens, HEAD_DIM)] + [along(tokens, block)] * more
        in_specs = [
            along(*b.shape[:-1], block) if b.shape[-1] == width else whole(*b.shape)
            for b in blocks
        ]
        return pl.pallas_call(
            kernel,
            out_shape=out_shape,
            grid_spec=pltpu.PrefetchScalarGridSpec(
                num_scalar_prefetch=len(scalars),
                grid=(width // block,),
                in_specs=in_specs,
                out_specs=out_specs,
                scratch_shapes=[pltpu.VMEM((tokens, heads * HEAD_DIM), F32)],
            ),
        )(*scalars, *blocks)

    def whole_of(*shape):
        return pl.BlockSpec(shape, lambda n, *_: (0,) * len(shape))

    def rows_of(active, own, other, other_wv, dy):
        def pick(n, on):
            return (n * on[0], 0)

        return pl.pallas_call(
            rows_kernel,
            out_shape=shaped(tokens, width),
            grid_spec=pltpu.PrefetchScalarGridSpec(
                num_scalar_prefetch=1,
                grid=(pairs * 2,),
                in_specs=[
                    pl.BlockSpec((seq, HEAD_DIM), pick),
                    pl.BlockSpec((seq, HEAD_DIM), pick),
                    whole_of(width, HEAD_DIM),
                    whole_of(width, HEAD_DIM),
                    pl.BlockSpec((seq, width), pick),
                    whole_of(1, width),
                    pl.BlockSpec((seq, width), pick),
                ],
                out_specs=pl.BlockSpec((seq, width), pick),
            ),
        )(active, own, other, wv, other_wv, x, norm_gain, dy)

    def own_rows_of(active, weight, done, own, other, other_wv, dy):
        def pick(n, on, t):
            return ((n * 2 + t[0]) * on[0], 0)

        def mine(n, on, t):
            return (n * 2 + t[0], 0)

        return pl.pallas_call(
            own_rows_kernel,
            out_shape=shaped(1, pairs * seq, width),
            grid_spec=pltpu.PrefetchScalarGridSpec(
                num_scalar_prefetch=2,
                grid=(pairs,),
                in_specs=[
                    pl.BlockSpec((seq, 1), mine),
                    pl.BlockSpec((seq, width), lambda n, on, t: ((n * 2 + t[0]) * (1 - on[0]), 0)),
                    pl.BlockSpec((seq, HEAD_DIM), pick),
                    pl.BlockSpec((seq, HEAD_DIM), pick),
                    whole_of(width, HEAD_DIM),
                    whole_of(width, HEAD_DIM),
                    pl.BlockSpec((seq, width), pick),
                    whole_of(1, width),
                    pl.BlockSpec((seq, width), pick),
                ],
                out_specs=pl.BlockSpec((1, seq, width), lambda n, on, t: (0, n, 0)),
            ),
        )(active, tensor, weight, done, own, other, wv, other_wv, x, norm_gain, dy)

    def swapped(values, section_id):
        route = [(section_id * 2, section_id * 2 + 1), (section_id * 2 + 1, section_id * 2)]
        return lax.ppermute(values, ("pipe", "t"), route)

    columns = HEAD_DIM * (heads + 1)
    share_rows = width // (NZ * NY * NX)

    mask_column = mask.reshape(tokens, 1)
    own_1, raw = values_of(
        upper_values_kernel,
        (is_upper, tensor),
        (own_head, other_head, mask_column, wo, turned_0, turned_1),
        1,
    )
    other_1 = swapped(own_1, 1)
    rows_1 = rows_of(is_upper, own_1, other_1, other_wv_1, raw)
    incoming = lax.ppermute(rows_1, "pipe", [(1, 0)])

    partial_count = lax.ppermute(count, "pipe", [(0, 1)])
    full_count = partial_count + exchanged(partial_count, 2, 0, 0, 1)
    full_count = full_count + exchanged(full_count, 4, 0, 0, 1)
    count_down = lax.ppermute(full_count, "pipe", [(1, 0)])
    chosen_total = jnp.where(upper, full_count, count_down)[0, 0]
    pair_total = pairs * NZ * NY * NX
    scale = LIKELIHOOD_COEF * jnp.asarray(pair_total, F32) / chosen_total.astype(F32)
    bare = jnp.stack([-DPO_BETA * weight_pair, DPO_BETA * weight_pair], axis=1)
    bare_row = jnp.broadcast_to(bare[:, :, None], (pairs, 2, seq)).reshape(1, tokens)
    bare_row = lax.optimization_barrier(bare_row)
    lane = lax.broadcasted_iota(jnp.int32, (1, tokens), 1)
    weight = bare_row - jnp.where(lane // seq % 2 == 0, scale, 0.0)
    weight = weight.reshape(tokens, 1)

    (own_0,) = values_of(lower_values_kernel, (is_lower,), (incoming, wo, turned_0, turned_1), 0)
    other_0 = swapped(own_0, 0)
    other_wv_0 = across(wv, 0)

    below = HEAD_DIM + EXTRA
    turned = pl.pallas_call(
        owners_kernel,
        out_shape=(shaped(width // NY + below, tokens),) * NY,
        in_specs=[SMEM, SMEM, ANY, VMEM, ANY, VMEM, VMEM],
        out_specs=(VMEM,) * NY,
        scratch_shapes=[
            pltpu.VMEM((width, tokens), BF16),
            pltpu.VMEM((4, tokens, 896), BF16),
            pltpu.SemaphoreType.DMA((4,)),
        ],
    )(is_upper, y_index, raw, own_1, incoming, own_0, bare_row)
    blocks = [turned[0]] + [around(turned[s], s) for s in range(1, NY)]

    first_own = ((zi % 2) * NX + xi).astype(jnp.int32).reshape(1)
    group = width // NY // 2

    parts = pl.pallas_call(
        products_kernel,
        out_shape=(shaped(4, share_rows, columns),) * 4,
        grid_spec=pltpu.PrefetchScalarGridSpec(
            num_scalar_prefetch=1,
            grid=(2,),
            in_specs=[SMEM]
            + [pl.BlockSpec((group, tokens), lambda i, own: (i, 0))] * NY
            + [pl.BlockSpec((HEAD_DIM, tokens), lambda i, own: (2 * group // HEAD_DIM, 0))] * NY
            + [pl.BlockSpec((EXTRA, tokens), lambda i, own: ((2 * group + HEAD_DIM) // EXTRA, 0))]
            * NY
            + [pl.BlockSpec((group, tokens), lambda i, own: (i + above // group, 0))] * NY
            + [whole_of(above, tokens)] * NY,
            out_specs=(pl.BlockSpec((2, share_rows, columns), lambda i, own: (i, 0, 0)),) * 4,
            scratch_shapes=[pltpu.VMEM((group, columns), F32)],
        ),
    )(
        first_own, scale.reshape(1), *after(tuple(blocks), other_0), *blocks, *blocks,
        *operands, *operands,
    )
    got = [parts[0]] + [over_xz(parts[k], k) for k in (1, 2, 3)]
    parts = pl.pallas_call(
        stage_kernel,
        out_shape=(jax.ShapeDtypeStruct((share_rows, columns), F32),)
        + (shaped(share_rows, columns),) * 3,
        in_specs=[SMEM] + [VMEM] * 4,
        out_specs=(VMEM,) * 4,
    )((zi // 2).astype(jnp.int32).reshape(1), *got)
    got = [parts[0]] + [over_xz(parts[k], k << 2) for k in (1, 2, 3)]

    own_rows = own_rows_of(is_lower, weight, rows_1, own_0, other_0, other_wv_0, incoming)
    start = ((zi * NY + yi) * NX + xi) * share_rows
    own_wv = lax.dynamic_slice_in_dim(wv, start, share_rows, 0).astype(F32)
    own_gain = lax.dynamic_slice_in_dim(gain, start, share_rows, 0).reshape(1, share_rows)
    first_columns = [pl.BlockSpec((share_rows, HEAD_DIM), lambda i: (0, 0))] * 5
    value_share, gain_part = pl.pallas_call(
        gain_kernel,
        out_shape=(
            jax.ShapeDtypeStruct((1, share_rows, HEAD_DIM), F32),
            jax.ShapeDtypeStruct((1, share_rows), F32),
        ),
        grid=(1,),
        in_specs=first_columns + [pl.BlockSpec((1, share_rows), lambda i: (0, 0))],
        out_specs=(
            pl.BlockSpec((1, share_rows, HEAD_DIM), lambda i: (0, 0, 0)),
            pl.BlockSpec((1, share_rows), lambda i: (0, 0)),
        ),
    )(*got, own_wv, own_gain)
    other_part = paired(gain_part, "t", NT, 1)
    output_share = pl.pallas_call(
        last_kernel,
        out_shape=jax.ShapeDtypeStruct((1, share_rows, columns - HEAD_DIM), F32),
        in_specs=[VMEM] * 4,
        out_specs=VMEM,
    )(*got)
    gain_rows = gain_part + other_part
    return own_rows.reshape(1, pairs, 1, seq, width), value_share, output_share, gain_rows


def solution(mesh):
    fine = Mesh(
        mesh.devices.reshape(2, NZ, NY, NX, NT), ("pipe", "z", "y", "x", "t")
    )
    dp = ("z", "y", "x")
    in_specs = (
        P("pipe", dp, None, None, None),
        P("pipe", dp, None, "t", None, None),
        P("pipe", None),
        P("pipe", None, "t"),
        P("pipe", "t", None),
        P(dp, "t", None, None),
        P(dp, None, None),
        P(dp, None),
        P(dp, None),
    )
    out_specs = (
        P("pipe", dp, "t", None, None),
        P("pipe", dp, "t"),
        P("pipe", dp, "t"),
        P("pipe", dp),
    )
    return jax.shard_map(section_step, mesh=fine, in_specs=in_specs, out_specs=out_specs, check_vma=False)
```

```python
import jax
import jax.numpy as jnp
from jax import lax
from jax.experimental import pallas as pl
from jax.experimental.pallas import tpu as pltpu
from jax.sharding import Mesh, PartitionSpec as P


HEAD_DIM = 128
EPSILON = 1e-06
DPO_BETA = 0.25
LIKELIHOOD_COEF = 0.2
NZ, NY, NX, NT = 8, 4, 2, 2
F32, BF16 = jnp.float32, jnp.bfloat16


def paired(block, axis, size, distance, section=None):
    if section is None:
        return lax.ppermute(block, axis, [(i, i ^ distance) for i in range(size)])
    base = section * size
    route = [(base + i, base + (i ^ distance)) for i in range(size)]
    return lax.ppermute(block, ("pipe", axis), route)


def over_xz(block, k):
    route = [
        (z * NX + x, (z ^ (k >> 1)) * NX + (x ^ (k & 1))) for z in range(NZ) for x in range(NX)
    ]
    return lax.ppermute(block, ("z", "x"), route)


VMEM = pl.BlockSpec(memory_space=pltpu.VMEM)
SMEM = pl.BlockSpec(memory_space=pltpu.SMEM)
ANY = pl.BlockSpec(memory_space=pl.ANY)


def dot(a, b, contract):
    return lax.dot_general(a, b, (contract, ((), ())), preferred_element_type=F32)


def rms_of(x):
    return lax.rsqrt(jnp.mean(x * x, axis=-1, keepdims=True) + EPSILON)


def deal(out_refs, source_ref, first_owner):
    size = source_ref.shape[0] // (NZ * NY)
    for s, out_ref in enumerate(out_refs):
        owner = (first_owner + s) % NY
        for z in range(NZ):
            start = pl.multiple_of((z * NY + owner) * size, 16)
            out_ref[z * size : (z + 1) * size] = source_ref[pl.ds(start, size)]


def forward_kernel(y_ref, x_ref, gain_ref, wv_ref, pattern_ref, *refs):
    turned_ref, operand_refs, normed_t_ref = refs[-6], refs[-5:-1], refs[-1]
    heads, seq = pattern_ref.shape[1:3]
    x = x_ref[...].astype(F32)
    normed = (x * rms_of(x) * gain_ref[...]).astype(BF16)
    normed_t_ref[...] = normed.T
    deal(operand_refs, normed_t_ref, y_ref[0])
    values_t = dot(normed, wv_ref[...], ((1,), (0,))).astype(BF16).T
    turned = [pattern_ref[part].reshape(heads * seq, seq).T for part in range(2)]
    for part in range(2):
        turned_ref[part] = turned[part]
    pattern = jnp.concatenate(turned, axis=0).T
    end = operand_refs[0].shape[0]
    for operand_ref in operand_refs:
        operand_ref[end - HEAD_DIM - heads * seq : end - HEAD_DIM] = pattern
        operand_ref[end - HEAD_DIM :] = values_t


def mixed_kernel(*refs):
    count = len(refs) // 2
    for operand_ref, mixed_ref in zip(refs[:count], refs[count:]):
        end = operand_ref.shape[0]
        heads = mixed_ref.shape[1] // HEAD_DIM
        seq = mixed_ref.shape[0] // 4
        for p in range(2):
            lanes = slice(p * 2 * seq, (p + 1) * 2 * seq)
            pattern = operand_ref[end - HEAD_DIM - heads * seq : end - HEAD_DIM, lanes].astype(F32)
            values_t = operand_ref[end - HEAD_DIM :, lanes]
            lane = lax.broadcasted_iota(jnp.int32, pattern.shape, 1)
            for part in range(2):
                mine = jnp.where(lane // seq == part, pattern, 0.0).astype(BF16)
                mixed = dot(mine, values_t, ((1,), (1,))).astype(BF16)
                row = (2 * p + part) * seq
                for h in range(heads):
                    mixed_ref[row : row + seq, h * HEAD_DIM : (h + 1) * HEAD_DIM] = mixed[
                        h * seq : (h + 1) * seq
                    ]


def add_values(step, dy, wo_ref, turned_refs, values_ref, mixed_ref):
    part = dot(dy, wo_ref[...], ((1,), (1,)))

    @pl.when(step == 0)
    def _():
        mixed_ref[...] = part

    @pl.when(step > 0)
    def _():
        mixed_ref[...] += part

    @pl.when(step == pl.num_programs(0) - 1)
    def _():
        per_pair, seq, depth = turned_refs[0].shape
        for n in range(per_pair * len(turned_refs)):
            at = slice(n * seq, (n + 1) * seq)
            mixed = mixed_ref[at].astype(BF16)
            stacked = jnp.concatenate(
                [mixed[:, h * HEAD_DIM : (h + 1) * HEAD_DIM] for h in range(depth // seq)], axis=0
            )
            turned = turned_refs[n // per_pair][n % per_pair]
            values_ref[at] = dot(turned, stacked, ((1,), (0,))).astype(BF16)


def upper_values_kernel(
    active_ref, tensor_ref, own_ref, other_ref, mask_ref, wo_ref, a_ref, b_ref,
    values_ref, raw_ref, mixed_ref,
):
    @pl.when(active_ref[0] == 1)
    def _():
        first = tensor_ref[0] == 0
        seq = own_ref.shape[1]
        for p in range(own_ref.shape[0]):
            own, other = own_ref[p].astype(F32), other_ref[p].astype(F32)
            for c, head in enumerate((jnp.where(first, own, other), jnp.where(first, other, own))):
                at = slice((2 * p + c) * seq, (2 * p + c + 1) * seq)
                raw_ref[at] = (mask_ref[at] * head).astype(BF16)
        step = pl.program_id(0)
        add_values(step, raw_ref[...], wo_ref, (a_ref, b_ref), values_ref, mixed_ref)


def lower_values_kernel(active_ref, dy_ref, wo_ref, a_ref, b_ref, values_ref, mixed_ref):
    @pl.when(active_ref[0] == 1)
    def _():
        step = pl.program_id(0)
        add_values(step, dy_ref[...], wo_ref, (a_ref, b_ref), values_ref, mixed_ref)


def rows_of_sequence(own_ref, other_ref, own_wv_ref, other_wv_ref, x_ref, gain_ref, dy_ref):
    first = dot(own_ref[...], own_wv_ref[...], ((1,), (1,))).astype(BF16)
    second = dot(other_ref[...], other_wv_ref[...], ((1,), (1,))).astype(BF16)
    scaled = (first.astype(F32) + second.astype(F32)) * gain_ref[...]
    x = x_ref[...].astype(F32)
    inverse = rms_of(x)
    pull = (inverse * inverse * inverse) * jnp.mean(x * scaled, axis=-1, keepdims=True)
    return dy_ref[...].astype(F32) + (inverse * scaled - x * pull)


def rows_kernel(active_ref, *refs):
    @pl.when(active_ref[0] == 1)
    def _():
        refs[-1][...] = rows_of_sequence(*refs[:-1]).astype(BF16)


def own_rows_kernel(active_ref, tensor_ref, weight_ref, done_ref, *refs):
    @pl.when(active_ref[0] == 1)
    def _():
        refs[-1][0] = (weight_ref[...] * rows_of_sequence(*refs[:-1])).astype(BF16)

    @pl.when(active_ref[0] == 0)
    def _():
        refs[-1][0] = (weight_ref[...] * done_ref[...].astype(F32)).astype(BF16)


EXTRA = 16


def owners_kernel(upper_ref, y_ref, *refs):
    (upper_dy, upper_values, lower_dy, lower_values, weight_ref), refs = refs[:5], refs[5:]
    out_refs, turned_ref, dy_buffer, sems = refs[:NY], refs[NY], refs[NY + 1], refs[NY + 2]
    block = dy_buffer.shape[2]

    def turn(dy_hbm, values_ref):
        tokens, width = dy_hbm.shape
        copies = [
            pltpu.make_async_copy(
                dy_hbm.at[:, start : start + block], dy_buffer.at[n], sems.at[n]
            )
            for n, start in enumerate(range(0, width, block))
        ]
        for copy in copies:
            copy.start()
        weight = weight_ref[...]
        high = weight.astype(BF16).astype(F32)
        rest = jnp.zeros((EXTRA - 2, tokens), F32)
        below = jnp.concatenate([high, weight - high, rest], axis=0).astype(BF16)
        values_t = values_ref[...].T
        for out_ref in out_refs:
            rows = out_ref.shape[0]
            out_ref[rows - EXTRA - HEAD_DIM : rows - EXTRA] = values_t
            out_ref[rows - EXTRA :] = below
        for n, copy in enumerate(copies):
            copy.wait()
            turned_ref[n * block : (n + 1) * block] = dy_buffer[n].T

    @pl.when(upper_ref[0] == 1)
    def _():
        turn(upper_dy, upper_values)

    @pl.when(upper_ref[0] == 0)
    def _():
        turn(lower_dy, lower_values)

    deal(out_refs, turned_ref, y_ref[0])


def products_kernel(own_ref, scale_ref, *refs):
    groups, refs = [refs[n * NY : (n + 1) * NY] for n in range(5)], refs[5 * NY :]
    out_refs, total_ref = refs[:-1], refs[-1]
    tokens = groups[0][0].shape[1]
    lane = lax.broadcasted_iota(jnp.int32, (1, tokens), 1)
    chosen = jnp.where(lane // 64 % 2 == 0, scale_ref[0], 0.0)
    value, output = 0.0, 0.0
    for dy_ref, values_ref, weight_ref, normed_ref, mixed_ref in zip(*groups):
        rows = weight_ref[...].astype(F32)
        weight = rows[0:1] + rows[1:2] - chosen
        dy = (weight * dy_ref[...].astype(F32)).astype(BF16)
        values_t = (weight * values_ref[...].astype(F32)).astype(BF16)
        output = output + dot(dy, mixed_ref[...], ((1,), (0,)))
        value = value + dot(normed_ref[...], values_t, ((1,), (1,)))
    total_ref[:, :HEAD_DIM] = value
    total_ref[:, HEAD_DIM:] = output
    count, size = out_refs[0].shape[:2]
    for k, out_ref in enumerate(out_refs):
        for n in range(count):
            start = pl.multiple_of((n * 4 + (own_ref[0] ^ k)) * size, 8)
            out_ref[n] = total_ref[pl.ds(start, size)].astype(BF16)


def stage_kernel(own_ref, a_ref, b_ref, c_ref, d_ref, *out_refs):
    for k, out_ref in enumerate(out_refs):
        j = own_ref[0] ^ k
        total = sum(r[j].astype(F32) for r in (a_ref, b_ref, c_ref, d_ref))
        out_ref[...] = total.astype(out_ref.dtype)


def gain_kernel(a_ref, b_ref, c_ref, d_ref, wv_ref, gain_ref, value_ref, part_ref):
    value = a_ref[...] + sum(r[...].astype(F32) for r in (b_ref, c_ref, d_ref))
    value_ref[0] = value
    row = lax.dot_general(
        jnp.ones((8, HEAD_DIM), F32),
        wv_ref[...] * value,
        (((1,), (1,)), ((), ())),
        precision=lax.Precision.HIGHEST,
        preferred_element_type=F32,
    )
    part_ref[...] = row[:1] / gain_ref[...]


def last_kernel(a_ref, b_ref, c_ref, d_ref, output_ref):
    total = a_ref[:, HEAD_DIM:]
    output_ref[0] = total + sum(r[:, HEAD_DIM:].astype(F32) for r in (b_ref, c_ref, d_ref))


def shaped(*dims):
    return jax.ShapeDtypeStruct(dims, BF16)


def after(block, *others):
    return lax.optimization_barrier((block, *others))[0]


def section_step(
    hidden_in,
    attention_probs,
    norm_gain,
    value_weight,
    output_weight,
    head_grad,
    policy_logprob,
    reference_logprob,
    sequence_bounds,
):
    section = lax.axis_index("pipe")
    zi, yi, xi, ti = (lax.axis_index(a) for a in ("z", "y", "x", "t"))
    pairs, _, seq, width = hidden_in.shape[1:]
    heads = attention_probs.shape[3]
    tokens = pairs * 2 * seq
    gain = norm_gain[0]
    wv = value_weight[0]
    wo = output_weight[0]
    inputs = hidden_in[0]
    pattern = attention_probs[0]
    own_head = head_grad[:, 0]

    other_head = lax.ppermute(own_head, ("pipe", "t"), [(2, 3), (3, 2)])

    positions = jnp.arange(seq, dtype=jnp.int32)
    response_bool = (positions[None, None, :] >= sequence_bounds[:, 0:1, None]) & (
        positions[None, None, :] < sequence_bounds[:, 1:3, None]
    )
    ends = jnp.clip(sequence_bounds[:, :2], 0, seq)
    count = jnp.sum(jnp.maximum(ends[:, 1] - ends[:, 0], 0)).reshape(1, 1)
    count = lax.optimization_barrier(jnp.broadcast_to(count, (8, 128)))

    def exchanged(block, z, y, x, section_id):
        base = NZ * NY * NX
        route = []
        for device in range(base):
            zz, yy, xx = device // (NY * NX), device // NX % NY, device % NX
            other = ((zz ^ z) * NY + (yy ^ y)) * NX + (xx ^ x)
            route.append((section_id * base + device, section_id * base + other))
        return lax.ppermute(block, ("pipe", "z", "y", "x"), route)

    for steps in (((0, 0, 1), (0, 1, 0), (0, 1, 1)), ((1, 0, 0), (0, 2, 0), (1, 2, 0))):
        got = [exchanged(count, *at, 0) for at in steps]
        count = count + sum(got)
    mask = response_bool.astype(F32)
    sequence_logprob = jnp.sum(mask * policy_logprob, axis=-1)
    margin = DPO_BETA * (
        sequence_logprob[:, 0]
        - reference_logprob[:, 0]
        - (sequence_logprob[:, 1] - reference_logprob[:, 1])
    )
    weight_pair = jax.nn.sigmoid(-margin)

    def across(block, section_id):
        pairs_xt = ((0, 3), (3, 0), (1, 2), (2, 1))
        base = section_id * 4
        route = [(base + a, base + b) for a, b in pairs_xt]
        return lax.ppermute(block, ("pipe", "x", "t"), route)

    other_wv_1 = across(wv, 1)

    x = inputs.reshape(tokens, width)
    patterns = pattern.reshape(pairs * 2, heads, seq, seq)
    half = tokens // pairs

    y_index = yi.astype(jnp.int32).reshape(1)

    operand_rows = width // NY + heads * seq + HEAD_DIM

    def forward(p, *earlier):
        return pl.pallas_call(
            forward_kernel,
            out_shape=(shaped(2, seq, heads * seq),)
            + (shaped(operand_rows, tokens),) * NY,
            grid_spec=pltpu.PrefetchScalarGridSpec(
                num_scalar_prefetch=1,
                grid=(1,),
                in_specs=[
                    pl.BlockSpec((half, width), lambda i, y: (p, 0)),
                    pl.BlockSpec((1, width), lambda i, y: (0, 0)),
                    pl.BlockSpec((width, HEAD_DIM), lambda i, y: (0, 0)),
                    pl.BlockSpec((2, heads, seq, seq), lambda i, y: (p, 0, 0, 0)),
                ]
                + [ANY] * len(earlier),
                out_specs=(pl.BlockSpec((2, seq, heads * seq), lambda i, y: (0, 0, 0)),)
                + (pl.BlockSpec((operand_rows, half), lambda i, y: (0, p)),) * NY,
                scratch_shapes=[pltpu.VMEM((width, half), BF16)],
            ),
            input_output_aliases={5 + n: 1 + n for n in range(len(earlier))},
        )(y_index, x, norm_gain, wv, patterns, *earlier)

    turned_0, *operands = forward(0)
    turned_1, *operands = forward(1, *operands)

    def around(block, shift):
        return lax.ppermute(block, "y", [(i, (i + shift) % NY) for i in range(NY)])

    operands = [operands[0]] + [around(operands[s], s) for s in range(1, NY)]

    upper = section == 1
    is_upper = upper.astype(jnp.int32).reshape(1)
    is_lower = 1 - is_upper
    tensor = ti.astype(jnp.int32).reshape(1)
    block = width // 2

    def values_of(kernel, scalars, blocks, more):
        def along(*shape):
            rank = len(shape)
            return pl.BlockSpec(shape, lambda i, on, *_: (0,) * (rank - 1) + (i * on[0],))

        def whole(*shape):
            return pl.BlockSpec(shape, lambda i, *_: (0,) * len(shape))

        out_shape = [shaped(tokens, HEAD_DIM)] + [shaped(tokens, width)] * more
        out_specs = [whole(tokens, HEAD_DIM)] + [along(tokens, block)] * more
        in_specs = [
            along(*b.shape[:-1], block) if b.shape[-1] == width else whole(*b.shape)
            for b in blocks
        ]
        return pl.pallas_call(
            kernel,
            out_shape=out_shape,
            grid_spec=pltpu.PrefetchScalarGridSpec(
                num_scalar_prefetch=len(scalars),
                grid=(width // block,),
                in_specs=in_specs,
                out_specs=out_specs,
                scratch_shapes=[pltpu.VMEM((tokens, heads * HEAD_DIM), F32)],
            ),
        )(*scalars, *blocks)

    def whole_of(*shape):
        return pl.BlockSpec(shape, lambda n, *_: (0,) * len(shape))

    def rows_of(active, own, other, other_wv, dy):
        def pick(n, on):
            return (n * on[0], 0)

        return pl.pallas_call(
            rows_kernel,
            out_shape=shaped(tokens, width),
            grid_spec=pltpu.PrefetchScalarGridSpec(
                num_scalar_prefetch=1,
                grid=(pairs * 2,),
                in_specs=[
                    pl.BlockSpec((seq, HEAD_DIM), pick),
                    pl.BlockSpec((seq, HEAD_DIM), pick),
                    whole_of(width, HEAD_DIM),
                    whole_of(width, HEAD_DIM),
                    pl.BlockSpec((seq, width), pick),
                    whole_of(1, width),
                    pl.BlockSpec((seq, width), pick),
                ],
                out_specs=pl.BlockSpec((seq, width), pick),
            ),
        )(active, own, other, wv, other_wv, x, norm_gain, dy)

    def own_rows_of(active, weight, done, own, other, other_wv, dy):
        def pick(n, on, t):
            return ((n * 2 + t[0]) * on[0], 0)

        def mine(n, on, t):
            return (n * 2 + t[0], 0)

        return pl.pallas_call(
            own_rows_kernel,
            out_shape=shaped(1, pairs * seq, width),
            grid_spec=pltpu.PrefetchScalarGridSpec(
                num_scalar_prefetch=2,
                grid=(pairs,),
                in_specs=[
                    pl.BlockSpec((seq, 1), mine),
                    pl.BlockSpec((seq, width), lambda n, on, t: ((n * 2 + t[0]) * (1 - on[0]), 0)),
                    pl.BlockSpec((seq, HEAD_DIM), pick),
                    pl.BlockSpec((seq, HEAD_DIM), pick),
                    whole_of(width, HEAD_DIM),
                    whole_of(width, HEAD_DIM),
                    pl.BlockSpec((seq, width), pick),
                    whole_of(1, width),
                    pl.BlockSpec((seq, width), pick),
                ],
                out_specs=pl.BlockSpec((1, seq, width), lambda n, on, t: (0, n, 0)),
            ),
        )(active, tensor, weight, done, own, other, wv, other_wv, x, norm_gain, dy)

    def swapped(values, section_id):
        route = [(section_id * 2, section_id * 2 + 1), (section_id * 2 + 1, section_id * 2)]
        return lax.ppermute(values, ("pipe", "t"), route)

    columns = HEAD_DIM * (heads + 1)
    share_rows = width // (NZ * NY * NX)

    mask_column = mask.reshape(tokens, 1)
    own_1, raw = values_of(
        upper_values_kernel,
        (is_upper, tensor),
        (own_head, other_head, mask_column, wo, turned_0, turned_1),
        1,
    )
    other_1 = swapped(own_1, 1)
    rows_1 = rows_of(is_upper, own_1, other_1, other_wv_1, raw)
    incoming = lax.ppermute(rows_1, "pipe", [(1, 0)])

    partial_count = lax.ppermute(count, "pipe", [(0, 1)])
    full_count = partial_count + exchanged(partial_count, 2, 0, 0, 1)
    full_count = full_count + exchanged(full_count, 4, 0, 0, 1)
    count_down = lax.ppermute(full_count, "pipe", [(1, 0)])
    chosen_total = jnp.where(upper, full_count, count_down)[0, 0]
    pair_total = pairs * NZ * NY * NX
    scale = LIKELIHOOD_COEF * jnp.asarray(pair_total, F32) / chosen_total.astype(F32)
    bare = jnp.stack([-DPO_BETA * weight_pair, DPO_BETA * weight_pair], axis=1)
    bare_row = jnp.broadcast_to(bare[:, :, None], (pairs, 2, seq)).reshape(1, tokens)
    bare_row = lax.optimization_barrier(bare_row)
    lane = lax.broadcasted_iota(jnp.int32, (1, tokens), 1)
    weight = bare_row - jnp.where(lane // seq % 2 == 0, scale, 0.0)
    weight = weight.reshape(tokens, 1)

    (own_0,) = values_of(lower_values_kernel, (is_lower,), (incoming, wo, turned_0, turned_1), 0)
    other_0 = swapped(own_0, 0)
    other_wv_0 = across(wv, 0)

    below = HEAD_DIM + EXTRA
    turned = pl.pallas_call(
        owners_kernel,
        out_shape=(shaped(width // NY + below, tokens),) * NY,
        in_specs=[SMEM, SMEM, ANY, VMEM, ANY, VMEM, VMEM],
        out_specs=(VMEM,) * NY,
        scratch_shapes=[
            pltpu.VMEM((width, tokens), BF16),
            pltpu.VMEM((4, tokens, 896), BF16),
            pltpu.SemaphoreType.DMA((4,)),
        ],
    )(is_upper, y_index, raw, own_1, incoming, own_0, bare_row)
    blocks = [turned[0]] + [around(turned[s], s) for s in range(1, NY)]

    first_own = ((zi % 2) * NX + xi).astype(jnp.int32).reshape(1)
    group = width // NY // 2

    mixed_all = pl.pallas_call(
        mixed_kernel,
        out_shape=(shaped(tokens, heads * HEAD_DIM),) * NY,
        in_specs=[VMEM] * NY,
        out_specs=(VMEM,) * NY,
    )(*operands)
    parts = pl.pallas_call(
        products_kernel,
        out_shape=(shaped(4, share_rows, columns),) * 4,
        grid_spec=pltpu.PrefetchScalarGridSpec(
            num_scalar_prefetch=1,
            grid=(2,),
            in_specs=[SMEM]
            + [pl.BlockSpec((group, tokens), lambda i, own: (i, 0))] * NY
            + [pl.BlockSpec((HEAD_DIM, tokens), lambda i, own: (2 * group // HEAD_DIM, 0))] * NY
            + [pl.BlockSpec((EXTRA, tokens), lambda i, own: ((2 * group + HEAD_DIM) // EXTRA, 0))]
            * NY
            + [pl.BlockSpec((group, tokens), lambda i, own: (i, 0))] * NY
            + [whole_of(tokens, heads * HEAD_DIM)] * NY,
            out_specs=(pl.BlockSpec((2, share_rows, columns), lambda i, own: (i, 0, 0)),) * 4,
            scratch_shapes=[pltpu.VMEM((group, columns), F32)],
        ),
    )(
        first_own, scale.reshape(1), *after(tuple(blocks), other_0), *blocks, *blocks,
        *operands, *mixed_all,
    )
    got = [parts[0]] + [over_xz(parts[k], k) for k in (1, 2, 3)]
    parts = pl.pallas_call(
        stage_kernel,
        out_shape=(jax.ShapeDtypeStruct((share_rows, columns), F32),)
        + (shaped(share_rows, columns),) * 3,
        in_specs=[SMEM] + [VMEM] * 4,
        out_specs=(VMEM,) * 4,
    )((zi // 2).astype(jnp.int32).reshape(1), *got)
    got = [parts[0]] + [over_xz(parts[k], k << 2) for k in (1, 2, 3)]

    own_rows = own_rows_of(is_lower, weight, rows_1, own_0, other_0, other_wv_0, incoming)
    start = ((zi * NY + yi) * NX + xi) * share_rows
    own_wv = lax.dynamic_slice_in_dim(wv, start, share_rows, 0).astype(F32)
    own_gain = lax.dynamic_slice_in_dim(gain, start, share_rows, 0).reshape(1, share_rows)
    first_columns = [pl.BlockSpec((share_rows, HEAD_DIM), lambda i: (0, 0))] * 5
    value_share, gain_part = pl.pallas_call(
        gain_kernel,
        out_shape=(
            jax.ShapeDtypeStruct((1, share_rows, HEAD_DIM), F32),
            jax.ShapeDtypeStruct((1, share_rows), F32),
        ),
        grid=(1,),
        in_specs=first_columns + [pl.BlockSpec((1, share_rows), lambda i: (0, 0))],
        out_specs=(
            pl.BlockSpec((1, share_rows, HEAD_DIM), lambda i: (0, 0, 0)),
            pl.BlockSpec((1, share_rows), lambda i: (0, 0)),
        ),
    )(*got, own_wv, own_gain)
    other_part = paired(gain_part, "t", NT, 1)
    output_share = pl.pallas_call(
        last_kernel,
        out_shape=jax.ShapeDtypeStruct((1, share_rows, columns - HEAD_DIM), F32),
        in_specs=[VMEM] * 4,
        out_specs=VMEM,
    )(*got)
    gain_rows = gain_part + other_part
    return own_rows.reshape(1, pairs, 1, seq, width), value_share, output_share, gain_rows


def solution(mesh):
    fine = Mesh(
        mesh.devices.reshape(2, NZ, NY, NX, NT), ("pipe", "z", "y", "x", "t")
    )
    dp = ("z", "y", "x")
    in_specs = (
        P("pipe", dp, None, None, None),
        P("pipe", dp, None, "t", None, None),
        P("pipe", None),
        P("pipe", None, "t"),
        P("pipe", "t", None),
        P(dp, "t", None, None),
        P(dp, None, None),
        P(dp, None),
        P(dp, None),
    )
    out_specs = (
        P("pipe", dp, "t", None, None),
        P("pipe", dp, "t"),
        P("pipe", dp, "t"),
        P("pipe", dp),
    )
    return jax.shard_map(section_step, mesh=fine, in_specs=in_specs, out_specs=out_specs, check_vma=False)
```
